32 devices in a mesh: groups: 2 (over y), seq: 4 (over z), head: 2 (over x), sub: 2 (over core).
Axes of the slice: x: 2, y: 2, z: 4, core: 2. Of those that a mesh axis runs over, the one named last changes fastest.
Arguments:
- queries: bfloat16 [32, 64, 8192], P(('groups', 'seq'), None, 'head'), parts along dimension 0, may hold values from -6 to 6
- new_kv: bfloat16 [32, 64, 2, 1024], P(('groups', 'seq'), None, None, 'head'), parts along dimension 0, may hold values from -6 to 6
- kv_pages: bfloat16 [336, 2, 128, 1024], P(('groups', 'seq', 'sub'), None, None, 'head'), parts along dimension 0, may hold values from -6 to 6
- page_table: int32 [32, 16], P('groups'), parts along dimension 0, may hold values from -1 to 167, as said below
- cached_len: int32 [32], P('groups'), parts along dimension 0, may hold values from 1 to 2048, as said below
- is_prefill: int32 [32], P('groups'), parts along dimension 0, may hold values from 0 to 1, as said below
Outputs:
- attended: bfloat16 [32, 64, 8192], P(('groups', 'seq'), None, 'head'), parts along dimension 0
The draws below stay inside these ranges and needn't reach their ends.
There are 2 independent parts, one for each index of `groups`. The reference program is written for one: setup_inputs(seed, part) draws one part's arguments, and reference() takes and returns one part's arrays. A program takes and returns all parts, laid end to end along the dimension named above; each array names one. Nothing has to cross between parts.
Inputs may be any that keep to these rules, and one draw needn't show every extreme that they name: `page_table`: entry [s, p] is the page number of page p of sequence s for p < ceil(cached_len[s] / 128) and -1 after; page number q lies on owner q // 21 (owner index = seq index * 2 + sub index) in its slot q % 21. Listing the pages of all sequences in order of sequence and page as t = 0, 1, ..., page t has owner (t + c) % 8 and slot (t + c) // 8 for one drawn c. No owner holds more than 8 page of the 4 sequences of one seq shard, and some owner holds exactly 8. `cached_len`: A decode sequence has 1 to 4 cache pages, a prefill sequence 8 to 16; all 4 sequences of one drawn seq shard are prefill sequences with 16 pages. `is_prefill`: exactly 8 sequences are prefill sequences.
All inputs are finite; a program needn't handle non-finite values.
Results may differ from the reference program's by a relative error of at most 0.014.
Values may be sent and summed in bfloat16 or wider, within the bound.
A program may use at most 64 MiB of HBM per device.

```python
import jax
import jax.numpy as jnp
from jax import lax

HQ = 64
KVH = 8
HD = 128
PAGE = 128
MAXP = 16
DEC_MAXP = 4
QROWS = 64
SEQ_DEV = 4
SEQS = 16
PREFILL = 8
OWNERS = 8
PAGES_DEV = 21


def page_layout(key):
    heavy_key = jax.random.fold_in(key, 101)
    order_key = jax.random.fold_in(key, 102)
    long_key = jax.random.fold_in(key, 103)
    short_key = jax.random.fold_in(key, 104)
    tail_key = jax.random.fold_in(key, 105)
    rotate_key = jax.random.fold_in(key, 106)
    shard_total = SEQS // SEQ_DEV
    heavy = jax.random.randint(heavy_key, (), 0, shard_total)
    seq_ids = jnp.arange(SEQS, dtype=jnp.int32)
    in_heavy = seq_ids // SEQ_DEV == heavy
    shuffled = jax.random.permutation(order_key, SEQS).astype(jnp.int32)
    keyed = jnp.where(in_heavy, -1, shuffled)
    standing = jnp.sum((keyed[None, :] < keyed[:, None]).astype(jnp.int32), axis=1)
    prefill = standing < PREFILL
    long_pages = jax.random.randint(long_key, (SEQS,), MAXP // 2, MAXP + 1)
    short_pages = jax.random.randint(short_key, (SEQS,), 1, DEC_MAXP + 1)
    page_total = jnp.where(in_heavy, MAXP, jnp.where(prefill, long_pages, short_pages)).astype(jnp.int32)
    cached = (page_total - 1) * PAGE + jax.random.randint(tail_key, (SEQS,), 1, PAGE + 1)
    first_page = jnp.cumsum(page_total) - page_total
    rotation = jax.random.randint(rotate_key, (), 0, OWNERS)
    page_ids = jnp.arange(MAXP, dtype=jnp.int32)
    linear = first_page[:, None] + page_ids[None, :] + rotation
    number = linear % OWNERS * PAGES_DEV + linear // OWNERS
    table_rows = jnp.where(page_ids[None, :] < page_total[:, None], number, -1)
    return (table_rows.astype(jnp.int32), cached.astype(jnp.int32), prefill.astype(jnp.int32))


def draw_page_table(key, part):
    return page_layout(key)[0]


def draw_cached_len(key, part):
    return page_layout(key)[1]


def draw_is_prefill(key, part):
    return page_layout(key)[2]


def draw_queries(key, part):
    shape = (SEQS, QROWS, HQ * HD)
    values = jnp.clip(jax.random.normal(jax.random.fold_in(key, 11), shape, jnp.float32), -5.0, 5.0)
    return values.astype(jnp.bfloat16)


def draw_kv_pages(key, part):
    shape = (PAGES_DEV * OWNERS, 2, PAGE, KVH * HD)
    values = jnp.clip(jax.random.normal(jax.random.fold_in(key, 12), shape, jnp.float32), -5.0, 5.0)
    return values.astype(jnp.bfloat16)


def block_levels(stream_key, extent, pieces, least, largest):
    loudness, own = 1.0, jax.random.fold_in(stream_key, 6)
    for dim, blocks in pieces:
        steps = jnp.exp(jax.random.uniform(jax.random.fold_in(own, dim), (blocks,), jnp.float32, least / len(pieces), largest / len(pieces)))
        loudness = loudness * jnp.repeat(steps, extent[dim] // blocks).reshape([-1 if axis == dim else 1 for axis in range(len(extent))])
    return loudness


def normal_values(rng, shape, scale, bound, pieces=(), kind=jnp.bfloat16):
    level = block_levels(rng, shape, pieces, -0.22, 0.18) if pieces else 1.0
    values = jax.random.normal(rng, shape, jnp.float32) * scale * level
    return jnp.minimum(jnp.maximum(values, -bound), bound).astype(kind)


def setup_inputs(seed: int = 0, part: int = 0) -> dict:
    splits = jax.random.split(jax.random.key(seed), 7)
    own_keys = jax.random.split(jax.random.fold_in(splits[6], part), 7)
    return {
        "queries": draw_queries(jax.random.fold_in(jax.random.fold_in(splits[6], part), 71), part),
        "new_kv": normal_values(own_keys[1], (SEQS, QROWS, 2, KVH * HD), 1.0, 6.0, ((0, 4), (3, 2))),
        "kv_pages": draw_kv_pages(jax.random.fold_in(jax.random.fold_in(splits[6], part), 71), part),
        "page_table": draw_page_table(jax.random.fold_in(jax.random.fold_in(splits[6], part), 71), part),
        "cached_len": draw_cached_len(jax.random.fold_in(jax.random.fold_in(splits[6], part), 71), part),
        "is_prefill": draw_is_prefill(jax.random.fold_in(jax.random.fold_in(splits[6], part), 71), part),
    }


NEG_FILL = -1e30


def reference(queries, new_kv, kv_pages, page_table, cached_len, is_prefill):
    group_size = HQ // KVH
    score_scale = HD ** -0.5
    positions = jnp.arange(MAXP * PAGE, dtype=jnp.int32)
    row_ids = jnp.arange(QROWS, dtype=jnp.int32)
    causal = row_ids[None, :] <= row_ids[:, None]

    def one_sequence(inputs):
        query_rows, fresh_rows, table_row, length, flag = inputs
        fetched = jnp.take(kv_pages, jnp.maximum(table_row, 0).astype(jnp.int32), axis=0)
        cache_keys = fetched[:, 0].reshape(MAXP * PAGE, KVH, HD).astype(jnp.float32)
        cache_values = fetched[:, 1].reshape(MAXP * PAGE, KVH, HD).astype(jnp.float32)
        cache_valid = positions < length
        live_row = (flag == 1) | (row_ids == 0)
        query_heads = query_rows.reshape(QROWS, KVH, group_size, HD).astype(jnp.float32)
        fresh_keys = fresh_rows[:, 0].reshape(QROWS, KVH, HD).astype(jnp.float32)
        fresh_values = fresh_rows[:, 1].reshape(QROWS, KVH, HD).astype(jnp.float32)
        fresh_valid = causal & live_row[:, None]
        cache_scores = jnp.einsum("rkgd,nkd->kgrn", query_heads, cache_keys) * score_scale
        fresh_scores = jnp.einsum("rkgd,jkd->kgrj", query_heads, fresh_keys) * score_scale
        cache_mask = cache_valid[None, None, None, :]
        fresh_mask = fresh_valid[None, None, :, :]
        peak = jnp.maximum(jnp.max(jnp.where(cache_mask, cache_scores, NEG_FILL), axis=-1),
                           jnp.max(jnp.where(fresh_mask, fresh_scores, NEG_FILL), axis=-1))
        cache_weights = jnp.where(cache_mask, jnp.exp(cache_scores - peak[..., None]), 0.0)
        fresh_weights = jnp.where(fresh_mask, jnp.exp(fresh_scores - peak[..., None]), 0.0)
        weight_sum = jnp.sum(cache_weights, axis=-1) + jnp.sum(fresh_weights, axis=-1)
        cache_rounded = lax.optimization_barrier(cache_weights.astype(jnp.bfloat16)).astype(jnp.float32)
        fresh_rounded = lax.optimization_barrier(fresh_weights.astype(jnp.bfloat16)).astype(jnp.float32)
        numerator = jnp.einsum("kgrn,nkd->kgrd", cache_rounded, cache_values)
        numerator = numerator + jnp.einsum("kgrj,jkd->kgrd", fresh_rounded, fresh_values)
        unused_rows = 1.0 - live_row.astype(jnp.float32)
        attended = numerator / (weight_sum + unused_rows[None, None, :])[..., None]
        attended = jnp.where(live_row[None, None, :, None], attended, 0.0)
        return jnp.transpose(attended, (2, 0, 1, 3)).reshape(QROWS, HQ * HD).astype(jnp.bfloat16)

    return lax.map(one_sequence, (queries, new_kv, page_table, cached_len, is_prefill))
```

```python
import functools
import itertools

import jax
import jax.numpy as jnp
from jax import lax
from jax.experimental import pallas as pl
from jax.experimental.pallas import tpu as pltpu
from jax.sharding import PartitionSpec as P

HD = 128
PAGE = 128


NEG_FILL = -1e30


def partial_softmax(
    query_heads, cache_keys, cache_values, cache_valid, fresh_keys, fresh_values, fresh_valid
):
    score_scale = HD ** (-0.5)
    cache_scores = (
        jnp.einsum("rkgd,nkd->kgrn", query_heads, cache_keys, preferred_element_type=jnp.float32)
        * score_scale
    )
    fresh_scores = (
        jnp.einsum("rkgd,jkd->kgrj", query_heads, fresh_keys, preferred_element_type=jnp.float32)
        * score_scale
    )
    cache_mask = cache_valid[None, None, None, :]
    fresh_mask = fresh_valid[None, None, :, :]
    peak = jnp.maximum(
        jnp.max(jnp.where(cache_mask, cache_scores, NEG_FILL), axis=-1),
        jnp.max(jnp.where(fresh_mask, fresh_scores, NEG_FILL), axis=-1),
    )
    cache_weights = jnp.where(cache_mask, jnp.exp(cache_scores - peak[..., None]), 0.0)
    fresh_weights = jnp.where(fresh_mask, jnp.exp(fresh_scores - peak[..., None]), 0.0)
    weight_sum = jnp.sum(cache_weights, axis=-1) + jnp.sum(fresh_weights, axis=-1)
    numerator = jnp.einsum(
        "kgrn,nkd->kgrd",
        cache_weights.astype(jnp.bfloat16),
        cache_values,
        preferred_element_type=jnp.float32,
    )
    numerator = numerator + jnp.einsum(
        "kgrj,jkd->kgrd",
        fresh_weights.astype(jnp.bfloat16),
        fresh_values,
        preferred_element_type=jnp.float32,
    )
    return (peak, weight_sum, numerator)


def attend_all(
    query_block, fresh_block, received, fetch_index, page_here, lengths, live_rows, causal, fresh_on
):
    kv_width = received.shape[-1]
    heads_kv = kv_width // HD
    row_count = query_block.shape[1]
    group_size = query_block.shape[2] // kv_width
    page_count = fetch_index.shape[1]
    positions = jnp.arange(page_count * PAGE, dtype=jnp.int32)

    def one_sequence(inputs):
        query_rows, fresh_rows, index_row, here_row, length, live_row = inputs
        fetched = jnp.take(received, index_row, axis=0)
        cache_keys = fetched[:, 0].reshape(page_count * PAGE, heads_kv, HD)
        cache_values = fetched[:, 1].reshape(page_count * PAGE, heads_kv, HD)
        page_mask = jnp.broadcast_to(here_row[:, None], (page_count, PAGE)).reshape(
            page_count * PAGE
        )
        cache_valid = page_mask & (positions < length)
        query_heads = query_rows.reshape(row_count, heads_kv, group_size, HD)
        fresh_keys = fresh_rows[:, 0].reshape(row_count, heads_kv, HD)
        fresh_values = fresh_rows[:, 1].reshape(row_count, heads_kv, HD)
        fresh_valid = causal & live_row[:, None] & fresh_on
        return partial_softmax(
            query_heads,
            cache_keys,
            cache_values,
            cache_valid,
            fresh_keys,
            fresh_values,
            fresh_valid,
        )

    return lax.map(
        one_sequence, (query_block, fresh_block, fetch_index, page_here, lengths, live_rows)
    )


def finish(weight_sum, numerator, live_rows):
    unused_rows = 1.0 - live_rows.astype(jnp.float32)
    attended = numerator / (weight_sum + unused_rows[:, None, None, :])[..., None]
    attended = jnp.where(live_rows[:, None, None, :, None], attended, 0.0)
    seq_dev, heads_kv, group_size, row_count, head_dim = attended.shape
    return (
        jnp.transpose(attended, (0, 3, 1, 2, 4))
        .reshape(seq_dev, row_count, heads_kv * group_size * head_dim)
        .astype(jnp.bfloat16)
    )


def exchange_pages(queries, new_kv, kv_pages, page_table, cached_len, is_prefill):
    seq_shards = lax.axis_size("seq")
    sub_count = lax.axis_size("sub")
    owners = seq_shards * sub_count
    seq_index = lax.axis_index("seq")
    core_index = lax.axis_index("sub")
    owner_self = seq_index * sub_count + core_index
    seq_dev, row_count, query_width = queries.shape
    pages_dev = kv_pages.shape[0]
    kv_width = kv_pages.shape[3]
    page_count = page_table.shape[1]
    entries = seq_dev * page_count
    capacity = (entries + owners - 1) // owners
    table_rows = page_table.reshape(seq_shards, entries)
    holder = jnp.where(table_rows >= 0, table_rows // pages_dev, -1)
    slot_of = jnp.where(table_rows >= 0, table_rows % pages_dev, 0)
    owned_here = holder == owner_self
    rank_among = jnp.cumsum(owned_here.astype(jnp.int32), axis=1) - 1
    picked = owned_here[:, :, None] & (
        rank_among[:, :, None] == jnp.arange(capacity, dtype=jnp.int32)[None, None, :]
    )
    send_slots = jnp.sum(jnp.where(picked, slot_of[:, :, None], 0), axis=1).reshape(
        seq_shards * capacity
    )
    first_seq = seq_index * seq_dev
    my_table = lax.dynamic_slice_in_dim(page_table, first_seq, seq_dev, 0)
    my_lengths = lax.dynamic_slice_in_dim(cached_len, first_seq, seq_dev, 0)
    my_flags = lax.dynamic_slice_in_dim(is_prefill, first_seq, seq_dev, 0)
    flat_table = my_table.reshape(entries)
    my_holder = jnp.where(flat_table >= 0, flat_table // pages_dev, -1)
    entry_order = jnp.arange(entries, dtype=jnp.int32)
    earlier = (my_holder[:, None] == my_holder[None, :]) & (
        entry_order[None, :] < entry_order[:, None]
    )
    my_rank = jnp.sum(earlier.astype(jnp.int32), axis=1)
    row_ids = jnp.arange(row_count, dtype=jnp.int32)
    live_rows = (my_flags[:, None] == 1) | (row_ids[None, :] == 0)
    causal = row_ids[None, :] <= row_ids[:, None]
    part_width = kv_width // sub_count
    split_pages = kv_pages.reshape(pages_dev, 2, PAGE, sub_count, part_width)
    chosen = jnp.take(split_pages, send_slots, axis=0).reshape(
        seq_shards, capacity, 2, PAGE, sub_count, part_width
    )
    outgoing = jnp.moveaxis(chosen, 4, 1).reshape(owners, capacity, 2, PAGE, part_width)
    received = lax.all_to_all(
        outgoing, ("seq", "sub"), split_axis=0, concat_axis=0, tiled=True
    ).reshape(owners * capacity, 2, PAGE, part_width)
    present = flat_table >= 0
    fetch_index = jnp.where(present, my_holder * capacity + my_rank, 0)
    query_part = query_width // sub_count
    my_queries = lax.dynamic_slice_in_dim(queries, core_index * query_part, query_part, 2)
    my_fresh = lax.dynamic_slice_in_dim(new_kv, core_index * part_width, part_width, 3)
    peak, weight_sum, numerator = attend_all(
        my_queries,
        my_fresh,
        received,
        fetch_index.reshape(seq_dev, page_count),
        present.reshape(seq_dev, page_count),
        my_lengths,
        live_rows,
        causal,
        core_index >= 0,
    )
    own_heads = finish(weight_sum, numerator, live_rows)
    return lax.all_gather(own_heads, "sub", axis=2, tiled=True)


MESH = pl.DeviceIdType.MESH
SCALE = HD ** (-0.5)
LOG2E = 1.4426950408889634
DEC_MAXP = 4
LANES = 256
LAG = 3
ROWS16 = 16


def hi(a, b):
    return max(a, b) if isinstance(a, int) and isinstance(b, int) else jnp.maximum(a, b)


def lo(a, b):
    return min(a, b) if isinstance(a, int) and isinstance(b, int) else jnp.minimum(a, b)


def output_bases(m, total):
    n = len(m)
    bases, before, base = [], 0, 0
    for z in range(n):
        both = lo(before, total - m[z])
        base = hi(hi(base, m[z]), both + 1 + LAG * (max(z, n - 1 - z) - z))
        bases.append(base)
        before = m[z]
    return bases


def link_lengths(n, seq_dev, slots, parts):
    total = slots * parts
    lengths = [0] * (n - 1)
    for counts in itertools.product(range(seq_dev + 1), repeat=n):
        if sum(counts) != slots or max(counts) != seq_dev:
            continue
        m = [parts * c for c in itertools.accumulate(counts)]
        bases = output_bases(m, total)
        for z in range(n - 1):
            lengths[z] = max(lengths[z], m[z], bases[z] + total - m[z] if m[z] < total else 0)
    return lengths


def pick(values, z):
    found = 0
    for j, value in enumerate(values):
        found = found + jnp.where(z == j, value, 0)
    return found


def merge(o1, e1, o2, e2):
    top = jnp.maximum(e1, e2)
    w1, w2 = jnp.exp(e1 - top), jnp.exp(e2 - top)
    total = w1 + w2
    inv = 1.0 / total
    return o1 * (w1 * inv) + o2 * (w2 * inv), top + jnp.log(total)


def attend(query, blocks):
    scored = []
    for keys, _, mask in blocks:
        s = lax.dot_general(keys, query, (((1,), (0,)), ((), ())), preferred_element_type=jnp.float32)
        scored.append(jnp.where(mask, s, NEG_FILL))
    peak = functools.reduce(jnp.maximum, [jnp.max(s, axis=0, keepdims=True) for s in scored])
    peak = jnp.maximum(peak, 0.1 * NEG_FILL)
    acc, total = None, None
    for s, (_, values, _) in zip(scored, blocks):
        weights = jnp.exp2((s - peak) * (SCALE * LOG2E))
        part = jnp.sum(weights, axis=0, keepdims=True)
        prod = lax.dot_general(
            values, weights.astype(jnp.bfloat16), (((0,), (0,)), ((), ())), preferred_element_type=jnp.float32
        )
        acc = prod if acc is None else acc + prod
        total = part if total is None else total + part
    empty = total == 0.0
    total = jnp.where(empty, 1.0, total)
    return acc * (1.0 / total), jnp.where(empty, NEG_FILL, peak * SCALE + jnp.log(total))


def fused_kernel(
    n, lengths, heads, group_size, rows, seq_dev, pages_dev,
    table, cached, flags, q_hbm, fresh, kv_hbm, out_hbm,
    kv, q_vm, own_t, out_vm, dec_rows, dec_own, dec_all, dec_o, dec_e, dec_fin,
    a_o, a_e, b_o, b_e, c_o, c_e, d_o, d_e, la_o, la_e, lc_o, lc_e, po, pe,
    dqa, dqb, dqc, dqd, doa, dea, dob, deb, doc, dec, dod, ded,
    slot_seq, rest_seq, slot_of,
    q_sem, kv_sem, kvs_sem, kvr_sem, out_sem, outs_sem, outr_sem,
    bs, br, bes, ber, ds, dr, des, der, xs, xr,
):
    z, core = lax.axis_index("seq"), lax.axis_index("sub")
    other = 1 - core
    has_left, has_right = z > 0, z < n - 1
    seqs, page_count = table.shape
    owners = 2 * n
    each = page_count // owners
    slots = seqs // 2
    rests = seqs - slots
    width = q_vm.shape[2]
    groups_part = LANES // rows
    parts_head = group_size // groups_part
    parts = heads * parts_head
    total = slots * parts
    first_seq = z * seq_dev
    dec_lanes = group_size * seqs

    q_copy = pltpu.make_async_copy(q_hbm.at[:, :, pl.ds(pl.multiple_of(core * width, width), width)], q_vm, q_sem)
    q_copy.start()

    def kv_cols(side, k):
        return kv_hbm.at[:, :, :, pl.ds(pl.multiple_of((side * heads + k) * HD, HD), HD)]

    kv_own = [pltpu.make_async_copy(kv_cols(core, k), kv.at[0, k], kv_sem.at[k]) for k in range(heads)]
    for x in kv_own:
        x.start()
    kv_far = [
        pltpu.make_async_remote_copy(
            src_ref=kv_cols(other, k), dst_ref=kv.at[1, k], send_sem=kvs_sem.at[k], recv_sem=kvr_sem.at[k],
            device_id={"sub": other}, device_id_type=MESH,
        )
        for k in range(heads)
    ]

    barrier = pltpu.get_barrier_semaphore()

    @pl.when(has_left)
    def _():
        pl.semaphore_signal(barrier, inc=1, device_id={"seq": z - 1}, device_id_type=MESH)

    @pl.when(has_right)
    def _():
        pl.semaphore_signal(barrier, inc=1, device_id={"seq": z + 1}, device_id_type=MESH)

    pl.semaphore_signal(barrier, inc=1, device_id={"sub": other}, device_id_type=MESH)

    count, cum, homes = 0, [], []
    for j in range(seqs):
        count = count + flags[j]
        cum.append(count)
        slot_of[j] = jnp.clip(count - 1, 0, slots - 1)
        if j % seq_dev == seq_dev - 1:
            homes.append(count * parts)
    for i in range(slots):
        slot_seq[i] = jnp.minimum(sum((c <= i).astype(jnp.int32) for c in cum), seqs - 1)
    for i in range(rests):
        rest_seq[i] = jnp.minimum(
            sum((j + 1 - c <= i).astype(jnp.int32) for j, c in enumerate(cum)), seqs - 1
        )
    base_r = output_bases(homes, total)
    mirrored = [total - homes[n - 2 - j] for j in range(n - 1)] + [total]
    base_l = output_bases(mirrored, total)[::-1]
    m_left, m_right = pick([0] + homes[:-1], z), pick(homes, z)
    far_left, far_right = m_left, total - m_right
    both = jnp.minimum(far_left, far_right)
    out_base_r, in_base_r = pick(base_r, z), pick([0] + base_r[:-1], z)
    out_base_l, in_base_l = pick(base_l, z), pick(base_l[1:] + [0], z)
    in_r, out_r = pick([0] + lengths, z), pick(lengths + [0], z)
    in_l, out_l = pick(lengths[::-1] + [0], z), pick([0] + lengths[::-1], z)
    top = max(lengths) - 1
    reach = LAG * jnp.maximum(z, n - 1 - z)
    dec_at = LAG * (n - 1) + rests

    def when_right(k):
        return jnp.clip(jnp.where(k < both, 2 * k, k + both), 0, total - 1)

    def when_left(k):
        return jnp.clip(jnp.where(k < both, 2 * k + 1, k + both), 0, total - 1)

    def when_own(i):
        return jnp.clip(i + far_right, 0, total - 1)

    def send(src, dst, s, r, to):
        return pltpu.make_async_remote_copy(
            src_ref=src, dst_ref=dst, send_sem=s, recv_sem=r, device_id={"seq": to}, device_id_type=MESH
        )

    def right(p):
        return (
            send(b_o.at[p], a_o.at[p], bs.at[p], br.at[p], z + 1),
            send(b_e.at[p], a_e.at[p], bes.at[p], ber.at[p], z + 1),
        )

    def left(p):
        return (
            send(d_o.at[p], c_o.at[p], ds.at[p], dr.at[p], z - 1),
            send(d_e.at[p], c_e.at[p], des.at[p], der.at[p], z - 1),
        )

    def right_dq():
        return send(dqb, dqa, xs.at[0], xr.at[0], z + 1)

    def left_dq():
        return send(dqd, dqc, xs.at[1], xr.at[1], z - 1)

    def right_do():
        return (send(dob, doa, xs.at[2], xr.at[2], z + 1), send(deb, dea, xs.at[3], xr.at[3], z + 1))

    def left_do():
        return (send(dod, doc, xs.at[4], xr.at[4], z - 1), send(ded, dec, xs.at[5], xr.at[5], z - 1))

    q_copy.wait()
    dec_rows[...] = jnp.zeros_like(dec_rows)
    for j in range(seq_dev):
        dec_rows[pl.ds(first_seq + j, 1), :] = q_vm[j, 0:ROWS16, :].astype(jnp.float32)[0:1]
    for k in range(heads):
        stacked = jnp.concatenate(
            [dec_rows[:, (k * group_size + g) * HD : (k * group_size + g + 1) * HD] for g in range(group_size)],
            axis=0,
        )
        dec_own[:, k * dec_lanes : (k + 1) * dec_lanes] = stacked.T.astype(jnp.bfloat16)

    def turn(j, carry):
        for c in range(parts):
            stacked = jnp.concatenate(
                [q_vm[j, :, (c * groups_part + g) * HD : (c * groups_part + g + 1) * HD] for g in range(groups_part)],
                axis=0,
            )
            own_t[j * parts + c] = stacked.astype(jnp.float32).T.astype(jnp.bfloat16)
        return carry

    lax.fori_loop(0, seq_dev, turn, 0)
    dec_o[...] = jnp.zeros_like(dec_o)
    dec_e[...] = jnp.full_like(dec_e, NEG_FILL)

    pl.semaphore_wait(barrier, has_left.astype(jnp.int32) + has_right.astype(jnp.int32) + 1)
    for x in kv_far:
        x.start()

    key_id = lax.broadcasted_iota(jnp.int32, (PAGE, 1), 0)
    fresh_id = lax.broadcasted_iota(jnp.int32, (rows, LANES), 0)
    lane_row = lax.broadcasted_iota(jnp.int32, (rows, LANES), 1) % rows
    causal = fresh_id <= lane_row
    dec_lane = lax.broadcasted_iota(jnp.int32, (1, heads * dec_lanes), 1) % seqs
    dec_home = dec_lane // seq_dev
    dec_seq = lax.broadcasted_iota(jnp.int32, (1, dec_lanes), 1) % seqs
    dec_fresh = lax.broadcasted_iota(jnp.int32, (ROWS16, 1), 0)

    def own_query(slot, c):
        local = jnp.clip(slot_seq[slot] - first_seq, 0, seq_dev - 1)
        return own_t[local * parts + c]

    def pages_of(seq, k, few):
        found = []
        start = table[seq, 0] // pages_dev
        for side, owner in enumerate((2 * z + core, 2 * z + other)):
            place = lax.rem(owner - start + owners, owners)
            for j in range(few):
                at = place + owners * j
                valid = jnp.clip(cached[seq] - PAGE * at, 0, PAGE)
                slot = jnp.where(valid > 0, table[seq, jnp.minimum(at, page_count - 1)] - owner * pages_dev, 0)
                slot = jnp.clip(slot, 0, pages_dev - 1)
                found.append((kv[side, k, slot, 0], kv[side, k, slot, 1], key_id < valid))
        return found

    def join(o1, e1, o2, e2, present):
        o2 = jnp.where(present, o2.astype(jnp.float32), 0.0)
        return merge(o1, e1, o2, jnp.where(present, e2, NEG_FILL))

    def assemble_right(p):
        k = jnp.clip(p - out_base_r, 0, total - 1)
        at = jnp.clip(k + in_base_r, 0, top)
        t = when_left(k)
        o, e = join(po[t], pe[t], la_o[at], la_e[at], has_left)
        q = jnp.minimum(p, total - 1)
        query = jnp.where(p < m_left, la_o[p], own_query(q // parts, q % parts))
        b_o[p] = jnp.where(p < m_right, query, o.astype(jnp.bfloat16))
        b_e[p] = e

    def assemble_left(p):
        k = jnp.clip(p - out_base_l, 0, total - 1)
        at = jnp.clip(k + in_base_l, 0, top)
        t = when_right(k)
        o, e = join(po[t], pe[t], lc_o[at], lc_e[at], has_right)
        q = jnp.minimum(p, total - 1)
        query = jnp.where(p < far_right, lc_o[p], own_query(slots - 1 - q // parts, q % parts))
        d_o[p] = jnp.where(p < total - m_left, query, o.astype(jnp.bfloat16))
        d_e[p] = e

    def compute(t):
        nearer = t - both
        apart = far_left + far_right
        paired = t < 2 * both
        is_own = t >= apart
        from_left = jnp.where(paired, t % 2 == 0, far_left > far_right)
        index = jnp.where(paired, t // 2, nearer)
        own_index = jnp.clip(t - far_right, 0, total - 1)
        index = jnp.clip(jnp.where(is_own, own_index, index), 0, total - 1)
        slot = jnp.where(is_own | from_left, index // parts, slots - 1 - index // parts)
        c = index % parts
        seq = slot_seq[slot]
        k = c // parts_head
        at = jnp.minimum(index, top)
        query = jnp.where(from_left, la_o[at], lc_o[at])
        query = jnp.where(is_own, own_query(slot, c), query)
        blocks = pages_of(seq, k, each)
        local = jnp.clip(seq - first_seq, 0, seq_dev - 1)
        head = core * heads + k
        blocks.append((fresh[local, 0, head], fresh[local, 1, head], causal & is_own))
        o, e = attend(query, blocks)
        po[t] = o
        pe[t] = e

    few = min(each, -(-DEC_MAXP // owners))

    def compute_decode(d):
        seq = rest_seq[d]
        local = jnp.clip(seq - first_seq, 0, seq_dev - 1)
        mine = dec_seq == seq
        at_home = (seq // seq_dev == z).astype(jnp.int32)
        for k in range(heads):
            cols = slice(k * dec_lanes, (k + 1) * dec_lanes)
            blocks = pages_of(seq, k, few)
            head = core * heads + k
            blocks.append(
                (fresh[local, 0, head][:ROWS16], fresh[local, 1, head][:ROWS16], dec_fresh < at_home)
            )
            o, e = attend(dec_all[:, cols], blocks)
            dec_o[:, cols] = jnp.where(mine, o, dec_o[:, cols])
            dec_e[:, cols] = jnp.where(mine, e, dec_e[:, cols])

    def step(s, carry):
        p = s - LAG * z
        w = s - LAG * (n - 1 - z)
        t = s - reach

        @pl.when(has_left & (p == 0))
        def _():
            right_dq().wait_recv()

        @pl.when(has_right & (p == 0))
        def _():
            dqb[...] = jnp.where(dec_home == z, dec_own[...], dqa[...])
            right_dq().start()

        @pl.when(has_right & (w == 0))
        def _():
            left_dq().wait_recv()

        @pl.when(has_left & (w == 0))
        def _():
            dqd[...] = jnp.where(dec_home == z, dec_own[...], dqc[...])
            left_dq().start()

        @pl.when((p >= 0) & (p < in_r))
        def _():
            for x in right(p):
                x.wait_recv()
            la_o[p] = a_o[p]
            la_e[p] = a_e[p]

        @pl.when((p >= 0) & (p < out_r))
        def _():
            assemble_right(p)
            for x in right(p):
                x.start()

        @pl.when((w >= 0) & (w < in_l))
        def _():
            for x in left(w):
                x.wait_recv()
            lc_o[w] = c_o[w]
            lc_e[w] = c_e[w]

        @pl.when((w >= 0) & (w < out_l))
        def _():
            assemble_left(w)
            for x in left(w):
                x.start()

        @pl.when(has_left & (p == dec_at))
        def _():
            for x in right_do():
                x.wait_recv()

        @pl.when(has_right & (p == dec_at))
        def _():
            o, e = join(dec_o[...], dec_e[...], doa[...], dea[...], has_left)
            dob[...] = o.astype(jnp.bfloat16)
            deb[...] = e
            for x in right_do():
                x.start()

        @pl.when(has_right & (w == dec_at))
        def _():
            for x in left_do():
                x.wait_recv()

        @pl.when(has_left & (w == dec_at))
        def _():
            o, e = join(dec_o[...], dec_e[...], doc[...], dec[...], has_right)
            dod[...] = o.astype(jnp.bfloat16)
            ded[...] = e
            for x in left_do():
                x.start()

        @pl.when(t == 0)
        def _():
            for x in kv_own:
                x.wait()
            for x in kv_far:
                x.wait_recv()
            dec_all[...] = jnp.where(dec_home < z, dqa[...], jnp.where(dec_home == z, dec_own[...], dqc[...]))

        @pl.when((t >= 0) & (t < total))
        def _():
            compute(t)

        @pl.when((t >= 0) & (t < rests))
        def _():
            compute_decode(t)

        return carry

    ends = [lengths[j] + LAG * (j + 1) for j in range(n - 1)] + [total + LAG * (n - 1)]
    ends.append(dec_at + 1 + LAG * (n - 1))
    lax.fori_loop(0, max(ends), step, 0)

    o, e = join(dec_o[...], dec_e[...], doa[...], dea[...], has_left)
    o, e = join(o, e, doc[...], dec[...], has_right)
    dec_fin[...] = o.T
    top_row = lax.broadcasted_iota(jnp.int32, (rows, 1), 0) == 0

    def out_copies(j):
        cols = pl.ds(pl.multiple_of(core * width, width), width)
        return (
            pltpu.make_async_copy(out_vm.at[j], out_hbm.at[j, :, cols], out_sem.at[j]),
            pltpu.make_async_remote_copy(
                src_ref=out_vm.at[j], dst_ref=out_hbm.at[j, :, cols], send_sem=outs_sem.at[j],
                recv_sem=outr_sem.at[j], device_id={"sub": other}, device_id_type=MESH,
            ),
        )

    def came_copies(j):
        cols = pl.ds(pl.multiple_of(other * width, width), width)
        return pltpu.make_async_remote_copy(
            src_ref=out_vm.at[j], dst_ref=out_hbm.at[j, :, cols], send_sem=outs_sem.at[j],
            recv_sem=outr_sem.at[j], device_id={"sub": other}, device_id_type=MESH,
        )

    def finish(j, carry):
        seq = first_seq + j
        chosen = flags[seq] == 1
        slot = slot_of[seq]
        for c in range(parts):
            i = slot * parts + c
            k = (slots - 1 - slot) * parts + c
            t = when_own(i)
            at_a = jnp.clip(k + in_base_r, 0, top)
            at_c = jnp.clip(i + in_base_l, 0, top)
            o, e = join(po[t], pe[t], la_o[at_a], la_e[at_a], has_left)
            o, e = join(o, e, lc_o[at_c], lc_e[at_c], has_right)
            turned = o.T
            for g in range(groups_part):
                h = c * groups_part + g
                line_at = (h // group_size) * dec_lanes + (h % group_size) * seqs + seq
                line = jnp.where(top_row, dec_fin[pl.ds(line_at, 1), :], 0.0)
                tile = jnp.where(chosen, turned[g * rows : (g + 1) * rows], line)
                out_vm[j, :, h * HD : (h + 1) * HD] = tile.astype(out_vm.dtype)
        for x in out_copies(j):
            x.start()
        return carry

    lax.fori_loop(0, seq_dev, finish, 0)

    def drain_right(p, carry):
        for x in right(p):
            x.wait_send()
        return carry

    def drain_left(p, carry):
        for x in left(p):
            x.wait_send()
        return carry

    for x in kv_far:
        x.wait_send()

    lax.fori_loop(0, out_r, drain_right, 0)
    lax.fori_loop(0, out_l, drain_left, 0)

    @pl.when(has_right)
    def _():
        right_dq().wait_send()
        for x in right_do():
            x.wait_send()

    @pl.when(has_left)
    def _():
        left_dq().wait_send()
        for x in left_do():
            x.wait_send()

    def drain_out(j, carry):
        mine, sent = out_copies(j)
        mine.wait()
        sent.wait_send()
        came_copies(j).wait_recv()
        return carry

    lax.fori_loop(0, seq_dev, drain_out, 0)


def fused_attention(queries, new_kv, kv_pages, page_table, cached_len, is_prefill):
    n = lax.axis_size("seq")
    sub_count = lax.axis_size("sub")
    seq_dev, rows, query_width = queries.shape
    pages_dev, kv_width = kv_pages.shape[0], kv_pages.shape[3]
    seqs = page_table.shape[0]
    slots = seqs // 2
    group_size = query_width // kv_width
    heads_all = kv_width // HD
    heads = heads_all // sub_count
    width = query_width // sub_count
    parts = heads * group_size * rows // LANES
    lengths = link_lengths(n, seq_dev, slots, parts)
    count, total = max(lengths), slots * parts
    fresh = jnp.transpose(new_kv.reshape(seq_dev, rows, 2, heads_all, HD), (0, 2, 3, 1, 4))
    bf, f32 = jnp.bfloat16, jnp.float32
    dec = heads * group_size * seqs

    def data(c, lanes=LANES):
        return pltpu.VMEM((c, HD, lanes), bf)

    def stat(c, lanes=LANES):
        return pltpu.VMEM((c, 1, lanes), f32)

    dma = pltpu.SemaphoreType.DMA
    scratch = [
        pltpu.VMEM((2, heads, pages_dev, 2, PAGE, HD), bf),
        pltpu.VMEM((seq_dev, rows, width), bf),
        data(seq_dev * parts),
        pltpu.VMEM((seq_dev, rows, width), bf),
        pltpu.VMEM((seqs, width), f32),
        pltpu.VMEM((HD, dec), bf),
        pltpu.VMEM((HD, dec), bf),
        pltpu.VMEM((HD, dec), f32),
        pltpu.VMEM((1, dec), f32),
        pltpu.VMEM((dec, HD), f32),
    ]
    scratch += [data(count), stat(count)] * 6
    scratch += [pltpu.VMEM((total, HD, LANES), f32), stat(total)]
    scratch += [pltpu.VMEM((HD, dec), bf)] * 4
    scratch += [pltpu.VMEM((HD, dec), bf), pltpu.VMEM((1, dec), f32)] * 4
    scratch += [pltpu.SMEM((slots,), jnp.int32), pltpu.SMEM((seqs - slots,), jnp.int32)]
    scratch += [pltpu.SMEM((seqs,), jnp.int32)]
    scratch += [dma, dma((heads,)), dma((heads,)), dma((heads,))] + [dma((seq_dev,))] * 3
    scratch += [dma((count,))] * 8 + [dma((6,))] * 2
    smem = pl.BlockSpec(memory_space=pltpu.SMEM)
    return pl.pallas_call(
        functools.partial(fused_kernel, n, lengths, heads, group_size, rows, seq_dev, pages_dev),
        out_shape=jax.ShapeDtypeStruct(queries.shape, queries.dtype),
        in_specs=[smem] * 3
        + [
            pl.BlockSpec(memory_space=pl.ANY),
            pl.BlockSpec(memory_space=pltpu.VMEM),
            pl.BlockSpec(memory_space=pl.ANY),
        ],
        out_specs=pl.BlockSpec(memory_space=pl.ANY),
        scratch_shapes=scratch,
        compiler_params=pltpu.CompilerParams(
            collective_id=0, has_side_effects=True, vmem_limit_bytes=60 * 1024 * 1024
        ),
        name="paged_attention",
    )(page_table, cached_len, is_prefill, queries, fresh, kv_pages)


def per_device(queries, new_kv, kv_pages, page_table, cached_len, is_prefill):
    owners = lax.axis_size("seq") * lax.axis_size("sub")
    if page_table.shape[1] >= owners:
        return fused_attention(queries, new_kv, kv_pages, page_table, cached_len, is_prefill)
    return exchange_pages(queries, new_kv, kv_pages, page_table, cached_len, is_prefill)


def solution(mesh):
    placed = (
        P(("groups", "seq"), None, "head"),
        P(("groups", "seq"), None, None, "head"),
        P(("groups", "seq", "sub"), None, None, "head"),
        P("groups", None),
        P("groups"),
        P("groups"),
    )
    return jax.shard_map(
        per_device,
        mesh=mesh,
        in_specs=placed,
        out_specs=P(("groups", "seq"), None, "head"),
        check_vma=False,
    )
```

```python
import functools
import itertools

import jax
import jax.numpy as jnp
from jax import lax
from jax.experimental import pallas as pl
from jax.experimental.pallas import tpu as pltpu
from jax.sharding import PartitionSpec as P

HD = 128
PAGE = 128


NEG_FILL = -1e30


def partial_softmax(
    query_heads, cache_keys, cache_values, cache_valid, fresh_keys, fresh_values, fresh_valid
):
    score_scale = HD ** (-0.5)
    cache_scores = (
        jnp.einsum("rkgd,nkd->kgrn", query_heads, cache_keys, preferred_element_type=jnp.float32)
        * score_scale
    )
    fresh_scores = (
        jnp.einsum("rkgd,jkd->kgrj", query_heads, fresh_keys, preferred_element_type=jnp.float32)
        * score_scale
    )
    cache_mask = cache_valid[None, None, None, :]
    fresh_mask = fresh_valid[None, None, :, :]
    peak = jnp.maximum(
        jnp.max(jnp.where(cache_mask, cache_scores, NEG_FILL), axis=-1),
        jnp.max(jnp.where(fresh_mask, fresh_scores, NEG_FILL), axis=-1),
    )
    cache_weights = jnp.where(cache_mask, jnp.exp(cache_scores - peak[..., None]), 0.0)
    fresh_weights = jnp.where(fresh_mask, jnp.exp(fresh_scores - peak[..., None]), 0.0)
    weight_sum = jnp.sum(cache_weights, axis=-1) + jnp.sum(fresh_weights, axis=-1)
    numerator = jnp.einsum(
        "kgrn,nkd->kgrd",
        cache_weights.astype(jnp.bfloat16),
        cache_values,
        preferred_element_type=jnp.float32,
    )
    numerator = numerator + jnp.einsum(
        "kgrj,jkd->kgrd",
        fresh_weights.astype(jnp.bfloat16),
        fresh_values,
        preferred_element_type=jnp.float32,
    )
    return (peak, weight_sum, numerator)


def attend_all(
    query_block, fresh_block, received, fetch_index, page_here, lengths, live_rows, causal, fresh_on
):
    kv_width = received.shape[-1]
    heads_kv = kv_width // HD
    row_count = query_block.shape[1]
    group_size = query_block.shape[2] // kv_width
    page_count = fetch_index.shape[1]
    positions = jnp.arange(page_count * PAGE, dtype=jnp.int32)

    def one_sequence(inputs):
        query_rows, fresh_rows, index_row, here_row, length, live_row = inputs
        fetched = jnp.take(received, index_row, axis=0)
        cache_keys = fetched[:, 0].reshape(page_count * PAGE, heads_kv, HD)
        cache_values = fetched[:, 1].reshape(page_count * PAGE, heads_kv, HD)
        page_mask = jnp.broadcast_to(here_row[:, None], (page_count, PAGE)).reshape(
            page_count * PAGE
        )
        cache_valid = page_mask & (positions < length)
        query_heads = query_rows.reshape(row_count, heads_kv, group_size, HD)
        fresh_keys = fresh_rows[:, 0].reshape(row_count, heads_kv, HD)
        fresh_values = fresh_rows[:, 1].reshape(row_count, heads_kv, HD)
        fresh_valid = causal & live_row[:, None] & fresh_on
        return partial_softmax(
            query_heads,
            cache_keys,
            cache_values,
            cache_valid,
            fresh_keys,
            fresh_values,
            fresh_valid,
        )

    return lax.map(
        one_sequence, (query_block, fresh_block, fetch_index, page_here, lengths, live_rows)
    )


def finish(weight_sum, numerator, live_rows):
    unused_rows = 1.0 - live_rows.astype(jnp.float32)
    attended = numerator / (weight_sum + unused_rows[:, None, None, :])[..., None]
    attended = jnp.where(live_rows[:, None, None, :, None], attended, 0.0)
    seq_dev, heads_kv, group_size, row_count, head_dim = attended.shape
    return (
        jnp.transpose(attended, (0, 3, 1, 2, 4))
        .reshape(seq_dev, row_count, heads_kv * group_size * head_dim)
        .astype(jnp.bfloat16)
    )


def exchange_pages(queries, new_kv, kv_pages, page_table, cached_len, is_prefill):
    seq_shards = lax.axis_size("seq")
    sub_count = lax.axis_size("sub")
    owners = seq_shards * sub_count
    seq_index = lax.axis_index("seq")
    core_index = lax.axis_index("sub")
    owner_self = seq_index * sub_count + core_index
    seq_dev, row_count, query_width = queries.shape
    pages_dev = kv_pages.shape[0]
    kv_width = kv_pages.shape[3]
    page_count = page_table.shape[1]
    entries = seq_dev * page_count
    capacity = (entries + owners - 1) // owners
    table_rows = page_table.reshape(seq_shards, entries)
    holder = jnp.where(table_rows >= 0, table_rows // pages_dev, -1)
    slot_of = jnp.where(table_rows >= 0, table_rows % pages_dev, 0)
    owned_here = holder == owner_self
    rank_among = jnp.cumsum(owned_here.astype(jnp.int32), axis=1) - 1
    picked = owned_here[:, :, None] & (
        rank_among[:, :, None] == jnp.arange(capacity, dtype=jnp.int32)[None, None, :]
    )
    send_slots = jnp.sum(jnp.where(picked, slot_of[:, :, None], 0), axis=1).reshape(
        seq_shards * capacity
    )
    first_seq = seq_index * seq_dev
    my_table = lax.dynamic_slice_in_dim(page_table, first_seq, seq_dev, 0)
    my_lengths = lax.dynamic_slice_in_dim(cached_len, first_seq, seq_dev, 0)
    my_flags = lax.dynamic_slice_in_dim(is_prefill, first_seq, seq_dev, 0)
    flat_table = my_table.reshape(entries)
    my_holder = jnp.where(flat_table >= 0, flat_table // pages_dev, -1)
    entry_order = jnp.arange(entries, dtype=jnp.int32)
    earlier = (my_holder[:, None] == my_holder[None, :]) & (
        entry_order[None, :] < entry_order[:, None]
    )
    my_rank = jnp.sum(earlier.astype(jnp.int32), axis=1)
    row_ids = jnp.arange(row_count, dtype=jnp.int32)
    live_rows = (my_flags[:, None] == 1) | (row_ids[None, :] == 0)
    causal = row_ids[None, :] <= row_ids[:, None]
    part_width = kv_width // sub_count
    split_pages = kv_pages.reshape(pages_dev, 2, PAGE, sub_count, part_width)
    chosen = jnp.take(split_pages, send_slots, axis=0).reshape(
        seq_shards, capacity, 2, PAGE, sub_count, part_width
    )
    outgoing = jnp.moveaxis(chosen, 4, 1).reshape(owners, capacity, 2, PAGE, part_width)
    received = lax.all_to_all(
        outgoing, ("seq", "sub"), split_axis=0, concat_axis=0, tiled=True
    ).reshape(owners * capacity, 2, PAGE, part_width)
    present = flat_table >= 0
    fetch_index = jnp.where(present, my_holder * capacity + my_rank, 0)
    query_part = query_width // sub_count
    my_queries = lax.dynamic_slice_in_dim(queries, core_index * query_part, query_part, 2)
    my_fresh = lax.dynamic_slice_in_dim(new_kv, core_index * part_width, part_width, 3)
    peak, weight_sum, numerator = attend_all(
        my_queries,
        my_fresh,
        received,
        fetch_index.reshape(seq_dev, page_count),
        present.reshape(seq_dev, page_count),
        my_lengths,
        live_rows,
        causal,
        core_index >= 0,
    )
    own_heads = finish(weight_sum, numerator, live_rows)
    return lax.all_gather(own_heads, "sub", axis=2, tiled=True)


MESH = pl.DeviceIdType.MESH
SCALE = HD ** (-0.5)
LOG2E = 1.4426950408889634
DEC_MAXP = 4
LANES = 256
LAG = 3
ROWS16 = 16


def hi(a, b):
    return max(a, b) if isinstance(a, int) and isinstance(b, int) else jnp.maximum(a, b)


def lo(a, b):
    return min(a, b) if isinstance(a, int) and isinstance(b, int) else jnp.minimum(a, b)


def output_bases(m, total):
    n = len(m)
    bases, before, base = [], 0, 0
    for z in range(n):
        both = lo(before, total - m[z])
        base = hi(hi(base, m[z]), both + 1 + LAG * (max(z, n - 1 - z) - z))
        bases.append(base)
        before = m[z]
    return bases


def link_lengths(n, seq_dev, slots, parts):
    total = slots * parts
    lengths = [0] * (n - 1)
    for counts in itertools.product(range(seq_dev + 1), repeat=n):
        if sum(counts) != slots or max(counts) != seq_dev:
            continue
        m = [parts * c for c in itertools.accumulate(counts)]
        bases = output_bases(m, total)
        for z in range(n - 1):
            lengths[z] = max(lengths[z], m[z], bases[z] + total - m[z] if m[z] < total else 0)
    return lengths


def pick(values, z):
    found = 0
    for j, value in enumerate(values):
        found = found + jnp.where(z == j, value, 0)
    return found


def merge(o1, e1, o2, e2):
    top = jnp.maximum(e1, e2)
    w1, w2 = jnp.exp(e1 - top), jnp.exp(e2 - top)
    total = w1 + w2
    inv = 1.0 / total
    return o1 * (w1 * inv) + o2 * (w2 * inv), top + jnp.log(total)


def attend(query, blocks):
    scored = []
    for keys, _, mask in blocks:
        s = lax.dot_general(keys, query, (((1,), (0,)), ((), ())), preferred_element_type=jnp.float32)
        scored.append(jnp.where(mask, s, NEG_FILL))
    peak = functools.reduce(jnp.maximum, [jnp.max(s, axis=0, keepdims=True) for s in scored])
    peak = jnp.maximum(peak, 0.1 * NEG_FILL)
    acc, total = None, None
    for s, (_, values, _) in zip(scored, blocks):
        weights = jnp.exp2((s - peak) * (SCALE * LOG2E))
        part = jnp.sum(weights, axis=0, keepdims=True)
        prod = lax.dot_general(
            values, weights.astype(jnp.bfloat16), (((0,), (0,)), ((), ())), preferred_element_type=jnp.float32
        )
        acc = prod if acc is None else acc + prod
        total = part if total is None else total + part
    empty = total == 0.0
    total = jnp.where(empty, 1.0, total)
    return acc * (1.0 / total), jnp.where(empty, NEG_FILL, peak * SCALE + jnp.log(total))


def fused_kernel(
    n, lengths, heads, group_size, rows, seq_dev, pages_dev,
    table_hbm, cached_hbm, flags_hbm, q_hbm, new_hbm, kv_hbm, out,
    table, cached, flags, new_kv,
    kv, q_vm, own_t, fresh, dec_rows, dec_own, dec_all, dec_o, dec_e, dec_fin,
    a_o, a_e, b_o, b_e, c_o, c_e, d_o, d_e, la_o, la_e, lc_o, lc_e, po, pe,
    dqa, dqb, dqc, dqd, doa, dea, dob, deb, doc, dec, dod, ded,
    slot_seq, rest_seq, slot_of, rest_of,
    in_sem, q_sem, kv_sem, kvs_sem, kvr_sem, outs_sem, outr_sem,
    bs, br, bes, ber, ds, dr, des, der, xs, xr,
):
    z, core = lax.axis_index("seq"), lax.axis_index("sub")
    other = 1 - core
    has_left, has_right = z > 0, z < n - 1
    seqs, page_count = table.shape
    owners = 2 * n
    each = page_count // owners
    slots = seqs // 2
    rests = seqs - slots
    width = q_vm.shape[2]
    groups_part = LANES // rows
    parts_head = group_size // groups_part
    parts = heads * parts_head
    total = slots * parts
    first_seq = z * seq_dev
    head_lanes = group_size * rests
    dec_lanes = heads * head_lanes

    small = [
        pltpu.make_async_copy(src, dst, in_sem.at[i])
        for i, (src, dst) in enumerate(
            ((table_hbm, table), (cached_hbm, cached), (flags_hbm, flags), (new_hbm, new_kv))
        )
    ]
    for x in small:
        x.start()
    q_copy = pltpu.make_async_copy(q_hbm.at[:, :, pl.ds(pl.multiple_of(core * width, width), width)], q_vm, q_sem)
    q_copy.start()

    def kv_cols(side, k):
        return kv_hbm.at[:, :, :, pl.ds(pl.multiple_of((side * heads + k) * HD, HD), HD)]

    kv_own = [pltpu.make_async_copy(kv_cols(core, k), kv.at[0, k], kv_sem.at[k]) for k in range(heads)]
    for x in kv_own:
        x.start()
    kv_far = [
        pltpu.make_async_remote_copy(
            src_ref=kv_cols(other, k), dst_ref=kv.at[1, k], send_sem=kvs_sem.at[k], recv_sem=kvr_sem.at[k],
            device_id={"sub": other}, device_id_type=MESH,
        )
        for k in range(heads)
    ]

    barrier = pltpu.get_barrier_semaphore()

    @pl.when(has_left)
    def _():
        pl.semaphore_signal(barrier, inc=1, device_id={"seq": z - 1}, device_id_type=MESH)

    @pl.when(has_right)
    def _():
        pl.semaphore_signal(barrier, inc=1, device_id={"seq": z + 1}, device_id_type=MESH)

    pl.semaphore_signal(barrier, inc=1, device_id={"sub": other}, device_id_type=MESH)

    for x in small[:3]:
        x.wait()
    count, cum, homes = 0, [], []
    for j in range(seqs):
        count = count + flags[j]
        cum.append(count)
        slot_of[j] = jnp.clip(count - 1, 0, slots - 1)
        rest_of[j] = jnp.clip(j - count, 0, rests - 1)
        if j % seq_dev == seq_dev - 1:
            homes.append(count * parts)
    for i in range(slots):
        slot_seq[i] = jnp.minimum(sum((c <= i).astype(jnp.int32) for c in cum), seqs - 1)
    for i in range(rests):
        rest_seq[i] = jnp.minimum(
            sum((j + 1 - c <= i).astype(jnp.int32) for j, c in enumerate(cum)), seqs - 1
        )
    base_r = output_bases(homes, total)
    mirrored = [total - homes[n - 2 - j] for j in range(n - 1)] + [total]
    base_l = output_bases(mirrored, total)[::-1]
    m_left, m_right = pick([0] + homes[:-1], z), pick(homes, z)
    far_left, far_right = m_left, total - m_right
    both = jnp.minimum(far_left, far_right)
    out_base_r, in_base_r = pick(base_r, z), pick([0] + base_r[:-1], z)
    out_base_l, in_base_l = pick(base_l, z), pick(base_l[1:] + [0], z)
    in_r, out_r = pick([0] + lengths, z), pick(lengths + [0], z)
    in_l, out_l = pick(lengths[::-1] + [0], z), pick([0] + lengths[::-1], z)
    top = max(lengths) - 1
    reach = LAG * jnp.maximum(z, n - 1 - z)
    dec_at = LAG * (n - 1) + rests

    def when_right(k):
        return jnp.clip(jnp.where(k < both, 2 * k, k + both), 0, total - 1)

    def when_left(k):
        return jnp.clip(jnp.where(k < both, 2 * k + 1, k + both), 0, total - 1)

    def when_own(i):
        return jnp.clip(i + far_right, 0, total - 1)

    def send(src, dst, s, r, to):
        return pltpu.make_async_remote_copy(
            src_ref=src, dst_ref=dst, send_sem=s, recv_sem=r, device_id={"seq": to}, device_id_type=MESH
        )

    def right(p):
        return (
            send(b_o.at[p], a_o.at[p], bs.at[p], br.at[p], z + 1),
            send(b_e.at[p], a_e.at[p], bes.at[p], ber.at[p], z + 1),
        )

    def left(p):
        return (
            send(d_o.at[p], c_o.at[p], ds.at[p], dr.at[p], z - 1),
            send(d_e.at[p], c_e.at[p], des.at[p], der.at[p], z - 1),
        )

    def right_dq():
        return send(dqb, dqa, xs.at[0], xr.at[0], z + 1)

    def left_dq():
        return send(dqd, dqc, xs.at[1], xr.at[1], z - 1)

    def right_do():
        return (send(dob, doa, xs.at[2], xr.at[2], z + 1), send(deb, dea, xs.at[3], xr.at[3], z + 1))

    def left_do():
        return (send(dod, doc, xs.at[4], xr.at[4], z - 1), send(ded, dec, xs.at[5], xr.at[5], z - 1))

    dec_lane = lax.broadcasted_iota(jnp.int32, (1, dec_lanes), 1)
    dec_of = dec_lane % rests
    dec_head = dec_lane // head_lanes
    dec_home = jnp.zeros((1, dec_lanes), jnp.int32)
    q_copy.wait()
    for d in range(rests):
        home = rest_seq[d] // seq_dev
        local = jnp.clip(rest_seq[d] - first_seq, 0, seq_dev - 1)
        dec_rows[d : d + 1, :] = q_vm[local, 0:ROWS16, :].astype(jnp.float32)[0:1]
        dec_home = jnp.where(dec_of == d, home, dec_home)
    stacked = jnp.concatenate(
        [dec_rows[:, h * HD : (h + 1) * HD] for h in range(heads * group_size)], axis=0
    )
    dec_own[...] = stacked.T.astype(jnp.bfloat16)

    def turn(j, carry):
        for c in range(parts):
            stacked = jnp.concatenate(
                [q_vm[j, :, (c * groups_part + g) * HD : (c * groups_part + g + 1) * HD] for g in range(groups_part)],
                axis=0,
            )
            own_t[j * parts + c] = stacked.astype(jnp.float32).T.astype(jnp.bfloat16)
        return carry

    lax.fori_loop(0, seq_dev, turn, 0)
    small[3].wait()
    for j in range(seq_dev):
        for t in range(2):
            for h in range(2 * heads):
                fresh[j, t, h] = new_kv[j, :, t, h * HD : (h + 1) * HD]
    dec_o[...] = jnp.zeros_like(dec_o)
    dec_e[...] = jnp.full_like(dec_e, NEG_FILL)

    pl.semaphore_wait(barrier, has_left.astype(jnp.int32) + has_right.astype(jnp.int32) + 1)
    for x in kv_far:
        x.start()

    key_id = lax.broadcasted_iota(jnp.int32, (PAGE, 1), 0)
    fresh_id = lax.broadcasted_iota(jnp.int32, (rows, LANES), 0)
    lane_row = lax.broadcasted_iota(jnp.int32, (rows, LANES), 1) % rows
    causal = fresh_id <= lane_row
    dec_fresh = lax.broadcasted_iota(jnp.int32, (ROWS16, 1), 0)

    def own_query(slot, c):
        local = jnp.clip(slot_seq[slot] - first_seq, 0, seq_dev - 1)
        return own_t[local * parts + c]

    def pages_of(seq, k, few):
        found = []
        start = table[seq, 0] // pages_dev
        for side, owner in enumerate((2 * z + core, 2 * z + other)):
            place = lax.rem(owner - start + owners, owners)
            for j in range(few):
                at = place + owners * j
                valid = jnp.clip(cached[seq] - PAGE * at, 0, PAGE)
                slot = jnp.where(valid > 0, table[seq, jnp.minimum(at, page_count - 1)] - owner * pages_dev, 0)
                slot = jnp.clip(slot, 0, pages_dev - 1)
                found.append((kv[side, k, slot, 0], kv[side, k, slot, 1], key_id < valid))
        return found

    def join(o1, e1, o2, e2, present):
        o2 = jnp.where(present, o2.astype(jnp.float32), 0.0)
        return merge(o1, e1, o2, jnp.where(present, e2, NEG_FILL))

    def assemble_right(p):
        k = jnp.clip(p - out_base_r, 0, total - 1)
        at = jnp.clip(k + in_base_r, 0, top)
        t = when_left(k)
        o, e = join(po[t], pe[t], la_o[at], la_e[at], has_left)
        q = jnp.minimum(p, total - 1)
        query = jnp.where(p < m_left, la_o[p], own_query(q // parts, q % parts))
        b_o[p] = jnp.where(p < m_right, query, o.astype(jnp.bfloat16))
        b_e[p] = e

    def assemble_left(p):
        k = jnp.clip(p - out_base_l, 0, total - 1)
        at = jnp.clip(k + in_base_l, 0, top)
        t = when_right(k)
        o, e = join(po[t], pe[t], lc_o[at], lc_e[at], has_right)
        q = jnp.minimum(p, total - 1)
        query = jnp.where(p < far_right, lc_o[p], own_query(slots - 1 - q // parts, q % parts))
        d_o[p] = jnp.where(p < total - m_left, query, o.astype(jnp.bfloat16))
        d_e[p] = e

    def compute(t):
        nearer = t - both
        apart = far_left + far_right
        paired = t < 2 * both
        is_own = t >= apart
        from_left = jnp.where(paired, t % 2 == 0, far_left > far_right)
        index = jnp.where(paired, t // 2, nearer)
        own_index = jnp.clip(t - far_right, 0, total - 1)
        index = jnp.clip(jnp.where(is_own, own_index, index), 0, total - 1)
        slot = jnp.where(is_own | from_left, index // parts, slots - 1 - index // parts)
        c = index % parts
        seq = slot_seq[slot]
        k = c // parts_head
        at = jnp.minimum(index, top)
        query = jnp.where(from_left, la_o[at], lc_o[at])
        query = jnp.where(is_own, own_query(slot, c), query)
        blocks = pages_of(seq, k, each)
        local = jnp.clip(seq - first_seq, 0, seq_dev - 1)
        head = core * heads + k
        blocks.append((fresh[local, 0, head], fresh[local, 1, head], causal & is_own))
        o, e = attend(query, blocks)
        po[t] = o
        pe[t] = e

    few = min(each, -(-DEC_MAXP // owners))

    def compute_decode(d):
        seq = rest_seq[d]
        local = jnp.clip(seq - first_seq, 0, seq_dev - 1)
        at_home = (seq // seq_dev == z).astype(jnp.int32)
        for k in range(heads):
            mine = (dec_of == d) & (dec_head == k)
            blocks = pages_of(seq, k, few)
            head = core * heads + k
            blocks.append(
                (fresh[local, 0, head][:ROWS16], fresh[local, 1, head][:ROWS16], dec_fresh < at_home)
            )
            o, e = attend(dec_all[...], blocks)
            dec_o[...] = jnp.where(mine, o, dec_o[...])
            dec_e[...] = jnp.where(mine, e, dec_e[...])

    def step(s, carry):
        p = s - LAG * z
        w = s - LAG * (n - 1 - z)
        t = s - reach

        @pl.when(has_left & (p == 0))
        def _():
            right_dq().wait_recv()

        @pl.when(has_right & (p == 0))
        def _():
            dqb[...] = jnp.where(dec_home == z, dec_own[...], dqa[...])
            right_dq().start()

        @pl.when(has_right & (w == 0))
        def _():
            left_dq().wait_recv()

        @pl.when(has_left & (w == 0))
        def _():
            dqd[...] = jnp.where(dec_home == z, dec_own[...], dqc[...])
            left_dq().start()

        @pl.when((p >= 0) & (p < in_r))
        def _():
            for x in right(p):
                x.wait_recv()
            la_o[p] = a_o[p]
            la_e[p] = a_e[p]

        @pl.when((p >= 0) & (p < out_r))
        def _():
            assemble_right(p)
            for x in right(p):
                x.start()

        @pl.when((w >= 0) & (w < in_l))
        def _():
            for x in left(w):
                x.wait_recv()
            lc_o[w] = c_o[w]
            lc_e[w] = c_e[w]

        @pl.when((w >= 0) & (w < out_l))
        def _():
            assemble_left(w)
            for x in left(w):
                x.start()

        @pl.when(has_left & (p == dec_at))
        def _():
            for x in right_do():
                x.wait_recv()

        @pl.when(has_right & (p == dec_at))
        def _():
            o, e = join(dec_o[...], dec_e[...], doa[...], dea[...], has_left)
            dob[...] = o.astype(jnp.bfloat16)
            deb[...] = e
            for x in right_do():
                x.start()

        @pl.when(has_right & (w == dec_at))
        def _():
            for x in left_do():
                x.wait_recv()

        @pl.when(has_left & (w == dec_at))
        def _():
            o, e = join(dec_o[...], dec_e[...], doc[...], dec[...], has_right)
            dod[...] = o.astype(jnp.bfloat16)
            ded[...] = e
            for x in left_do():
                x.start()

        @pl.when(t == 0)
        def _():
            for x in kv_own:
                x.wait()
            for x in kv_far:
                x.wait_recv()
            dec_all[...] = jnp.where(dec_home < z, dqa[...], jnp.where(dec_home == z, dec_own[...], dqc[...]))

        @pl.when((t >= 0) & (t < total))
        def _():
            compute(t)

        @pl.when((t >= 0) & (t < rests))
        def _():
            compute_decode(t)

        return carry

    ends = [lengths[j] + LAG * (j + 1) for j in range(n - 1)] + [total + LAG * (n - 1)]
    ends.append(dec_at + 1 + LAG * (n - 1))
    lax.fori_loop(0, max(ends), step, 0)

    o, e = join(dec_o[...], dec_e[...], doa[...], dea[...], has_left)
    o, e = join(o, e, doc[...], dec[...], has_right)
    dec_fin[...] = o.T
    top_row = lax.broadcasted_iota(jnp.int32, (rows, 1), 0) == 0

    def share(j, side):
        part = out.at[j, :, pl.ds(pl.multiple_of(side * width, width), width)]
        return pltpu.make_async_remote_copy(
            src_ref=part, dst_ref=part, send_sem=outs_sem.at[j], recv_sem=outr_sem.at[j],
            device_id={"sub": other}, device_id_type=MESH,
        )

    def finish(j, carry):
        seq = first_seq + j
        chosen = flags[seq] == 1
        slot = slot_of[seq]
        for c in range(parts):
            i = slot * parts + c
            k = (slots - 1 - slot) * parts + c
            t = when_own(i)
            at_a = jnp.clip(k + in_base_r, 0, top)
            at_c = jnp.clip(i + in_base_l, 0, top)
            o, e = join(po[t], pe[t], la_o[at_a], la_e[at_a], has_left)
            o, e = join(o, e, lc_o[at_c], lc_e[at_c], has_right)
            turned = o.T
            for g in range(groups_part):
                h = c * groups_part + g
                line_at = h * rests + rest_of[seq]
                line = jnp.where(top_row, dec_fin[pl.ds(line_at, 1), :], 0.0)
                tile = jnp.where(chosen, turned[g * rows : (g + 1) * rows], line)
                place = pl.multiple_of(core * width + h * HD, HD)
                out[j, :, pl.ds(place, HD)] = tile.astype(out.dtype)
        share(j, core).start()
        return carry

    lax.fori_loop(0, seq_dev, finish, 0)

    def drain_right(p, carry):
        for x in right(p):
            x.wait_send()
        return carry

    def drain_left(p, carry):
        for x in left(p):
            x.wait_send()
        return carry

    for x in kv_far:
        x.wait_send()

    lax.fori_loop(0, out_r, drain_right, 0)
    lax.fori_loop(0, out_l, drain_left, 0)

    @pl.when(has_right)
    def _():
        right_dq().wait_send()
        for x in right_do():
            x.wait_send()

    @pl.when(has_left)
    def _():
        left_dq().wait_send()
        for x in left_do():
            x.wait_send()

    def drain_out(j, carry):
        share(j, core).wait_send()
        share(j, other).wait_recv()
        return carry

    lax.fori_loop(0, seq_dev, drain_out, 0)


def fused_attention(queries, new_kv, kv_pages, page_table, cached_len, is_prefill):
    n = lax.axis_size("seq")
    sub_count = lax.axis_size("sub")
    seq_dev, rows, query_width = queries.shape
    pages_dev, kv_width = kv_pages.shape[0], kv_pages.shape[3]
    seqs = page_table.shape[0]
    slots = seqs // 2
    group_size = query_width // kv_width
    heads_all = kv_width // HD
    heads = heads_all // sub_count
    width = query_width // sub_count
    parts = heads * group_size * rows // LANES
    lengths = link_lengths(n, seq_dev, slots, parts)
    count, total = max(lengths), slots * parts
    bf, f32 = jnp.bfloat16, jnp.float32
    dec = heads * group_size * (seqs - slots)

    def data(c, lanes=LANES):
        return pltpu.VMEM((c, HD, lanes), bf)

    def stat(c, lanes=LANES):
        return pltpu.VMEM((c, 1, lanes), f32)

    dma = pltpu.SemaphoreType.DMA
    scratch = [
        pltpu.SMEM(page_table.shape, jnp.int32),
        pltpu.SMEM(cached_len.shape, jnp.int32),
        pltpu.SMEM(is_prefill.shape, jnp.int32),
        pltpu.VMEM(new_kv.shape, bf),
        pltpu.VMEM((2, heads, pages_dev, 2, PAGE, HD), bf),
        pltpu.VMEM((seq_dev, rows, width), bf),
        data(seq_dev * parts),
        pltpu.VMEM((seq_dev, 2, heads_all, rows, HD), bf),
        pltpu.VMEM((seqs - slots, width), f32),
        pltpu.VMEM((HD, dec), bf),
        pltpu.VMEM((HD, dec), bf),
        pltpu.VMEM((HD, dec), f32),
        pltpu.VMEM((1, dec), f32),
        pltpu.VMEM((dec, HD), f32),
    ]
    scratch += [data(count), stat(count)] * 6
    scratch += [pltpu.VMEM((total, HD, LANES), f32), stat(total)]
    scratch += [pltpu.VMEM((HD, dec), bf)] * 4
    scratch += [pltpu.VMEM((HD, dec), bf), pltpu.VMEM((1, dec), f32)] * 4
    scratch += [pltpu.SMEM((slots,), jnp.int32), pltpu.SMEM((seqs - slots,), jnp.int32)]
    scratch += [pltpu.SMEM((seqs,), jnp.int32)] * 2
    scratch += [dma((4,)), dma, dma((heads,)), dma((heads,)), dma((heads,))] + [dma((seq_dev,))] * 2
    scratch += [dma((count,))] * 8 + [dma((6,))] * 2
    operands = (page_table, cached_len, is_prefill, queries, new_kv, kv_pages)
    return pl.pallas_call(
        functools.partial(fused_kernel, n, lengths, heads, group_size, rows, seq_dev, pages_dev),
        out_shape=jax.ShapeDtypeStruct(queries.shape, queries.dtype),
        in_specs=[pl.BlockSpec(memory_space=pltpu.HBM)] * 6,
        out_specs=pl.BlockSpec(memory_space=pltpu.VMEM),
        scratch_shapes=scratch,
        compiler_params=pltpu.CompilerParams(
            collective_id=0, has_side_effects=True, vmem_limit_bytes=48 * 1024 * 1024
        ),
        name="paged_attention",
    )(*[pltpu.with_memory_space_constraint(x, pltpu.HBM) for x in operands])


def per_device(queries, new_kv, kv_pages, page_table, cached_len, is_prefill):
    owners = lax.axis_size("seq") * lax.axis_size("sub")
    if page_table.shape[1] >= owners:
        return fused_attention(queries, new_kv, kv_pages, page_table, cached_len, is_prefill)
    return exchange_pages(queries, new_kv, kv_pages, page_table, cached_len, is_prefill)


def solution(mesh):
    placed = (
        P(("groups", "seq"), None, "head"),
        P(("groups", "seq"), None, None, "head"),
        P(("groups", "seq", "sub"), None, None, "head"),
        P("groups", None),
        P("groups"),
        P("groups"),
    )
    return jax.shard_map(
        per_device,
        mesh=mesh,
        in_specs=placed,
        out_specs=P(("groups", "seq"), None, "head"),
        check_vma=False,
    )
```

```python
import functools
import itertools

import jax
import jax.numpy as jnp
from jax import lax
from jax.experimental import pallas as pl
from jax.experimental.pallas import tpu as pltpu
from jax.sharding import PartitionSpec as P

HD = 128
PAGE = 128


NEG_FILL = -1e30


def partial_softmax(
    query_heads, cache_keys, cache_values, cache_valid, fresh_keys, fresh_values, fresh_valid
):
    score_scale = HD ** (-0.5)
    cache_scores = (
        jnp.einsum("rkgd,nkd->kgrn", query_heads, cache_keys, preferred_element_type=jnp.float32)
        * score_scale
    )
    fresh_scores = (
        jnp.einsum("rkgd,jkd->kgrj", query_heads, fresh_keys, preferred_element_type=jnp.float32)
        * score_scale
    )
    cache_mask = cache_valid[None, None, None, :]
    fresh_mask = fresh_valid[None, None, :, :]
    peak = jnp.maximum(
        jnp.max(jnp.where(cache_mask, cache_scores, NEG_FILL), axis=-1),
        jnp.max(jnp.where(fresh_mask, fresh_scores, NEG_FILL), axis=-1),
    )
    cache_weights = jnp.where(cache_mask, jnp.exp(cache_scores - peak[..., None]), 0.0)
    fresh_weights = jnp.where(fresh_mask, jnp.exp(fresh_scores - peak[..., None]), 0.0)
    weight_sum = jnp.sum(cache_weights, axis=-1) + jnp.sum(fresh_weights, axis=-1)
    numerator = jnp.einsum(
        "kgrn,nkd->kgrd",
        cache_weights.astype(jnp.bfloat16),
        cache_values,
        preferred_element_type=jnp.float32,
    )
    numerator = numerator + jnp.einsum(
        "kgrj,jkd->kgrd",
        fresh_weights.astype(jnp.bfloat16),
        fresh_values,
        preferred_element_type=jnp.float32,
    )
    return (peak, weight_sum, numerator)


def attend_all(
    query_block, fresh_block, received, fetch_index, page_here, lengths, live_rows, causal, fresh_on
):
    kv_width = received.shape[-1]
    heads_kv = kv_width // HD
    row_count = query_block.shape[1]
    group_size = query_block.shape[2] // kv_width
    page_count = fetch_index.shape[1]
    positions = jnp.arange(page_count * PAGE, dtype=jnp.int32)

    def one_sequence(inputs):
        query_rows, fresh_rows, index_row, here_row, length, live_row = inputs
        fetched = jnp.take(received, index_row, axis=0)
        cache_keys = fetched[:, 0].reshape(page_count * PAGE, heads_kv, HD)
        cache_values = fetched[:, 1].reshape(page_count * PAGE, heads_kv, HD)
        page_mask = jnp.broadcast_to(here_row[:, None], (page_count, PAGE)).reshape(
            page_count * PAGE
        )
        cache_valid = page_mask & (positions < length)
        query_heads = query_rows.reshape(row_count, heads_kv, group_size, HD)
        fresh_keys = fresh_rows[:, 0].reshape(row_count, heads_kv, HD)
        fresh_values = fresh_rows[:, 1].reshape(row_count, heads_kv, HD)
        fresh_valid = causal & live_row[:, None] & fresh_on
        return partial_softmax(
            query_heads,
            cache_keys,
            cache_values,
            cache_valid,
            fresh_keys,
            fresh_values,
            fresh_valid,
        )

    return lax.map(
        one_sequence, (query_block, fresh_block, fetch_index, page_here, lengths, live_rows)
    )


def finish(weight_sum, numerator, live_rows):
    unused_rows = 1.0 - live_rows.astype(jnp.float32)
    attended = numerator / (weight_sum + unused_rows[:, None, None, :])[..., None]
    attended = jnp.where(live_rows[:, None, None, :, None], attended, 0.0)
    seq_dev, heads_kv, group_size, row_count, head_dim = attended.shape
    return (
        jnp.transpose(attended, (0, 3, 1, 2, 4))
        .reshape(seq_dev, row_count, heads_kv * group_size * head_dim)
        .astype(jnp.bfloat16)
    )


def exchange_pages(queries, new_kv, kv_pages, page_table, cached_len, is_prefill):
    seq_shards = lax.axis_size("seq")
    sub_count = lax.axis_size("sub")
    owners = seq_shards * sub_count
    seq_index = lax.axis_index("seq")
    core_index = lax.axis_index("sub")
    owner_self = seq_index * sub_count + core_index
    seq_dev, row_count, query_width = queries.shape
    pages_dev = kv_pages.shape[0]
    kv_width = kv_pages.shape[3]
    page_count = page_table.shape[1]
    entries = seq_dev * page_count
    capacity = (entries + owners - 1) // owners
    table_rows = page_table.reshape(seq_shards, entries)
    holder = jnp.where(table_rows >= 0, table_rows // pages_dev, -1)
    slot_of = jnp.where(table_rows >= 0, table_rows % pages_dev, 0)
    owned_here = holder == owner_self
    rank_among = jnp.cumsum(owned_here.astype(jnp.int32), axis=1) - 1
    picked = owned_here[:, :, None] & (
        rank_among[:, :, None] == jnp.arange(capacity, dtype=jnp.int32)[None, None, :]
    )
    send_slots = jnp.sum(jnp.where(picked, slot_of[:, :, None], 0), axis=1).reshape(
        seq_shards * capacity
    )
    first_seq = seq_index * seq_dev
    my_table = lax.dynamic_slice_in_dim(page_table, first_seq, seq_dev, 0)
    my_lengths = lax.dynamic_slice_in_dim(cached_len, first_seq, seq_dev, 0)
    my_flags = lax.dynamic_slice_in_dim(is_prefill, first_seq, seq_dev, 0)
    flat_table = my_table.reshape(entries)
    my_holder = jnp.where(flat_table >= 0, flat_table // pages_dev, -1)
    entry_order = jnp.arange(entries, dtype=jnp.int32)
    earlier = (my_holder[:, None] == my_holder[None, :]) & (
        entry_order[None, :] < entry_order[:, None]
    )
    my_rank = jnp.sum(earlier.astype(jnp.int32), axis=1)
    row_ids = jnp.arange(row_count, dtype=jnp.int32)
    live_rows = (my_flags[:, None] == 1) | (row_ids[None, :] == 0)
    causal = row_ids[None, :] <= row_ids[:, None]
    part_width = kv_width // sub_count
    split_pages = kv_pages.reshape(pages_dev, 2, PAGE, sub_count, part_width)
    chosen = jnp.take(split_pages, send_slots, axis=0).reshape(
        seq_shards, capacity, 2, PAGE, sub_count, part_width
    )
    outgoing = jnp.moveaxis(chosen, 4, 1).reshape(owners, capacity, 2, PAGE, part_width)
    received = lax.all_to_all(
        outgoing, ("seq", "sub"), split_axis=0, concat_axis=0, tiled=True
    ).reshape(owners * capacity, 2, PAGE, part_width)
    present = flat_table >= 0
    fetch_index = jnp.where(present, my_holder * capacity + my_rank, 0)
    query_part = query_width // sub_count
    my_queries = lax.dynamic_slice_in_dim(queries, core_index * query_part, query_part, 2)
    my_fresh = lax.dynamic_slice_in_dim(new_kv, core_index * part_width, part_width, 3)
    peak, weight_sum, numerator = attend_all(
        my_queries,
        my_fresh,
        received,
        fetch_index.reshape(seq_dev, page_count),
        present.reshape(seq_dev, page_count),
        my_lengths,
        live_rows,
        causal,
        core_index >= 0,
    )
    own_heads = finish(weight_sum, numerator, live_rows)
    return lax.all_gather(own_heads, "sub", axis=2, tiled=True)


MESH = pl.DeviceIdType.MESH
SCALE = HD ** (-0.5)
LOG2E = 1.4426950408889634
DEC_MAXP = 4
LANES = 256
LAG = 3
FIRST = 1
ROWS16 = 16


def hi(a, b):
    return max(a, b) if isinstance(a, int) and isinstance(b, int) else jnp.maximum(a, b)


def lo(a, b):
    return min(a, b) if isinstance(a, int) and isinstance(b, int) else jnp.minimum(a, b)


def sel(c, a, b):
    return (a if c else b) if isinstance(c, bool) else jnp.where(c, a, b)


def query_spans(own):
    spans, leads, span, lead = [], [], 0, 0
    for count in own:
        lead = sel(count > 0, 0, LAG + lead)
        span = sel(span == 0, count, LAG + span + hi(count - LAG, 0))
        spans.append(span)
        leads.append(lead)
    return spans, leads


def stream_plan(own):
    n = len(own)
    spans, _ = query_spans(own)
    back, back_leads = query_spans(own[::-1])
    bases, base = [], 0
    for z in range(n - 1):
        ahead, behind = (spans[z - 1] if z else 0), back[n - 2 - z]
        clear = hi(spans[z] - back_leads[n - 2 - z], lo(ahead, behind) + LAG + FIRST)
        base = hi(base, clear)
        bases.append(base)
        base = base + 2 * LAG
    return spans, bases


def stream_lengths(n, seq_dev, slots, parts):
    lengths, work = [0] * (n - 1), 0
    for counts in itertools.product(range(seq_dev + 1), repeat=n):
        if sum(counts) != slots or max(counts) != seq_dev:
            continue
        own = [parts * c for c in counts]
        spans, bases = stream_plan(own)
        back = query_spans(own[::-1])[0]
        for z in range(n):
            ahead, behind = (spans[z - 1] if z else 0), (back[n - 2 - z] if z < n - 1 else 0)
            work = max(work, ahead + behind + own[z])
            if z < n - 1:
                lengths[z] = max(lengths[z], spans[z], bases[z] + behind if behind else 0)
    return lengths, work


def pick(values, z):
    found = 0
    for j, value in enumerate(values):
        found = found + jnp.where(z == j, value, 0)
    return found


def merge(o1, e1, o2, e2):
    top = jnp.maximum(e1, e2)
    w1, w2 = jnp.exp(e1 - top), jnp.exp(e2 - top)
    total = w1 + w2
    inv = 1.0 / total
    return o1 * (w1 * inv) + o2 * (w2 * inv), top + jnp.log(total)


def attend(query, blocks):
    scored = []
    for keys, _, mask in blocks:
        s = lax.dot_general(keys, query, (((1,), (0,)), ((), ())), preferred_element_type=jnp.float32)
        scored.append(jnp.where(mask, s, NEG_FILL))
    peak = functools.reduce(jnp.maximum, [jnp.max(s, axis=0, keepdims=True) for s in scored])
    peak = jnp.maximum(peak, 0.1 * NEG_FILL)
    acc, total = None, None
    for s, (_, values, _) in zip(scored, blocks):
        weights = jnp.exp2((s - peak) * (SCALE * LOG2E))
        part = jnp.sum(weights, axis=0, keepdims=True)
        prod = lax.dot_general(
            values, weights.astype(jnp.bfloat16), (((0,), (0,)), ((), ())), preferred_element_type=jnp.float32
        )
        acc = prod if acc is None else acc + prod
        total = part if total is None else total + part
    empty = total == 0.0
    total = jnp.where(empty, 1.0, total)
    return acc * (1.0 / total), jnp.where(empty, NEG_FILL, peak * SCALE + jnp.log(total))


def fused_kernel(
    n, lengths, work, heads, group_size, rows, seq_dev, pages_dev,
    table_hbm, cached_hbm, flags_hbm, q_hbm, new_hbm, kv_hbm, out,
    table, cached, flags, new_kv,
    kv, q_vm, own_t, fresh, dec_rows, dec_own, dec_all, dec_o, dec_e, dec_fin,
    a_o, a_e, b_o, b_e, c_o, c_e, d_o, d_e, la_o, la_e, lc_o, lc_e, po, pe,
    dqa, dqb, dqc, dqd, doa, dea, dob, deb, doc, dec, dod, ded,
    slot_seq, rest_seq, slot_of, rest_of, own_tab, start_tab, in_tab,
    in_sem, q_sem, kv_sem, kvs_sem, kvr_sem, outs_sem, outr_sem,
    bs, br, bes, ber, ds, dr, des, der, xs, xr,
):
    z, core = lax.axis_index("seq"), lax.axis_index("sub")
    other = 1 - core
    has_left, has_right = z > 0, z < n - 1
    seqs, page_count = table.shape
    owners = 2 * n
    each = page_count // owners
    slots = seqs // 2
    rests = seqs - slots
    width = q_vm.shape[2]
    groups_part = LANES // rows
    parts_head = group_size // groups_part
    parts = heads * parts_head
    first_seq = z * seq_dev
    head_lanes = group_size * rests
    dec_lanes = heads * head_lanes

    barrier = pltpu.get_barrier_semaphore()

    @pl.when(has_left)
    def _():
        pl.semaphore_signal(barrier, inc=1, device_id={"seq": z - 1}, device_id_type=MESH)

    @pl.when(has_right)
    def _():
        pl.semaphore_signal(barrier, inc=1, device_id={"seq": z + 1}, device_id_type=MESH)

    pl.semaphore_signal(barrier, inc=1, device_id={"sub": other}, device_id_type=MESH)

    small = [
        pltpu.make_async_copy(src, dst, in_sem.at[i])
        for i, (src, dst) in enumerate(
            ((table_hbm, table), (cached_hbm, cached), (flags_hbm, flags), (new_hbm, new_kv))
        )
    ]
    for x in small:
        x.start()
    q_copy = pltpu.make_async_copy(q_hbm.at[:, :, pl.ds(pl.multiple_of(core * width, width), width)], q_vm, q_sem)
    q_copy.start()

    def kv_cols(side, k):
        return kv_hbm.at[:, :, :, pl.ds(pl.multiple_of((side * heads + k) * HD, HD), HD)]

    kv_own = [pltpu.make_async_copy(kv_cols(core, k), kv.at[0, k], kv_sem.at[k]) for k in range(heads)]
    for x in kv_own:
        x.start()
    kv_far = [
        pltpu.make_async_remote_copy(
            src_ref=kv_cols(other, k), dst_ref=kv.at[1, k], send_sem=kvs_sem.at[k], recv_sem=kvr_sem.at[k],
            device_id={"sub": other}, device_id_type=MESH,
        )
        for k in range(heads)
    ]

    for x in small[:3]:
        x.wait()
    count, cum, own, before = 0, [], [], 0
    for j in range(seqs):
        count = count + flags[j]
        cum.append(count)
        slot_of[j] = jnp.clip(count - 1, 0, slots - 1)
        rest_of[j] = jnp.clip(j - count, 0, rests - 1)
        if j % seq_dev == seq_dev - 1:
            start_tab[j // seq_dev] = before
            own.append((count - before) * parts)
            own_tab[j // seq_dev] = own[-1]
            before = count
    for i in range(slots):
        slot_seq[i] = jnp.minimum(sum((c <= i).astype(jnp.int32) for c in cum), seqs - 1)
    for i in range(rests):
        rest_seq[i] = jnp.minimum(
            sum((j + 1 - c <= i).astype(jnp.int32) for j, c in enumerate(cum)), seqs - 1
        )
    spans_r, base_r = stream_plan(own)
    spans_l, base_l = stream_plan(own[::-1])
    ins_r, ins_l = [0] + spans_r[:-1], spans_l[::-1][1:] + [0]
    for w in range(n):
        in_tab[w] = ins_r[w]
        in_tab[n + w] = ins_l[w]
    query_in_r, query_in_l = pick(ins_r, z), pick(ins_l, z)
    query_out_r, query_out_l = pick(spans_r, z), pick(spans_l[::-1], z)
    both = jnp.minimum(query_in_r, query_in_l)
    foreign = query_in_r + query_in_l
    my_start = start_tab[z]
    out_base_r, in_base_r = pick(base_r + [0], z), pick([0] + base_r, z)
    out_base_l, in_base_l = pick(([0] + base_l[::-1]), z), pick(base_l[::-1] + [0], z)
    in_r, out_r = pick([0] + lengths, z), pick(lengths + [0], z)
    in_l, out_l = pick(lengths[::-1] + [0], z), pick([0] + lengths[::-1], z)
    top = max(lengths) - 1
    reach = LAG * jnp.maximum(z, n - 1 - z)
    dec_at = LAG * (n - 1) + rests

    def when_right(k):
        return jnp.clip(jnp.where(k < both, 2 * k, k + both), 0, work - 1)

    def when_left(k):
        return jnp.clip(jnp.where(k < both, 2 * k + 1, k + both), 0, work - 1)

    def send(src, dst, s, r, to):
        return pltpu.make_async_remote_copy(
            src_ref=src, dst_ref=dst, send_sem=s, recv_sem=r, device_id={"seq": to}, device_id_type=MESH
        )

    def right(p):
        return (
            send(b_o.at[p], a_o.at[p], bs.at[p], br.at[p], z + 1),
            send(b_e.at[p], a_e.at[p], bes.at[p], ber.at[p], z + 1),
        )

    def left(p):
        return (
            send(d_o.at[p], c_o.at[p], ds.at[p], dr.at[p], z - 1),
            send(d_e.at[p], c_e.at[p], des.at[p], der.at[p], z - 1),
        )

    def right_dq():
        return send(dqb, dqa, xs.at[0], xr.at[0], z + 1)

    def left_dq():
        return send(dqd, dqc, xs.at[1], xr.at[1], z - 1)

    def right_do():
        return (send(dob, doa, xs.at[2], xr.at[2], z + 1), send(deb, dea, xs.at[3], xr.at[3], z + 1))

    def left_do():
        return (send(dod, doc, xs.at[4], xr.at[4], z - 1), send(ded, dec, xs.at[5], xr.at[5], z - 1))

    pl.semaphore_wait(barrier, has_left.astype(jnp.int32) + has_right.astype(jnp.int32) + 1)
    for x in kv_far:
        x.start()

    dec_lane = lax.broadcasted_iota(jnp.int32, (1, dec_lanes), 1)
    dec_of = dec_lane % rests
    dec_head = dec_lane // head_lanes
    dec_home = jnp.zeros((1, dec_lanes), jnp.int32)
    q_copy.wait()
    for d in range(rests):
        home = rest_seq[d] // seq_dev
        local = jnp.clip(rest_seq[d] - first_seq, 0, seq_dev - 1)
        dec_rows[d : d + 1, :] = q_vm[local, 0:ROWS16, :].astype(jnp.float32)[0:1]
        dec_home = jnp.where(dec_of == d, home, dec_home)
    stacked = jnp.concatenate(
        [dec_rows[:, h * HD : (h + 1) * HD] for h in range(heads * group_size)], axis=0
    )
    dec_own[...] = stacked.T.astype(jnp.bfloat16)

    def turn(j, carry):
        for c in range(parts):
            stacked = jnp.concatenate(
                [q_vm[j, :, (c * groups_part + g) * HD : (c * groups_part + g + 1) * HD] for g in range(groups_part)],
                axis=0,
            )
            own_t[j * parts + c] = stacked.astype(jnp.float32).T.astype(jnp.bfloat16)
        return carry

    lax.fori_loop(0, seq_dev, turn, 0)
    dec_o[...] = jnp.zeros_like(dec_o)
    dec_e[...] = jnp.full_like(dec_e, NEG_FILL)

    key_id = lax.broadcasted_iota(jnp.int32, (PAGE, 1), 0)
    fresh_id = lax.broadcasted_iota(jnp.int32, (rows, LANES), 0)
    lane_row = lax.broadcasted_iota(jnp.int32, (rows, LANES), 1) % rows
    causal = fresh_id <= lane_row
    dec_fresh = lax.broadcasted_iota(jnp.int32, (ROWS16, 1), 0)

    def own_query(rank):
        rank = jnp.clip(rank, 0, seq_dev * parts - 1)
        slot = jnp.minimum(my_start + rank // parts, slots - 1)
        local = jnp.clip(slot_seq[slot] - first_seq, 0, seq_dev - 1)
        return own_t[local * parts + rank % parts]

    def resolve(q, side):
        w, home, rank, done = z - 1 + 2 * side, 0, 0, False
        for _ in range(n - 1):
            w = jnp.clip(w, 0, n - 1)
            ahead = in_tab[side * n + w]
            direct = (ahead == 0) | (q < jnp.minimum(own_tab[w], LAG))
            hit = direct | (q >= LAG + ahead)
            found = hit & jnp.logical_not(done)
            home = jnp.where(found, w, home)
            rank = jnp.where(found, jnp.where(direct, q, q - ahead), rank)
            done = done | hit
            q = q - LAG
            w = w + 2 * side - 1
        return home, jnp.clip(rank, 0, seq_dev * parts - 1)

    def pages_of(seq, k, few):
        found = []
        start = table[seq, 0] // pages_dev
        for side, owner in enumerate((2 * z + core, 2 * z + other)):
            place = lax.rem(owner - start + owners, owners)
            for j in range(few):
                at = place + owners * j
                valid = jnp.clip(cached[seq] - PAGE * at, 0, PAGE)
                slot = jnp.where(valid > 0, table[seq, jnp.minimum(at, page_count - 1)] - owner * pages_dev, 0)
                slot = jnp.clip(slot, 0, pages_dev - 1)
                found.append((kv[side, k, slot, 0], kv[side, k, slot, 1], key_id < valid))
        return found

    def join(o1, e1, o2, e2, present):
        o2 = jnp.where(present, o2.astype(jnp.float32), 0.0)
        return merge(o1, e1, o2, jnp.where(present, e2, NEG_FILL))

    def assemble_right(p):
        k = jnp.maximum(p - out_base_r, 0)
        at = jnp.clip(k + LAG + in_base_r, 0, top)
        t = when_left(k)
        o, e = join(po[t], pe[t], la_o[at], la_e[at], has_left)
        came = (query_in_r > 0) & (p >= LAG) & (p < LAG + query_in_r)
        mine = own_query(jnp.where((query_in_r == 0) | (p < LAG), p, p - query_in_r))
        query = jnp.where(came, la_o[jnp.clip(p - LAG, 0, top)], mine)
        b_o[p] = jnp.where(p < query_out_r, query, o.astype(jnp.bfloat16))
        b_e[p] = e

    def assemble_left(p):
        k = jnp.maximum(p - out_base_l, 0)
        at = jnp.clip(k + LAG + in_base_l, 0, top)
        t = when_right(k)
        o, e = join(po[t], pe[t], lc_o[at], lc_e[at], has_right)
        came = (query_in_l > 0) & (p >= LAG) & (p < LAG + query_in_l)
        mine = own_query(jnp.where((query_in_l == 0) | (p < LAG), p, p - query_in_l))
        query = jnp.where(came, lc_o[jnp.clip(p - LAG, 0, top)], mine)
        d_o[p] = jnp.where(p < query_out_l, query, o.astype(jnp.bfloat16))
        d_e[p] = e

    def compute(t):
        paired = t < 2 * both
        is_own = t >= foreign
        right_more = query_in_r <= query_in_l
        side = jnp.where(paired, t % 2, right_more.astype(jnp.int32))
        index = jnp.clip(jnp.where(paired, t // 2, t - both), 0, top)
        home, rank = resolve(index, side)
        home = jnp.where(is_own, z, home)
        own_rank = jnp.clip(t - foreign, 0, seq_dev * parts - 1)
        rank = jnp.where(is_own, own_rank, rank)
        seq = slot_seq[jnp.minimum(start_tab[home] + rank // parts, slots - 1)]
        k = (rank % parts) // parts_head
        query = jnp.where(side == 0, la_o[index], lc_o[index])
        query = jnp.where(is_own, own_query(own_rank), query)
        blocks = pages_of(seq, k, each)
        local = jnp.clip(seq - first_seq, 0, seq_dev - 1)
        head = core * heads + k
        blocks.append((fresh[local, 0, head], fresh[local, 1, head], causal & is_own))
        o, e = attend(query, blocks)
        po[t] = o
        pe[t] = e

    few = min(each, -(-DEC_MAXP // owners))

    def compute_decode(d):
        seq = rest_seq[d]
        local = jnp.clip(seq - first_seq, 0, seq_dev - 1)
        at_home = (seq // seq_dev == z).astype(jnp.int32)
        for k in range(heads):
            mine = (dec_of == d) & (dec_head == k)
            blocks = pages_of(seq, k, few)
            head = core * heads + k
            blocks.append(
                (fresh[local, 0, head][:ROWS16], fresh[local, 1, head][:ROWS16], dec_fresh < at_home)
            )
            o, e = attend(dec_all[...], blocks)
            dec_o[...] = jnp.where(mine, o, dec_o[...])
            dec_e[...] = jnp.where(mine, e, dec_e[...])

    def step(s, carry):
        p, w = s - LAG * z, s - LAG * (n - 1 - z)
        t, d, r = s - LAG, s - reach, s - LAG

        @pl.when(has_left & (p == 0))
        def _():
            right_dq().wait_recv()

        @pl.when(has_right & (p == 0))
        def _():
            dqb[...] = jnp.where(dec_home == z, dec_own[...], dqa[...])
            right_dq().start()

        @pl.when(has_right & (w == 0))
        def _():
            left_dq().wait_recv()

        @pl.when(has_left & (w == 0))
        def _():
            dqd[...] = jnp.where(dec_home == z, dec_own[...], dqc[...])
            left_dq().start()

        @pl.when((r >= 0) & (r < in_r))
        def _():
            for x in right(r):
                x.wait_recv()
            la_o[r] = a_o[r]
            la_e[r] = a_e[r]

        @pl.when(s < out_r)
        def _():
            assemble_right(s)
            for x in right(s):
                x.start()

        @pl.when((r >= 0) & (r < in_l))
        def _():
            for x in left(r):
                x.wait_recv()
            lc_o[r] = c_o[r]
            lc_e[r] = c_e[r]

        @pl.when(s < out_l)
        def _():
            assemble_left(s)
            for x in left(s):
                x.start()

        @pl.when(has_left & (p == dec_at))
        def _():
            for x in right_do():
                x.wait_recv()

        @pl.when(has_right & (p == dec_at))
        def _():
            o, e = join(dec_o[...], dec_e[...], doa[...], dea[...], has_left)
            dob[...] = o.astype(jnp.bfloat16)
            deb[...] = e
            for x in right_do():
                x.start()

        @pl.when(has_right & (w == dec_at))
        def _():
            for x in left_do():
                x.wait_recv()

        @pl.when(has_left & (w == dec_at))
        def _():
            o, e = join(dec_o[...], dec_e[...], doc[...], dec[...], has_right)
            dod[...] = o.astype(jnp.bfloat16)
            ded[...] = e
            for x in left_do():
                x.start()

        @pl.when(t == 0)
        def _():
            for x in kv_own:
                x.wait()
            for x in kv_far:
                x.wait_recv()
            small[3].wait()

        @pl.when((t >= 0) & (t < seq_dev))
        def _():
            for i in range(2):
                for h in range(2 * heads):
                    fresh[t, i, h] = new_kv[t, :, i, h * HD : (h + 1) * HD]

        @pl.when((t >= 0) & (t < work))
        def _():
            compute(t)

        @pl.when(d == 0)
        def _():
            dec_all[...] = jnp.where(dec_home < z, dqa[...], jnp.where(dec_home == z, dec_own[...], dqc[...]))

        @pl.when((d >= 0) & (d < rests))
        def _():
            compute_decode(d)

        return carry

    steps = max(max(lengths) + LAG, work + LAG, dec_at + 1 + LAG * (n - 1))
    lax.fori_loop(0, steps, step, 0)

    o, e = join(dec_o[...], dec_e[...], doa[...], dea[...], has_left)
    o, e = join(o, e, doc[...], dec[...], has_right)
    dec_fin[...] = o.T
    top_row = lax.broadcasted_iota(jnp.int32, (rows, 1), 0) == 0

    def share(j, side):
        part = out.at[j, :, pl.ds(pl.multiple_of(side * width, width), width)]
        return pltpu.make_async_remote_copy(
            src_ref=part, dst_ref=part, send_sem=outs_sem.at[j], recv_sem=outr_sem.at[j],
            device_id={"sub": other}, device_id_type=MESH,
        )

    def finish(j, carry):
        seq = first_seq + j
        chosen = flags[seq] == 1
        slot = slot_of[seq]
        for c in range(parts):
            rank = jnp.maximum((slot - my_start) * parts + c, 0)
            t = jnp.minimum(foreign + rank, work - 1)
            to_left = jnp.where((query_in_l == 0) | (rank < LAG), rank, rank + query_in_l)
            to_right = jnp.where((query_in_r == 0) | (rank < LAG), rank, rank + query_in_r)
            at_a = jnp.clip(to_left + in_base_r, 0, top)
            at_c = jnp.clip(to_right + in_base_l, 0, top)
            o, e = join(po[t], pe[t], la_o[at_a], la_e[at_a], has_left)
            o, e = join(o, e, lc_o[at_c], lc_e[at_c], has_right)
            turned = o.T
            for g in range(groups_part):
                h = c * groups_part + g
                line_at = h * rests + rest_of[seq]
                line = jnp.where(top_row, dec_fin[pl.ds(line_at, 1), :], 0.0)
                tile = jnp.where(chosen, turned[g * rows : (g + 1) * rows], line)
                place = pl.multiple_of(core * width + h * HD, HD)
                out[j, :, pl.ds(place, HD)] = tile.astype(out.dtype)
        share(j, core).start()
        return carry

    lax.fori_loop(0, seq_dev, finish, 0)

    def drain_right(p, carry):
        for x in right(p):
            x.wait_send()
        return carry

    def drain_left(p, carry):
        for x in left(p):
            x.wait_send()
        return carry

    for x in kv_far:
        x.wait_send()

    lax.fori_loop(0, out_r, drain_right, 0)
    lax.fori_loop(0, out_l, drain_left, 0)

    @pl.when(has_right)
    def _():
        right_dq().wait_send()
        for x in right_do():
            x.wait_send()

    @pl.when(has_left)
    def _():
        left_dq().wait_send()
        for x in left_do():
            x.wait_send()

    def drain_out(j, carry):
        share(j, core).wait_send()
        share(j, other).wait_recv()
        return carry

    lax.fori_loop(0, seq_dev, drain_out, 0)


def fused_attention(queries, new_kv, kv_pages, page_table, cached_len, is_prefill):
    n = lax.axis_size("seq")
    sub_count = lax.axis_size("sub")
    seq_dev, rows, query_width = queries.shape
    pages_dev, kv_width = kv_pages.shape[0], kv_pages.shape[3]
    seqs = page_table.shape[0]
    slots = seqs // 2
    group_size = query_width // kv_width
    heads_all = kv_width // HD
    heads = heads_all // sub_count
    width = query_width // sub_count
    parts = heads * group_size * rows // LANES
    lengths, work = stream_lengths(n, seq_dev, slots, parts)
    count = max(lengths)
    bf, f32 = jnp.bfloat16, jnp.float32
    dec = heads * group_size * (seqs - slots)

    def data(c, lanes=LANES):
        return pltpu.VMEM((c, HD, lanes), bf)

    def stat(c, lanes=LANES):
        return pltpu.VMEM((c, 1, lanes), f32)

    dma = pltpu.SemaphoreType.DMA
    scratch = [
        pltpu.SMEM(page_table.shape, jnp.int32),
        pltpu.SMEM(cached_len.shape, jnp.int32),
        pltpu.SMEM(is_prefill.shape, jnp.int32),
        pltpu.VMEM(new_kv.shape, bf),
        pltpu.VMEM((2, heads, pages_dev, 2, PAGE, HD), bf),
        pltpu.VMEM((seq_dev, rows, width), bf),
        data(seq_dev * parts),
        pltpu.VMEM((seq_dev, 2, heads_all, rows, HD), bf),
        pltpu.VMEM((seqs - slots, width), f32),
        pltpu.VMEM((HD, dec), bf),
        pltpu.VMEM((HD, dec), bf),
        pltpu.VMEM((HD, dec), f32),
        pltpu.VMEM((1, dec), f32),
        pltpu.VMEM((dec, HD), f32),
    ]
    scratch += [data(count), stat(count)] * 6
    scratch += [pltpu.VMEM((work, HD, LANES), f32), stat(work)]
    scratch += [pltpu.VMEM((HD, dec), bf)] * 4
    scratch += [pltpu.VMEM((HD, dec), bf), pltpu.VMEM((1, dec), f32)] * 4
    scratch += [pltpu.SMEM((slots,), jnp.int32), pltpu.SMEM((seqs - slots,), jnp.int32)]
    scratch += [pltpu.SMEM((seqs,), jnp.int32)] * 2
    scratch += [pltpu.SMEM((n,), jnp.int32)] * 2 + [pltpu.SMEM((2 * n,), jnp.int32)]
    scratch += [dma((4,)), dma, dma((heads,)), dma((heads,)), dma((heads,))] + [dma((seq_dev,))] * 2
    scratch += [dma((count,))] * 8 + [dma((6,))] * 2
    operands = (page_table, cached_len, is_prefill, queries, new_kv, kv_pages)
    return pl.pallas_call(
        functools.partial(fused_kernel, n, lengths, work, heads, group_size, rows, seq_dev, pages_dev),
        out_shape=jax.ShapeDtypeStruct(queries.shape, queries.dtype),
        in_specs=[pl.BlockSpec(memory_space=pltpu.HBM)] * 6,
        out_specs=pl.BlockSpec(memory_space=pltpu.VMEM),
        scratch_shapes=scratch,
        compiler_params=pltpu.CompilerParams(
            collective_id=0, has_side_effects=True, vmem_limit_bytes=48 * 1024 * 1024
        ),
        name="paged_attention",
    )(*[pltpu.with_memory_space_constraint(x, pltpu.HBM) for x in operands])


def per_device(queries, new_kv, kv_pages, page_table, cached_len, is_prefill):
    owners = lax.axis_size("seq") * lax.axis_size("sub")
    if page_table.shape[1] >= owners:
        return fused_attention(queries, new_kv, kv_pages, page_table, cached_len, is_prefill)
    return exchange_pages(queries, new_kv, kv_pages, page_table, cached_len, is_prefill)


def solution(mesh):
    placed = (
        P(("groups", "seq"), None, "head"),
        P(("groups", "seq"), None, None, "head"),
        P(("groups", "seq", "sub"), None, None, "head"),
        P("groups", None),
        P("groups"),
        P("groups"),
    )
    return jax.shard_map(
        per_device,
        mesh=mesh,
        in_specs=placed,
        out_specs=P(("groups", "seq"), None, "head"),
        check_vma=False,
    )
```

```python
import functools
import itertools

import jax
import jax.numpy as jnp
from jax import lax
from jax.experimental import pallas as pl
from jax.experimental.pallas import tpu as pltpu
from jax.sharding import PartitionSpec as P

HD = 128
PAGE = 128


NEG_FILL = -1e30


def partial_softmax(
    query_heads, cache_keys, cache_values, cache_valid, fresh_keys, fresh_values, fresh_valid
):
    score_scale = HD ** (-0.5)
    cache_scores = (
        jnp.einsum("rkgd,nkd->kgrn", query_heads, cache_keys, preferred_element_type=jnp.float32)
        * score_scale
    )
    fresh_scores = (
        jnp.einsum("rkgd,jkd->kgrj", query_heads, fresh_keys, preferred_element_type=jnp.float32)
        * score_scale
    )
    cache_mask = cache_valid[None, None, None, :]
    fresh_mask = fresh_valid[None, None, :, :]
    peak = jnp.maximum(
        jnp.max(jnp.where(cache_mask, cache_scores, NEG_FILL), axis=-1),
        jnp.max(jnp.where(fresh_mask, fresh_scores, NEG_FILL), axis=-1),
    )
    cache_weights = jnp.where(cache_mask, jnp.exp(cache_scores - peak[..., None]), 0.0)
    fresh_weights = jnp.where(fresh_mask, jnp.exp(fresh_scores - peak[..., None]), 0.0)
    weight_sum = jnp.sum(cache_weights, axis=-1) + jnp.sum(fresh_weights, axis=-1)
    numerator = jnp.einsum(
        "kgrn,nkd->kgrd",
        cache_weights.astype(jnp.bfloat16),
        cache_values,
        preferred_element_type=jnp.float32,
    )
    numerator = numerator + jnp.einsum(
        "kgrj,jkd->kgrd",
        fresh_weights.astype(jnp.bfloat16),
        fresh_values,
        preferred_element_type=jnp.float32,
    )
    return (peak, weight_sum, numerator)


def attend_all(
    query_block, fresh_block, received, fetch_index, page_here, lengths, live_rows, causal, fresh_on
):
    kv_width = received.shape[-1]
    heads_kv = kv_width // HD
    row_count = query_block.shape[1]
    group_size = query_block.shape[2] // kv_width
    page_count = fetch_index.shape[1]
    positions = jnp.arange(page_count * PAGE, dtype=jnp.int32)

    def one_sequence(inputs):
        query_rows, fresh_rows, index_row, here_row, length, live_row = inputs
        fetched = jnp.take(received, index_row, axis=0)
        cache_keys = fetched[:, 0].reshape(page_count * PAGE, heads_kv, HD)
        cache_values = fetched[:, 1].reshape(page_count * PAGE, heads_kv, HD)
        page_mask = jnp.broadcast_to(here_row[:, None], (page_count, PAGE)).reshape(
            page_count * PAGE
        )
        cache_valid = page_mask & (positions < length)
        query_heads = query_rows.reshape(row_count, heads_kv, group_size, HD)
        fresh_keys = fresh_rows[:, 0].reshape(row_count, heads_kv, HD)
        fresh_values = fresh_rows[:, 1].reshape(row_count, heads_kv, HD)
        fresh_valid = causal & live_row[:, None] & fresh_on
        return partial_softmax(
            query_heads,
            cache_keys,
            cache_values,
            cache_valid,
            fresh_keys,
            fresh_values,
            fresh_valid,
        )

    return lax.map(
        one_sequence, (query_block, fresh_block, fetch_index, page_here, lengths, live_rows)
    )


def finish(weight_sum, numerator, live_rows):
    unused_rows = 1.0 - live_rows.astype(jnp.float32)
    attended = numerator / (weight_sum + unused_rows[:, None, None, :])[..., None]
    attended = jnp.where(live_rows[:, None, None, :, None], attended, 0.0)
    seq_dev, heads_kv, group_size, row_count, head_dim = attended.shape
    return (
        jnp.transpose(attended, (0, 3, 1, 2, 4))
        .reshape(seq_dev, row_count, heads_kv * group_size * head_dim)
        .astype(jnp.bfloat16)
    )


def exchange_pages(queries, new_kv, kv_pages, page_table, cached_len, is_prefill):
    seq_shards = lax.axis_size("seq")
    sub_count = lax.axis_size("sub")
    owners = seq_shards * sub_count
    seq_index = lax.axis_index("seq")
    core_index = lax.axis_index("sub")
    owner_self = seq_index * sub_count + core_index
    seq_dev, row_count, query_width = queries.shape
    pages_dev = kv_pages.shape[0]
    kv_width = kv_pages.shape[3]
    page_count = page_table.shape[1]
    entries = seq_dev * page_count
    capacity = (entries + owners - 1) // owners
    table_rows = page_table.reshape(seq_shards, entries)
    holder = jnp.where(table_rows >= 0, table_rows // pages_dev, -1)
    slot_of = jnp.where(table_rows >= 0, table_rows % pages_dev, 0)
    owned_here = holder == owner_self
    rank_among = jnp.cumsum(owned_here.astype(jnp.int32), axis=1) - 1
    picked = owned_here[:, :, None] & (
        rank_among[:, :, None] == jnp.arange(capacity, dtype=jnp.int32)[None, None, :]
    )
    send_slots = jnp.sum(jnp.where(picked, slot_of[:, :, None], 0), axis=1).reshape(
        seq_shards * capacity
    )
    first_seq = seq_index * seq_dev
    my_table = lax.dynamic_slice_in_dim(page_table, first_seq, seq_dev, 0)
    my_lengths = lax.dynamic_slice_in_dim(cached_len, first_seq, seq_dev, 0)
    my_flags = lax.dynamic_slice_in_dim(is_prefill, first_seq, seq_dev, 0)
    flat_table = my_table.reshape(entries)
    my_holder = jnp.where(flat_table >= 0, flat_table // pages_dev, -1)
    entry_order = jnp.arange(entries, dtype=jnp.int32)
    earlier = (my_holder[:, None] == my_holder[None, :]) & (
        entry_order[None, :] < entry_order[:, None]
    )
    my_rank = jnp.sum(earlier.astype(jnp.int32), axis=1)
    row_ids = jnp.arange(row_count, dtype=jnp.int32)
    live_rows = (my_flags[:, None] == 1) | (row_ids[None, :] == 0)
    causal = row_ids[None, :] <= row_ids[:, None]
    part_width = kv_width // sub_count
    split_pages = kv_pages.reshape(pages_dev, 2, PAGE, sub_count, part_width)
    chosen = jnp.take(split_pages, send_slots, axis=0).reshape(
        seq_shards, capacity, 2, PAGE, sub_count, part_width
    )
    outgoing = jnp.moveaxis(chosen, 4, 1).reshape(owners, capacity, 2, PAGE, part_width)
    received = lax.all_to_all(
        outgoing, ("seq", "sub"), split_axis=0, concat_axis=0, tiled=True
    ).reshape(owners * capacity, 2, PAGE, part_width)
    present = flat_table >= 0
    fetch_index = jnp.where(present, my_holder * capacity + my_rank, 0)
    query_part = query_width // sub_count
    my_queries = lax.dynamic_slice_in_dim(queries, core_index * query_part, query_part, 2)
    my_fresh = lax.dynamic_slice_in_dim(new_kv, core_index * part_width, part_width, 3)
    peak, weight_sum, numerator = attend_all(
        my_queries,
        my_fresh,
        received,
        fetch_index.reshape(seq_dev, page_count),
        present.reshape(seq_dev, page_count),
        my_lengths,
        live_rows,
        causal,
        core_index >= 0,
    )
    own_heads = finish(weight_sum, numerator, live_rows)
    return lax.all_gather(own_heads, "sub", axis=2, tiled=True)


MESH = pl.DeviceIdType.MESH
SCALE = HD ** (-0.5)
LOG2E = 1.4426950408889634
DEC_MAXP = 4
LANES = 256
LAG = 3
FIRST = 1
ROWS16 = 16


def hi(a, b):
    return max(a, b) if isinstance(a, int) and isinstance(b, int) else jnp.maximum(a, b)


def lo(a, b):
    return min(a, b) if isinstance(a, int) and isinstance(b, int) else jnp.minimum(a, b)


def sel(c, a, b):
    return (a if c else b) if isinstance(c, bool) else jnp.where(c, a, b)


def query_spans(own):
    spans, leads, span, lead = [], [], 0, 0
    for count in own:
        lead = sel(count > 0, 0, LAG + lead)
        span = sel(span == 0, count, LAG + span + hi(count - LAG, 0))
        spans.append(span)
        leads.append(lead)
    return spans, leads


def stream_plan(own):
    n = len(own)
    spans, _ = query_spans(own)
    back, back_leads = query_spans(own[::-1])
    bases, base = [], 0
    for z in range(n - 1):
        ahead, behind = (spans[z - 1] if z else 0), back[n - 2 - z]
        clear = hi(spans[z] - back_leads[n - 2 - z], lo(ahead, behind) + LAG + FIRST)
        base = hi(base, clear)
        bases.append(base)
        base = base + 2 * LAG
    return spans, bases


def stream_lengths(n, seq_dev, slots, parts):
    lengths, work = [0] * (n - 1), 0
    for counts in itertools.product(range(seq_dev + 1), repeat=n):
        if sum(counts) != slots or max(counts) != seq_dev:
            continue
        own = [parts * c for c in counts]
        spans, bases = stream_plan(own)
        back = query_spans(own[::-1])[0]
        for z in range(n):
            ahead, behind = (spans[z - 1] if z else 0), (back[n - 2 - z] if z < n - 1 else 0)
            work = max(work, ahead + behind + own[z])
            if z < n - 1:
                lengths[z] = max(lengths[z], spans[z], bases[z] + behind if behind else 0)
    return lengths, work


def pick(values, z):
    found = 0
    for j, value in enumerate(values):
        found = found + jnp.where(z == j, value, 0)
    return found


def merge(o1, e1, o2, e2):
    top = jnp.maximum(e1, e2)
    w1, w2 = jnp.exp(e1 - top), jnp.exp(e2 - top)
    total = w1 + w2
    inv = 1.0 / total
    return o1 * (w1 * inv) + o2 * (w2 * inv), top + jnp.log(total)


def attend(query, blocks):
    scored = []
    for keys, _, mask in blocks:
        s = lax.dot_general(keys, query, (((1,), (0,)), ((), ())), preferred_element_type=jnp.float32)
        scored.append(jnp.where(mask, s, NEG_FILL))
    peak = functools.reduce(jnp.maximum, [jnp.max(s, axis=0, keepdims=True) for s in scored])
    peak = jnp.maximum(peak, 0.1 * NEG_FILL)
    acc, total = None, None
    for s, (_, values, _) in zip(scored, blocks):
        weights = jnp.exp2((s - peak) * (SCALE * LOG2E))
        part = jnp.sum(weights, axis=0, keepdims=True)
        prod = lax.dot_general(
            values, weights.astype(jnp.bfloat16), (((0,), (0,)), ((), ())), preferred_element_type=jnp.float32
        )
        acc = prod if acc is None else acc + prod
        total = part if total is None else total + part
    empty = total == 0.0
    total = jnp.where(empty, 1.0, total)
    return acc * (1.0 / total), jnp.where(empty, NEG_FILL, peak * SCALE + jnp.log(total))


def fused_kernel(
    n, lengths, work, heads, group_size, rows, seq_dev, pages_dev,
    table_hbm, cached_hbm, flags_hbm, q_hbm, new_hbm, kv_hbm, out,
    table, cached, flags, new_kv,
    kv, q_vm, own_t, fresh, dec_rows, dec_own, dec_all, dec_o, dec_e, dec_fin,
    a_o, a_e, b_o, b_e, c_o, c_e, d_o, d_e, la_o, la_e, lc_o, lc_e, po, pe,
    dqa, dqb, dqc, dqd, doa, dea, dob, deb, doc, dec, dod, ded,
    slot_seq, rest_seq, slot_of, rest_of, own_tab, start_tab, in_tab,
    in_sem, q_sem, kv_sem, kvs_sem, kvr_sem, outs_sem, outr_sem,
    bs, br, bes, ber, ds, dr, des, der, xs, xr,
):
    z, core = lax.axis_index("seq"), lax.axis_index("sub")
    other = 1 - core
    has_left, has_right = z > 0, z < n - 1
    seqs, page_count = table.shape
    owners = 2 * n
    each = page_count // owners
    slots = seqs // 2
    rests = seqs - slots
    width = q_vm.shape[2]
    groups_part = LANES // rows
    parts_head = group_size // groups_part
    parts = heads * parts_head
    first_seq = z * seq_dev
    head_lanes = group_size * rests
    dec_lanes = heads * head_lanes

    barrier = pltpu.get_barrier_semaphore()

    @pl.when(has_left)
    def _():
        pl.semaphore_signal(barrier, inc=1, device_id={"seq": z - 1}, device_id_type=MESH)

    @pl.when(has_right)
    def _():
        pl.semaphore_signal(barrier, inc=1, device_id={"seq": z + 1}, device_id_type=MESH)

    pl.semaphore_signal(barrier, inc=1, device_id={"sub": other}, device_id_type=MESH)

    small = [
        pltpu.make_async_copy(src, dst, in_sem.at[i])
        for i, (src, dst) in enumerate(
            ((table_hbm, table), (cached_hbm, cached), (flags_hbm, flags), (new_hbm, new_kv))
        )
    ]
    for x in small:
        x.start()
    q_copy = pltpu.make_async_copy(q_hbm.at[:, :, pl.ds(pl.multiple_of(core * width, width), width)], q_vm, q_sem)
    q_copy.start()

    def kv_cols(side, k):
        return kv_hbm.at[:, :, :, pl.ds(pl.multiple_of((side * heads + k) * HD, HD), HD)]

    kv_own = [pltpu.make_async_copy(kv_cols(core, k), kv.at[0, k], kv_sem.at[k]) for k in range(heads)]
    for x in kv_own:
        x.start()
    kv_far = [
        pltpu.make_async_remote_copy(
            src_ref=kv_cols(other, k), dst_ref=kv.at[1, k], send_sem=kvs_sem.at[k], recv_sem=kvr_sem.at[k],
            device_id={"sub": other}, device_id_type=MESH,
        )
        for k in range(heads)
    ]

    for x in small[:3]:
        x.wait()
    count, cum, own, before = 0, [], [], 0
    for j in range(seqs):
        count = count + flags[j]
        cum.append(count)
        slot_of[j] = jnp.clip(count - 1, 0, slots - 1)
        rest_of[j] = jnp.clip(j - count, 0, rests - 1)
        if j % seq_dev == seq_dev - 1:
            start_tab[j // seq_dev] = before
            own.append((count - before) * parts)
            own_tab[j // seq_dev] = own[-1]
            before = count
    for i in range(slots):
        slot_seq[i] = jnp.minimum(sum((c <= i).astype(jnp.int32) for c in cum), seqs - 1)
    for i in range(rests):
        rest_seq[i] = jnp.minimum(
            sum((j + 1 - c <= i).astype(jnp.int32) for j, c in enumerate(cum)), seqs - 1
        )
    spans_r, base_r = stream_plan(own)
    spans_l, base_l = stream_plan(own[::-1])
    ins_r, ins_l = [0] + spans_r[:-1], spans_l[::-1][1:] + [0]
    for w in range(n):
        in_tab[w] = ins_r[w]
        in_tab[n + w] = ins_l[w]
    query_in_r, query_in_l = pick(ins_r, z), pick(ins_l, z)
    query_out_r, query_out_l = pick(spans_r, z), pick(spans_l[::-1], z)
    both = jnp.minimum(query_in_r, query_in_l)
    foreign = query_in_r + query_in_l
    my_start = start_tab[z]
    out_base_r, in_base_r = pick(base_r + [0], z), pick([0] + base_r, z)
    out_base_l, in_base_l = pick(([0] + base_l[::-1]), z), pick(base_l[::-1] + [0], z)
    in_r, out_r = pick([0] + lengths, z), pick(lengths + [0], z)
    in_l, out_l = pick(lengths[::-1] + [0], z), pick([0] + lengths[::-1], z)
    top = max(lengths) - 1
    reach = LAG * jnp.maximum(z, n - 1 - z)
    dec_at = LAG * (n - 1) + rests * heads

    def when_right(k):
        return jnp.clip(jnp.where(k < both, 2 * k, k + both), 0, work - 1)

    def when_left(k):
        return jnp.clip(jnp.where(k < both, 2 * k + 1, k + both), 0, work - 1)

    def send(src, dst, s, r, to):
        return pltpu.make_async_remote_copy(
            src_ref=src, dst_ref=dst, send_sem=s, recv_sem=r, device_id={"seq": to}, device_id_type=MESH
        )

    def right(p):
        return (
            send(b_o.at[p], a_o.at[p], bs.at[p], br.at[p], z + 1),
            send(b_e.at[p], a_e.at[p], bes.at[p], ber.at[p], z + 1),
        )

    def left(p):
        return (
            send(d_o.at[p], c_o.at[p], ds.at[p], dr.at[p], z - 1),
            send(d_e.at[p], c_e.at[p], des.at[p], der.at[p], z - 1),
        )

    def right_dq():
        return send(dqb, dqa, xs.at[0], xr.at[0], z + 1)

    def left_dq():
        return send(dqd, dqc, xs.at[1], xr.at[1], z - 1)

    def right_do():
        return (send(dob, doa, xs.at[2], xr.at[2], z + 1), send(deb, dea, xs.at[3], xr.at[3], z + 1))

    def left_do():
        return (send(dod, doc, xs.at[4], xr.at[4], z - 1), send(ded, dec, xs.at[5], xr.at[5], z - 1))

    pl.semaphore_wait(barrier, has_left.astype(jnp.int32) + has_right.astype(jnp.int32) + 1)
    for x in kv_far:
        x.start()

    dec_lane = lax.broadcasted_iota(jnp.int32, (1, dec_lanes), 1)
    dec_of = dec_lane % rests
    dec_head = dec_lane // head_lanes
    dec_home = jnp.zeros((1, dec_lanes), jnp.int32)
    q_copy.wait()
    for d in range(rests):
        home = rest_seq[d] // seq_dev
        local = jnp.clip(rest_seq[d] - first_seq, 0, seq_dev - 1)
        dec_rows[d : d + 1, :] = q_vm[local, 0:ROWS16, :].astype(jnp.float32)[0:1]
        dec_home = jnp.where(dec_of == d, home, dec_home)
    stacked = jnp.concatenate(
        [dec_rows[:, h * HD : (h + 1) * HD] for h in range(heads * group_size)], axis=0
    )
    dec_own[...] = stacked.T.astype(jnp.bfloat16)

    def turn(j, carry):
        for c in range(parts):
            stacked = jnp.concatenate(
                [q_vm[j, :, (c * groups_part + g) * HD : (c * groups_part + g + 1) * HD] for g in range(groups_part)],
                axis=0,
            )
            own_t[j * parts + c] = stacked.astype(jnp.float32).T.astype(jnp.bfloat16)
        return carry

    lax.fori_loop(0, seq_dev, turn, 0)
    dec_o[...] = jnp.zeros_like(dec_o)
    dec_e[...] = jnp.full_like(dec_e, NEG_FILL)

    key_id = lax.broadcasted_iota(jnp.int32, (PAGE, 1), 0)
    fresh_id = lax.broadcasted_iota(jnp.int32, (rows, LANES), 0)
    lane_row = lax.broadcasted_iota(jnp.int32, (rows, LANES), 1) % rows
    causal = fresh_id <= lane_row
    dec_fresh = lax.broadcasted_iota(jnp.int32, (ROWS16, 1), 0)

    def own_query(rank):
        rank = jnp.clip(rank, 0, seq_dev * parts - 1)
        slot = jnp.minimum(my_start + rank // parts, slots - 1)
        local = jnp.clip(slot_seq[slot] - first_seq, 0, seq_dev - 1)
        return own_t[local * parts + rank % parts]

    def resolve(q, side):
        w, home, rank, done = z - 1 + 2 * side, 0, 0, False
        for _ in range(n - 1):
            w = jnp.clip(w, 0, n - 1)
            ahead = in_tab[side * n + w]
            direct = (ahead == 0) | (q < jnp.minimum(own_tab[w], LAG))
            hit = direct | (q >= LAG + ahead)
            found = hit & jnp.logical_not(done)
            home = jnp.where(found, w, home)
            rank = jnp.where(found, jnp.where(direct, q, q - ahead), rank)
            done = done | hit
            q = q - LAG
            w = w + 2 * side - 1
        return home, jnp.clip(rank, 0, seq_dev * parts - 1)

    def pages_of(seq, k, few):
        found = []
        start = table[seq, 0] // pages_dev
        for side, owner in enumerate((2 * z + core, 2 * z + other)):
            place = lax.rem(owner - start + owners, owners)
            for j in range(few):
                at = place + owners * j
                valid = jnp.clip(cached[seq] - PAGE * at, 0, PAGE)
                slot = jnp.where(valid > 0, table[seq, jnp.minimum(at, page_count - 1)] - owner * pages_dev, 0)
                slot = jnp.clip(slot, 0, pages_dev - 1)
                found.append((kv[side, k, slot, 0], kv[side, k, slot, 1], key_id < valid))
        return found

    def join(o1, e1, o2, e2, present):
        o2 = jnp.where(present, o2.astype(jnp.float32), 0.0)
        return merge(o1, e1, o2, jnp.where(present, e2, NEG_FILL))

    def assemble_right(p):
        k = jnp.maximum(p - out_base_r, 0)
        at = jnp.clip(k + LAG + in_base_r, 0, top)
        t = when_left(k)
        o, e = join(po[t], pe[t], la_o[at], la_e[at], has_left)
        came = (query_in_r > 0) & (p >= LAG) & (p < LAG + query_in_r)
        mine = own_query(jnp.where((query_in_r == 0) | (p < LAG), p, p - query_in_r))
        query = jnp.where(came, la_o[jnp.clip(p - LAG, 0, top)], mine)
        b_o[p] = jnp.where(p < query_out_r, query, o.astype(jnp.bfloat16))
        b_e[p] = e

    def assemble_left(p):
        k = jnp.maximum(p - out_base_l, 0)
        at = jnp.clip(k + LAG + in_base_l, 0, top)
        t = when_right(k)
        o, e = join(po[t], pe[t], lc_o[at], lc_e[at], has_right)
        came = (query_in_l > 0) & (p >= LAG) & (p < LAG + query_in_l)
        mine = own_query(jnp.where((query_in_l == 0) | (p < LAG), p, p - query_in_l))
        query = jnp.where(came, lc_o[jnp.clip(p - LAG, 0, top)], mine)
        d_o[p] = jnp.where(p < query_out_l, query, o.astype(jnp.bfloat16))
        d_e[p] = e

    def compute(t):
        paired = t < 2 * both
        is_own = t >= foreign
        right_more = query_in_r <= query_in_l
        side = jnp.where(paired, t % 2, right_more.astype(jnp.int32))
        index = jnp.clip(jnp.where(paired, t // 2, t - both), 0, top)
        home, rank = resolve(index, side)
        home = jnp.where(is_own, z, home)
        own_rank = jnp.clip(t - foreign, 0, seq_dev * parts - 1)
        rank = jnp.where(is_own, own_rank, rank)
        seq = slot_seq[jnp.minimum(start_tab[home] + rank // parts, slots - 1)]
        k = (rank % parts) // parts_head
        query = jnp.where(side == 0, la_o[index], lc_o[index])
        query = jnp.where(is_own, own_query(own_rank), query)
        blocks = pages_of(seq, k, each)
        local = jnp.clip(seq - first_seq, 0, seq_dev - 1)
        head = core * heads + k
        blocks.append((fresh[local, 0, head], fresh[local, 1, head], causal & is_own))
        o, e = attend(query, blocks)
        po[t] = o
        pe[t] = e

    few = min(each, -(-DEC_MAXP // owners))

    def compute_decode(i):
        d, k = i // heads, i % heads
        seq = rest_seq[d]
        local = jnp.clip(seq - first_seq, 0, seq_dev - 1)
        at_home = (seq // seq_dev == z).astype(jnp.int32)
        mine = (dec_of == d) & (dec_head == k)
        blocks = pages_of(seq, k, few)
        head = core * heads + k
        blocks.append((fresh[local, 0, head][:ROWS16], fresh[local, 1, head][:ROWS16], dec_fresh < at_home))
        o, e = attend(dec_all[...], blocks)
        dec_o[...] = jnp.where(mine, o, dec_o[...])
        dec_e[...] = jnp.where(mine, e, dec_e[...])

    def step(s, carry):
        p, w = s - LAG * z, s - LAG * (n - 1 - z)
        t, d, r = s - LAG, s - reach, s - LAG

        @pl.when(has_left & (p == 0))
        def _():
            right_dq().wait_recv()

        @pl.when(has_right & (p == 0))
        def _():
            dqb[...] = jnp.where(dec_home == z, dec_own[...], dqa[...])
            right_dq().start()

        @pl.when(has_right & (w == 0))
        def _():
            left_dq().wait_recv()

        @pl.when(has_left & (w == 0))
        def _():
            dqd[...] = jnp.where(dec_home == z, dec_own[...], dqc[...])
            left_dq().start()

        @pl.when((r >= 0) & (r < in_r))
        def _():
            for x in right(r):
                x.wait_recv()
            la_o[r] = a_o[r]
            la_e[r] = a_e[r]

        @pl.when(s < out_r)
        def _():
            assemble_right(s)
            for x in right(s):
                x.start()

        @pl.when((r >= 0) & (r < in_l))
        def _():
            for x in left(r):
                x.wait_recv()
            lc_o[r] = c_o[r]
            lc_e[r] = c_e[r]

        @pl.when(s < out_l)
        def _():
            assemble_left(s)
            for x in left(s):
                x.start()

        @pl.when(has_left & (p == dec_at))
        def _():
            for x in right_do():
                x.wait_recv()

        @pl.when(has_right & (p == dec_at))
        def _():
            o, e = join(dec_o[...], dec_e[...], doa[...], dea[...], has_left)
            dob[...] = o.astype(jnp.bfloat16)
            deb[...] = e
            for x in right_do():
                x.start()

        @pl.when(has_right & (w == dec_at))
        def _():
            for x in left_do():
                x.wait_recv()

        @pl.when(has_left & (w == dec_at))
        def _():
            o, e = join(dec_o[...], dec_e[...], doc[...], dec[...], has_right)
            dod[...] = o.astype(jnp.bfloat16)
            ded[...] = e
            for x in left_do():
                x.start()

        @pl.when(t == 0)
        def _():
            for x in kv_own:
                x.wait()
            for x in kv_far:
                x.wait_recv()
            small[3].wait()

        @pl.when((t >= 0) & (t < seq_dev))
        def _():
            for i in range(2):
                for h in range(2 * heads):
                    fresh[t, i, h] = new_kv[t, :, i, h * HD : (h + 1) * HD]

        @pl.when((t >= 0) & (t < work))
        def _():
            compute(t)

        @pl.when(d == 0)
        def _():
            dec_all[...] = jnp.where(dec_home < z, dqa[...], jnp.where(dec_home == z, dec_own[...], dqc[...]))

        @pl.when((d >= 0) & (d < rests * heads))
        def _():
            compute_decode(d)

        return carry

    steps = max(max(lengths) + LAG, work + LAG, dec_at + 1 + LAG * (n - 1))
    lax.fori_loop(0, steps, step, 0)

    o, e = join(dec_o[...], dec_e[...], doa[...], dea[...], has_left)
    o, e = join(o, e, doc[...], dec[...], has_right)
    dec_fin[...] = o.T
    top_row = lax.broadcasted_iota(jnp.int32, (rows, 1), 0) == 0

    def share(j, side):
        part = out.at[j, :, pl.ds(pl.multiple_of(side * width, width), width)]
        return pltpu.make_async_remote_copy(
            src_ref=part, dst_ref=part, send_sem=outs_sem.at[j], recv_sem=outr_sem.at[j],
            device_id={"sub": other}, device_id_type=MESH,
        )

    def finish(j, carry):
        seq = first_seq + j
        chosen = flags[seq] == 1
        slot = slot_of[seq]
        for c in range(parts):
            rank = jnp.maximum((slot - my_start) * parts + c, 0)
            t = jnp.minimum(foreign + rank, work - 1)
            to_left = jnp.where((query_in_l == 0) | (rank < LAG), rank, rank + query_in_l)
            to_right = jnp.where((query_in_r == 0) | (rank < LAG), rank, rank + query_in_r)
            at_a = jnp.clip(to_left + in_base_r, 0, top)
            at_c = jnp.clip(to_right + in_base_l, 0, top)
            o, e = join(po[t], pe[t], la_o[at_a], la_e[at_a], has_left)
            o, e = join(o, e, lc_o[at_c], lc_e[at_c], has_right)
            turned = o.T
            for g in range(groups_part):
                h = c * groups_part + g
                line_at = h * rests + rest_of[seq]
                line = jnp.where(top_row, dec_fin[pl.ds(line_at, 1), :], 0.0)
                tile = jnp.where(chosen, turned[g * rows : (g + 1) * rows], line)
                place = pl.multiple_of(core * width + h * HD, HD)
                out[j, :, pl.ds(place, HD)] = tile.astype(out.dtype)
        share(j, core).start()
        return carry

    lax.fori_loop(0, seq_dev, finish, 0)

    def drain_right(p, carry):
        for x in right(p):
            x.wait_send()
        return carry

    def drain_left(p, carry):
        for x in left(p):
            x.wait_send()
        return carry

    for x in kv_far:
        x.wait_send()

    lax.fori_loop(0, out_r, drain_right, 0)
    lax.fori_loop(0, out_l, drain_left, 0)

    @pl.when(has_right)
    def _():
        right_dq().wait_send()
        for x in right_do():
            x.wait_send()

    @pl.when(has_left)
    def _():
        left_dq().wait_send()
        for x in left_do():
            x.wait_send()

    def drain_out(j, carry):
        share(j, core).wait_send()
        share(j, other).wait_recv()
        return carry

    lax.fori_loop(0, seq_dev, drain_out, 0)


def fused_attention(queries, new_kv, kv_pages, page_table, cached_len, is_prefill):
    n = lax.axis_size("seq")
    sub_count = lax.axis_size("sub")
    seq_dev, rows, query_width = queries.shape
    pages_dev, kv_width = kv_pages.shape[0], kv_pages.shape[3]
    seqs = page_table.shape[0]
    slots = seqs // 2
    group_size = query_width // kv_width
    heads_all = kv_width // HD
    heads = heads_all // sub_count
    width = query_width // sub_count
    parts = heads * group_size * rows // LANES
    lengths, work = stream_lengths(n, seq_dev, slots, parts)
    count = max(lengths)
    bf, f32 = jnp.bfloat16, jnp.float32
    dec = heads * group_size * (seqs - slots)

    def data(c, lanes=LANES):
        return pltpu.VMEM((c, HD, lanes), bf)

    def stat(c, lanes=LANES):
        return pltpu.VMEM((c, 1, lanes), f32)

    dma = pltpu.SemaphoreType.DMA
    scratch = [
        pltpu.SMEM(page_table.shape, jnp.int32),
        pltpu.SMEM(cached_len.shape, jnp.int32),
        pltpu.SMEM(is_prefill.shape, jnp.int32),
        pltpu.VMEM(new_kv.shape, bf),
        pltpu.VMEM((2, heads, pages_dev, 2, PAGE, HD), bf),
        pltpu.VMEM((seq_dev, rows, width), bf),
        data(seq_dev * parts),
        pltpu.VMEM((seq_dev, 2, heads_all, rows, HD), bf),
        pltpu.VMEM((seqs - slots, width), f32),
        pltpu.VMEM((HD, dec), bf),
        pltpu.VMEM((HD, dec), bf),
        pltpu.VMEM((HD, dec), f32),
        pltpu.VMEM((1, dec), f32),
        pltpu.VMEM((dec, HD), f32),
    ]
    scratch += [data(count), stat(count)] * 6
    scratch += [pltpu.VMEM((work, HD, LANES), f32), stat(work)]
    scratch += [pltpu.VMEM((HD, dec), bf)] * 4
    scratch += [pltpu.VMEM((HD, dec), bf), pltpu.VMEM((1, dec), f32)] * 4
    scratch += [pltpu.SMEM((slots,), jnp.int32), pltpu.SMEM((seqs - slots,), jnp.int32)]
    scratch += [pltpu.SMEM((seqs,), jnp.int32)] * 2
    scratch += [pltpu.SMEM((n,), jnp.int32)] * 2 + [pltpu.SMEM((2 * n,), jnp.int32)]
    scratch += [dma((4,)), dma, dma((heads,)), dma((heads,)), dma((heads,))] + [dma((seq_dev,))] * 2
    scratch += [dma((count,))] * 8 + [dma((6,))] * 2
    operands = (page_table, cached_len, is_prefill, queries, new_kv, kv_pages)
    return pl.pallas_call(
        functools.partial(fused_kernel, n, lengths, work, heads, group_size, rows, seq_dev, pages_dev),
        out_shape=jax.ShapeDtypeStruct(queries.shape, queries.dtype),
        in_specs=[pl.BlockSpec(memory_space=pltpu.HBM)] * 6,
        out_specs=pl.BlockSpec(memory_space=pltpu.VMEM),
        scratch_shapes=scratch,
        compiler_params=pltpu.CompilerParams(
            collective_id=0, has_side_effects=True, vmem_limit_bytes=48 * 1024 * 1024
        ),
        name="paged_attention",
    )(*[pltpu.with_memory_space_constraint(x, pltpu.HBM) for x in operands])


def per_device(queries, new_kv, kv_pages, page_table, cached_len, is_prefill):
    owners = lax.axis_size("seq") * lax.axis_size("sub")
    if page_table.shape[1] >= owners:
        return fused_attention(queries, new_kv, kv_pages, page_table, cached_len, is_prefill)
    return exchange_pages(queries, new_kv, kv_pages, page_table, cached_len, is_prefill)


def solution(mesh):
    placed = (
        P(("groups", "seq"), None, "head"),
        P(("groups", "seq"), None, None, "head"),
        P(("groups", "seq", "sub"), None, None, "head"),
        P("groups", None),
        P("groups"),
        P("groups"),
    )
    return jax.shard_map(
        per_device,
        mesh=mesh,
        in_specs=placed,
        out_specs=P(("groups", "seq"), None, "head"),
        check_vma=False,
    )
```

```python
import functools
import itertools

import jax
import jax.numpy as jnp
from jax import lax
from jax.experimental import pallas as pl
from jax.experimental.pallas import tpu as pltpu
from jax.sharding import PartitionSpec as P

HD = 128
PAGE = 128


NEG_FILL = -1e30


def partial_softmax(
    query_heads, cache_keys, cache_values, cache_valid, fresh_keys, fresh_values, fresh_valid
):
    score_scale = HD ** (-0.5)
    cache_scores = (
        jnp.einsum("rkgd,nkd->kgrn", query_heads, cache_keys, preferred_element_type=jnp.float32)
        * score_scale
    )
    fresh_scores = (
        jnp.einsum("rkgd,jkd->kgrj", query_heads, fresh_keys, preferred_element_type=jnp.float32)
        * score_scale
    )
    cache_mask = cache_valid[None, None, None, :]
    fresh_mask = fresh_valid[None, None, :, :]
    peak = jnp.maximum(
        jnp.max(jnp.where(cache_mask, cache_scores, NEG_FILL), axis=-1),
        jnp.max(jnp.where(fresh_mask, fresh_scores, NEG_FILL), axis=-1),
    )
    cache_weights = jnp.where(cache_mask, jnp.exp(cache_scores - peak[..., None]), 0.0)
    fresh_weights = jnp.where(fresh_mask, jnp.exp(fresh_scores - peak[..., None]), 0.0)
    weight_sum = jnp.sum(cache_weights, axis=-1) + jnp.sum(fresh_weights, axis=-1)
    numerator = jnp.einsum(
        "kgrn,nkd->kgrd",
        cache_weights.astype(jnp.bfloat16),
        cache_values,
        preferred_element_type=jnp.float32,
    )
    numerator = numerator + jnp.einsum(
        "kgrj,jkd->kgrd",
        fresh_weights.astype(jnp.bfloat16),
        fresh_values,
        preferred_element_type=jnp.float32,
    )
    return (peak, weight_sum, numerator)


def attend_all(
    query_block, fresh_block, received, fetch_index, page_here, lengths, live_rows, causal, fresh_on
):
    kv_width = received.shape[-1]
    heads_kv = kv_width // HD
    row_count = query_block.shape[1]
    group_size = query_block.shape[2] // kv_width
    page_count = fetch_index.shape[1]
    positions = jnp.arange(page_count * PAGE, dtype=jnp.int32)

    def one_sequence(inputs):
        query_rows, fresh_rows, index_row, here_row, length, live_row = inputs
        fetched = jnp.take(received, index_row, axis=0)
        cache_keys = fetched[:, 0].reshape(page_count * PAGE, heads_kv, HD)
        cache_values = fetched[:, 1].reshape(page_count * PAGE, heads_kv, HD)
        page_mask = jnp.broadcast_to(here_row[:, None], (page_count, PAGE)).reshape(
            page_count * PAGE
        )
        cache_valid = page_mask & (positions < length)
        query_heads = query_rows.reshape(row_count, heads_kv, group_size, HD)
        fresh_keys = fresh_rows[:, 0].reshape(row_count, heads_kv, HD)
        fresh_values = fresh_rows[:, 1].reshape(row_count, heads_kv, HD)
        fresh_valid = causal & live_row[:, None] & fresh_on
        return partial_softmax(
            query_heads,
            cache_keys,
            cache_values,
            cache_valid,
            fresh_keys,
            fresh_values,
            fresh_valid,
        )

    return lax.map(
        one_sequence, (query_block, fresh_block, fetch_index, page_here, lengths, live_rows)
    )


def finish(weight_sum, numerator, live_rows):
    unused_rows = 1.0 - live_rows.astype(jnp.float32)
    attended = numerator / (weight_sum + unused_rows[:, None, None, :])[..., None]
    attended = jnp.where(live_rows[:, None, None, :, None], attended, 0.0)
    seq_dev, heads_kv, group_size, row_count, head_dim = attended.shape
    return (
        jnp.transpose(attended, (0, 3, 1, 2, 4))
        .reshape(seq_dev, row_count, heads_kv * group_size * head_dim)
        .astype(jnp.bfloat16)
    )


def exchange_pages(queries, new_kv, kv_pages, page_table, cached_len, is_prefill):
    seq_shards = lax.axis_size("seq")
    sub_count = lax.axis_size("sub")
    owners = seq_shards * sub_count
    seq_index = lax.axis_index("seq")
    core_index = lax.axis_index("sub")
    owner_self = seq_index * sub_count + core_index
    seq_dev, row_count, query_width = queries.shape
    pages_dev = kv_pages.shape[0]
    kv_width = kv_pages.shape[3]
    page_count = page_table.shape[1]
    entries = seq_dev * page_count
    capacity = (entries + owners - 1) // owners
    table_rows = page_table.reshape(seq_shards, entries)
    holder = jnp.where(table_rows >= 0, table_rows // pages_dev, -1)
    slot_of = jnp.where(table_rows >= 0, table_rows % pages_dev, 0)
    owned_here = holder == owner_self
    rank_among = jnp.cumsum(owned_here.astype(jnp.int32), axis=1) - 1
    picked = owned_here[:, :, None] & (
        rank_among[:, :, None] == jnp.arange(capacity, dtype=jnp.int32)[None, None, :]
    )
    send_slots = jnp.sum(jnp.where(picked, slot_of[:, :, None], 0), axis=1).reshape(
        seq_shards * capacity
    )
    first_seq = seq_index * seq_dev
    my_table = lax.dynamic_slice_in_dim(page_table, first_seq, seq_dev, 0)
    my_lengths = lax.dynamic_slice_in_dim(cached_len, first_seq, seq_dev, 0)
    my_flags = lax.dynamic_slice_in_dim(is_prefill, first_seq, seq_dev, 0)
    flat_table = my_table.reshape(entries)
    my_holder = jnp.where(flat_table >= 0, flat_table // pages_dev, -1)
    entry_order = jnp.arange(entries, dtype=jnp.int32)
    earlier = (my_holder[:, None] == my_holder[None, :]) & (
        entry_order[None, :] < entry_order[:, None]
    )
    my_rank = jnp.sum(earlier.astype(jnp.int32), axis=1)
    row_ids = jnp.arange(row_count, dtype=jnp.int32)
    live_rows = (my_flags[:, None] == 1) | (row_ids[None, :] == 0)
    causal = row_ids[None, :] <= row_ids[:, None]
    part_width = kv_width // sub_count
    split_pages = kv_pages.reshape(pages_dev, 2, PAGE, sub_count, part_width)
    chosen = jnp.take(split_pages, send_slots, axis=0).reshape(
        seq_shards, capacity, 2, PAGE, sub_count, part_width
    )
    outgoing = jnp.moveaxis(chosen, 4, 1).reshape(owners, capacity, 2, PAGE, part_width)
    received = lax.all_to_all(
        outgoing, ("seq", "sub"), split_axis=0, concat_axis=0, tiled=True
    ).reshape(owners * capacity, 2, PAGE, part_width)
    present = flat_table >= 0
    fetch_index = jnp.where(present, my_holder * capacity + my_rank, 0)
    query_part = query_width // sub_count
    my_queries = lax.dynamic_slice_in_dim(queries, core_index * query_part, query_part, 2)
    my_fresh = lax.dynamic_slice_in_dim(new_kv, core_index * part_width, part_width, 3)
    peak, weight_sum, numerator = attend_all(
        my_queries,
        my_fresh,
        received,
        fetch_index.reshape(seq_dev, page_count),
        present.reshape(seq_dev, page_count),
        my_lengths,
        live_rows,
        causal,
        core_index >= 0,
    )
    own_heads = finish(weight_sum, numerator, live_rows)
    return lax.all_gather(own_heads, "sub", axis=2, tiled=True)


MESH = pl.DeviceIdType.MESH
SCALE = HD ** (-0.5)
LOG2E = 1.4426950408889634
DEC_MAXP = 4
LANES = 256
LAG = 3
FIRST = 1
ROWS16 = 16


def hi(a, b):
    return max(a, b) if isinstance(a, int) and isinstance(b, int) else jnp.maximum(a, b)


def lo(a, b):
    return min(a, b) if isinstance(a, int) and isinstance(b, int) else jnp.minimum(a, b)


def sel(c, a, b):
    return (a if c else b) if isinstance(c, bool) else jnp.where(c, a, b)


def query_spans(own):
    spans, leads, span, lead = [], [], 0, 0
    for count in own:
        lead = sel(count > 0, 0, LAG + lead)
        span = sel(span == 0, count, LAG + span + hi(count - LAG, 0))
        spans.append(span)
        leads.append(lead)
    return spans, leads


def stream_plan(own):
    n = len(own)
    spans, _ = query_spans(own)
    back, back_leads = query_spans(own[::-1])
    bases, base = [], 0
    for z in range(n - 1):
        ahead, behind = (spans[z - 1] if z else 0), back[n - 2 - z]
        clear = hi(spans[z] - back_leads[n - 2 - z], lo(ahead, behind) + LAG + FIRST)
        base = hi(base, clear)
        bases.append(base)
        base = base + 2 * LAG
    return spans, bases


def stream_lengths(n, seq_dev, slots, parts):
    lengths, work, ready = [0] * (n - 1), 0, [0] * seq_dev
    for counts in itertools.product(range(seq_dev + 1), repeat=n):
        if sum(counts) != slots or max(counts) != seq_dev:
            continue
        own = [parts * c for c in counts]
        spans, bases = stream_plan(own)
        back, back_bases = stream_plan(own[::-1])
        for z in range(n):
            ahead, behind = (spans[z - 1] if z else 0), (back[n - 2 - z] if z < n - 1 else 0)
            for k in range(own[z]):
                done = [LAG + 1 + ahead + behind + k]
                if z:
                    done.append(LAG + bases[z - 1] + (k if behind == 0 or k < LAG else k + behind))
                if z < n - 1:
                    done.append(LAG + back_bases[n - 2 - z] + (k if ahead == 0 or k < LAG else k + ahead))
                for j in range(k // parts, seq_dev):
                    ready[j] = max(ready[j], *done)
            work = max(work, ahead + behind + own[z])
            if z < n - 1:
                lengths[z] = max(lengths[z], spans[z], bases[z] + behind if behind else 0)
    for j in range(1, seq_dev):
        ready[j] = max(ready[j], ready[j - 1] + 1)
    return lengths, work, ready


def pick(values, z):
    found = 0
    for j, value in enumerate(values):
        found = found + jnp.where(z == j, value, 0)
    return found


def merge(o1, e1, o2, e2):
    top = jnp.maximum(e1, e2)
    w1, w2 = jnp.exp(e1 - top), jnp.exp(e2 - top)
    total = w1 + w2
    inv = 1.0 / total
    return o1 * (w1 * inv) + o2 * (w2 * inv), top + jnp.log(total)


def attend(query, blocks):
    scored = []
    for keys, _, mask in blocks:
        s = lax.dot_general(keys, query, (((1,), (0,)), ((), ())), preferred_element_type=jnp.float32)
        scored.append(jnp.where(mask, s, NEG_FILL))
    peak = functools.reduce(jnp.maximum, [jnp.max(s, axis=0, keepdims=True) for s in scored])
    peak = jnp.maximum(peak, 0.1 * NEG_FILL)
    acc, total = None, None
    for s, (_, values, _) in zip(scored, blocks):
        weights = jnp.exp2((s - peak) * (SCALE * LOG2E))
        part = jnp.sum(weights, axis=0, keepdims=True)
        prod = lax.dot_general(
            values, weights.astype(jnp.bfloat16), (((0,), (0,)), ((), ())), preferred_element_type=jnp.float32
        )
        acc = prod if acc is None else acc + prod
        total = part if total is None else total + part
    empty = total == 0.0
    total = jnp.where(empty, 1.0, total)
    return acc * (1.0 / total), jnp.where(empty, NEG_FILL, peak * SCALE + jnp.log(total))


def fused_kernel(
    n, lengths, work, ready, heads, group_size, rows, seq_dev, pages_dev,
    table_hbm, cached_hbm, flags_hbm, q_hbm, new_hbm, kv_hbm, out,
    table, cached, flags, new_kv,
    kv, q_vm, own_t, fresh, dec_rows, dec_own, dec_all, dec_o, dec_e, dec_fin,
    a_o, a_e, b_o, b_e, c_o, c_e, d_o, d_e, la_o, la_e, lc_o, lc_e, po, pe,
    dqa, dqb, dqc, dqd, doa, dea, dob, deb, doc, dec, dod, ded,
    slot_seq, rest_seq, slot_of, rest_of, own_tab, start_tab, in_tab,
    in_sem, q_sem, kv_sem, kvs_sem, kvr_sem, outs_sem, outr_sem,
    bs, br, bes, ber, ds, dr, des, der, xs, xr,
):
    z, core = lax.axis_index("seq"), lax.axis_index("sub")
    other = 1 - core
    has_left, has_right = z > 0, z < n - 1
    seqs, page_count = table.shape
    owners = 2 * n
    each = page_count // owners
    slots = seqs // 2
    rests = seqs - slots
    width = q_vm.shape[2]
    groups_part = LANES // rows
    parts_head = group_size // groups_part
    parts = heads * parts_head
    first_seq = z * seq_dev
    head_lanes = group_size * rests
    dec_lanes = heads * head_lanes

    barrier = pltpu.get_barrier_semaphore()

    @pl.when(has_left)
    def _():
        pl.semaphore_signal(barrier, inc=1, device_id={"seq": z - 1}, device_id_type=MESH)

    @pl.when(has_right)
    def _():
        pl.semaphore_signal(barrier, inc=1, device_id={"seq": z + 1}, device_id_type=MESH)

    pl.semaphore_signal(barrier, inc=1, device_id={"sub": other}, device_id_type=MESH)

    small = [
        pltpu.make_async_copy(src, dst, in_sem.at[i])
        for i, (src, dst) in enumerate(
            ((table_hbm, table), (cached_hbm, cached), (flags_hbm, flags), (new_hbm, new_kv))
        )
    ]
    for x in small[:3]:
        x.start()
    q_copy = [
        pltpu.make_async_copy(
            q_hbm.at[j, :, pl.ds(pl.multiple_of(core * width, width), width)], q_vm.at[j], q_sem.at[j]
        )
        for j in range(seq_dev)
    ]
    for x in q_copy:
        x.start()

    def kv_cols(side, k):
        return kv_hbm.at[:, :, :, pl.ds(pl.multiple_of((side * heads + k) * HD, HD), HD)]

    kv_own = [pltpu.make_async_copy(kv_cols(core, k), kv.at[0, k], kv_sem.at[k]) for k in range(heads)]
    kv_far = [
        pltpu.make_async_remote_copy(
            src_ref=kv_cols(other, k), dst_ref=kv.at[1, k], send_sem=kvs_sem.at[k], recv_sem=kvr_sem.at[k],
            device_id={"sub": other}, device_id_type=MESH,
        )
        for k in range(heads)
    ]

    for x in small[:3]:
        x.wait()
    count, cum, own, before = 0, [], [], 0
    for j in range(seqs):
        count = count + flags[j]
        cum.append(count)
        slot_of[j] = jnp.clip(count - 1, 0, slots - 1)
        rest_of[j] = jnp.clip(j - count, 0, rests - 1)
        if j % seq_dev == seq_dev - 1:
            start_tab[j // seq_dev] = before
            own.append((count - before) * parts)
            own_tab[j // seq_dev] = own[-1]
            before = count
    for i in range(slots):
        slot_seq[i] = jnp.minimum(sum((c <= i).astype(jnp.int32) for c in cum), seqs - 1)
    for i in range(rests):
        rest_seq[i] = jnp.minimum(
            sum((j + 1 - c <= i).astype(jnp.int32) for j, c in enumerate(cum)), seqs - 1
        )
    spans_r, base_r = stream_plan(own)
    spans_l, base_l = stream_plan(own[::-1])
    ins_r, ins_l = [0] + spans_r[:-1], spans_l[::-1][1:] + [0]
    for w in range(n):
        in_tab[w] = ins_r[w]
        in_tab[n + w] = ins_l[w]
    query_in_r, query_in_l = pick(ins_r, z), pick(ins_l, z)
    query_out_r, query_out_l = pick(spans_r, z), pick(spans_l[::-1], z)
    both = jnp.minimum(query_in_r, query_in_l)
    foreign = query_in_r + query_in_l
    my_start = start_tab[z]
    out_base_r, in_base_r = pick(base_r + [0], z), pick([0] + base_r, z)
    out_base_l, in_base_l = pick(([0] + base_l[::-1]), z), pick(base_l[::-1] + [0], z)
    in_r, out_r = pick([0] + lengths, z), pick(lengths + [0], z)
    in_l, out_l = pick(lengths[::-1] + [0], z), pick([0] + lengths[::-1], z)
    top = max(lengths) - 1
    reach = LAG * jnp.maximum(z, n - 1 - z)
    dec_at = LAG * (n - 1) + rests * heads
    dec_done = dec_at + LAG * (n - 1)
    ready = [max(at, dec_done + 1 + j) for j, at in enumerate(ready)]

    def when_right(k):
        return jnp.clip(jnp.where(k < both, 2 * k, k + both), 0, work - 1)

    def when_left(k):
        return jnp.clip(jnp.where(k < both, 2 * k + 1, k + both), 0, work - 1)

    def send(src, dst, s, r, to):
        return pltpu.make_async_remote_copy(
            src_ref=src, dst_ref=dst, send_sem=s, recv_sem=r, device_id={"seq": to}, device_id_type=MESH
        )

    def right(p):
        return (
            send(b_o.at[p], a_o.at[p], bs.at[p], br.at[p], z + 1),
            send(b_e.at[p], a_e.at[p], bes.at[p], ber.at[p], z + 1),
        )

    def left(p):
        return (
            send(d_o.at[p], c_o.at[p], ds.at[p], dr.at[p], z - 1),
            send(d_e.at[p], c_e.at[p], des.at[p], der.at[p], z - 1),
        )

    def right_dq():
        return send(dqb, dqa, xs.at[0], xr.at[0], z + 1)

    def left_dq():
        return send(dqd, dqc, xs.at[1], xr.at[1], z - 1)

    def right_do():
        return (send(dob, doa, xs.at[2], xr.at[2], z + 1), send(deb, dea, xs.at[3], xr.at[3], z + 1))

    def left_do():
        return (send(dod, doc, xs.at[4], xr.at[4], z - 1), send(ded, dec, xs.at[5], xr.at[5], z - 1))

    pl.semaphore_wait(barrier, has_left.astype(jnp.int32) + has_right.astype(jnp.int32) + 1)
    for x in kv_far:
        x.start()

    dec_lane = lax.broadcasted_iota(jnp.int32, (1, dec_lanes), 1)
    dec_of = dec_lane % rests
    dec_head = dec_lane // head_lanes
    dec_home = jnp.zeros((1, dec_lanes), jnp.int32)
    for j in range(seq_dev):
        q_copy[j].wait()
        for c in range(parts):
            stacked = jnp.concatenate(
                [q_vm[j, :, (c * groups_part + g) * HD : (c * groups_part + g + 1) * HD] for g in range(groups_part)],
                axis=0,
            )
            own_t[j * parts + c] = stacked.astype(jnp.float32).T.astype(jnp.bfloat16)
    for x in kv_own:
        x.start()
    small[3].start()
    for d in range(rests):
        home = rest_seq[d] // seq_dev
        local = jnp.clip(rest_seq[d] - first_seq, 0, seq_dev - 1)
        dec_rows[d : d + 1, :] = q_vm[local, 0:ROWS16, :].astype(jnp.float32)[0:1]
        dec_home = jnp.where(dec_of == d, home, dec_home)
    stacked = jnp.concatenate(
        [dec_rows[:, h * HD : (h + 1) * HD] for h in range(heads * group_size)], axis=0
    )
    dec_own[...] = stacked.T.astype(jnp.bfloat16)

    dec_o[...] = jnp.zeros_like(dec_o)
    dec_e[...] = jnp.full_like(dec_e, NEG_FILL)

    key_id = lax.broadcasted_iota(jnp.int32, (PAGE, 1), 0)
    fresh_id = lax.broadcasted_iota(jnp.int32, (rows, LANES), 0)
    lane_row = lax.broadcasted_iota(jnp.int32, (rows, LANES), 1) % rows
    causal = fresh_id <= lane_row
    dec_fresh = lax.broadcasted_iota(jnp.int32, (ROWS16, 1), 0)

    def own_query(rank):
        rank = jnp.clip(rank, 0, seq_dev * parts - 1)
        slot = jnp.minimum(my_start + rank // parts, slots - 1)
        local = jnp.clip(slot_seq[slot] - first_seq, 0, seq_dev - 1)
        return own_t[local * parts + rank % parts]

    def resolve(q, side):
        w, home, rank, done = z - 1 + 2 * side, 0, 0, False
        for _ in range(n - 1):
            w = jnp.clip(w, 0, n - 1)
            ahead = in_tab[side * n + w]
            direct = (ahead == 0) | (q < jnp.minimum(own_tab[w], LAG))
            hit = direct | (q >= LAG + ahead)
            found = hit & jnp.logical_not(done)
            home = jnp.where(found, w, home)
            rank = jnp.where(found, jnp.where(direct, q, q - ahead), rank)
            done = done | hit
            q = q - LAG
            w = w + 2 * side - 1
        return home, jnp.clip(rank, 0, seq_dev * parts - 1)

    def pages_of(seq, k, few):
        found = []
        start = table[seq, 0] // pages_dev
        for side, owner in enumerate((2 * z + core, 2 * z + other)):
            place = lax.rem(owner - start + owners, owners)
            for j in range(few):
                at = place + owners * j
                valid = jnp.clip(cached[seq] - PAGE * at, 0, PAGE)
                slot = jnp.where(valid > 0, table[seq, jnp.minimum(at, page_count - 1)] - owner * pages_dev, 0)
                slot = jnp.clip(slot, 0, pages_dev - 1)
                found.append((kv[side, k, slot, 0], kv[side, k, slot, 1], key_id < valid))
        return found

    def join(o1, e1, o2, e2, present):
        o2 = jnp.where(present, o2.astype(jnp.float32), 0.0)
        return merge(o1, e1, o2, jnp.where(present, e2, NEG_FILL))

    def assemble_right(p):
        k = jnp.maximum(p - out_base_r, 0)
        at = jnp.clip(k + LAG + in_base_r, 0, top)
        t = when_left(k)
        o, e = join(po[t], pe[t], la_o[at], la_e[at], has_left)
        came = (query_in_r > 0) & (p >= LAG) & (p < LAG + query_in_r)
        mine = own_query(jnp.where((query_in_r == 0) | (p < LAG), p, p - query_in_r))
        query = jnp.where(came, la_o[jnp.clip(p - LAG, 0, top)], mine)
        b_o[p] = jnp.where(p < query_out_r, query, o.astype(jnp.bfloat16))
        b_e[p] = e

    def assemble_left(p):
        k = jnp.maximum(p - out_base_l, 0)
        at = jnp.clip(k + LAG + in_base_l, 0, top)
        t = when_right(k)
        o, e = join(po[t], pe[t], lc_o[at], lc_e[at], has_right)
        came = (query_in_l > 0) & (p >= LAG) & (p < LAG + query_in_l)
        mine = own_query(jnp.where((query_in_l == 0) | (p < LAG), p, p - query_in_l))
        query = jnp.where(came, lc_o[jnp.clip(p - LAG, 0, top)], mine)
        d_o[p] = jnp.where(p < query_out_l, query, o.astype(jnp.bfloat16))
        d_e[p] = e

    def compute(t):
        paired = t < 2 * both
        is_own = t >= foreign
        right_more = query_in_r <= query_in_l
        side = jnp.where(paired, t % 2, right_more.astype(jnp.int32))
        index = jnp.clip(jnp.where(paired, t // 2, t - both), 0, top)
        home, rank = resolve(index, side)
        home = jnp.where(is_own, z, home)
        own_rank = jnp.clip(t - foreign, 0, seq_dev * parts - 1)
        rank = jnp.where(is_own, own_rank, rank)
        seq = slot_seq[jnp.minimum(start_tab[home] + rank // parts, slots - 1)]
        k = (rank % parts) // parts_head
        query = jnp.where(side == 0, la_o[index], lc_o[index])
        query = jnp.where(is_own, own_query(own_rank), query)
        blocks = pages_of(seq, k, each)
        local = jnp.clip(seq - first_seq, 0, seq_dev - 1)
        head = core * heads + k
        blocks.append((fresh[local, 0, head], fresh[local, 1, head], causal & is_own))
        o, e = attend(query, blocks)
        po[t] = o
        pe[t] = e

    few = min(each, -(-DEC_MAXP // owners))

    def compute_decode(i):
        d, k = i // heads, i % heads
        seq = rest_seq[d]
        local = jnp.clip(seq - first_seq, 0, seq_dev - 1)
        at_home = (seq // seq_dev == z).astype(jnp.int32)
        mine = (dec_of == d) & (dec_head == k)
        blocks = pages_of(seq, k, few)
        head = core * heads + k
        blocks.append((fresh[local, 0, head][:ROWS16], fresh[local, 1, head][:ROWS16], dec_fresh < at_home))
        o, e = attend(dec_all[...], blocks)
        dec_o[...] = jnp.where(mine, o, dec_o[...])
        dec_e[...] = jnp.where(mine, e, dec_e[...])

    top_row = lax.broadcasted_iota(jnp.int32, (rows, 1), 0) == 0

    def share(j, side):
        part = out.at[j, :, pl.ds(pl.multiple_of(side * width, width), width)]
        return pltpu.make_async_remote_copy(
            src_ref=part, dst_ref=part, send_sem=outs_sem.at[j], recv_sem=outr_sem.at[j],
            device_id={"sub": other}, device_id_type=MESH,
        )

    def finish(j):
        seq = first_seq + j
        chosen = flags[seq] == 1
        slot = slot_of[seq]
        for c in range(parts):
            rank = jnp.maximum((slot - my_start) * parts + c, 0)
            t = jnp.minimum(foreign + rank, work - 1)
            to_left = jnp.where((query_in_l == 0) | (rank < LAG), rank, rank + query_in_l)
            to_right = jnp.where((query_in_r == 0) | (rank < LAG), rank, rank + query_in_r)
            at_a = jnp.clip(to_left + in_base_r, 0, top)
            at_c = jnp.clip(to_right + in_base_l, 0, top)
            o, e = join(po[t], pe[t], la_o[at_a], la_e[at_a], has_left)
            o, e = join(o, e, lc_o[at_c], lc_e[at_c], has_right)
            turned = o.T
            for g in range(groups_part):
                h = c * groups_part + g
                line_at = h * rests + rest_of[seq]
                line = jnp.where(top_row, dec_fin[pl.ds(line_at, 1), :], 0.0)
                tile = jnp.where(chosen, turned[g * rows : (g + 1) * rows], line)
                place = pl.multiple_of(core * width + h * HD, HD)
                out[j, :, pl.ds(place, HD)] = tile.astype(out.dtype)
        share(j, core).start()

    def step(s, carry):
        p, w = s - LAG * z, s - LAG * (n - 1 - z)
        t, d, r = s - LAG, s - reach, s - LAG

        @pl.when(has_left & (p == 0))
        def _():
            right_dq().wait_recv()

        @pl.when(has_right & (p == 0))
        def _():
            dqb[...] = jnp.where(dec_home == z, dec_own[...], dqa[...])
            right_dq().start()

        @pl.when(has_right & (w == 0))
        def _():
            left_dq().wait_recv()

        @pl.when(has_left & (w == 0))
        def _():
            dqd[...] = jnp.where(dec_home == z, dec_own[...], dqc[...])
            left_dq().start()

        @pl.when((r >= 0) & (r < in_r))
        def _():
            for x in right(r):
                x.wait_recv()
            la_o[r] = a_o[r]
            la_e[r] = a_e[r]

        @pl.when(s < out_r)
        def _():
            assemble_right(s)
            for x in right(s):
                x.start()

        @pl.when((r >= 0) & (r < in_l))
        def _():
            for x in left(r):
                x.wait_recv()
            lc_o[r] = c_o[r]
            lc_e[r] = c_e[r]

        @pl.when(s < out_l)
        def _():
            assemble_left(s)
            for x in left(s):
                x.start()

        @pl.when(has_left & (p == dec_at))
        def _():
            for x in right_do():
                x.wait_recv()

        @pl.when(has_right & (p == dec_at))
        def _():
            o, e = join(dec_o[...], dec_e[...], doa[...], dea[...], has_left)
            dob[...] = o.astype(jnp.bfloat16)
            deb[...] = e
            for x in right_do():
                x.start()

        @pl.when(has_right & (w == dec_at))
        def _():
            for x in left_do():
                x.wait_recv()

        @pl.when(has_left & (w == dec_at))
        def _():
            o, e = join(dec_o[...], dec_e[...], doc[...], dec[...], has_right)
            dod[...] = o.astype(jnp.bfloat16)
            ded[...] = e
            for x in left_do():
                x.start()

        @pl.when(t == 0)
        def _():
            for x in kv_own:
                x.wait()
            for x in kv_far:
                x.wait_recv()
            small[3].wait()

        @pl.when((t >= 0) & (t < seq_dev))
        def _():
            for i in range(2):
                for h in range(2 * heads):
                    fresh[t, i, h] = new_kv[t, :, i, h * HD : (h + 1) * HD]

        @pl.when((t >= 0) & (t < work))
        def _():
            compute(t)

        @pl.when(d == 0)
        def _():
            dec_all[...] = jnp.where(dec_home < z, dqa[...], jnp.where(dec_home == z, dec_own[...], dqc[...]))

        @pl.when((d >= 0) & (d < rests * heads))
        def _():
            compute_decode(d)

        @pl.when(s == dec_done)
        def _():
            o, e = join(dec_o[...], dec_e[...], doa[...], dea[...], has_left)
            o, e = join(o, e, doc[...], dec[...], has_right)
            dec_fin[...] = o.T

        @pl.when(functools.reduce(jnp.logical_or, [s == at for at in ready]))
        def _():
            finish(sum((s > at).astype(jnp.int32) for at in ready[:-1]))

        return carry

    steps = max(max(lengths) + LAG, work + LAG, dec_done + 1, ready[-1] + 1)
    lax.fori_loop(0, steps, step, 0)


    def drain_right(p, carry):
        for x in right(p):
            x.wait_send()
        return carry

    def drain_left(p, carry):
        for x in left(p):
            x.wait_send()
        return carry

    for x in kv_far:
        x.wait_send()

    lax.fori_loop(0, out_r, drain_right, 0)
    lax.fori_loop(0, out_l, drain_left, 0)

    @pl.when(has_right)
    def _():
        right_dq().wait_send()
        for x in right_do():
            x.wait_send()

    @pl.when(has_left)
    def _():
        left_dq().wait_send()
        for x in left_do():
            x.wait_send()

    def drain_out(j, carry):
        share(j, core).wait_send()
        share(j, other).wait_recv()
        return carry

    lax.fori_loop(0, seq_dev, drain_out, 0)


def fused_attention(queries, new_kv, kv_pages, page_table, cached_len, is_prefill):
    n = lax.axis_size("seq")
    sub_count = lax.axis_size("sub")
    seq_dev, rows, query_width = queries.shape
    pages_dev, kv_width = kv_pages.shape[0], kv_pages.shape[3]
    seqs = page_table.shape[0]
    slots = seqs // 2
    group_size = query_width // kv_width
    heads_all = kv_width // HD
    heads = heads_all // sub_count
    width = query_width // sub_count
    parts = heads * group_size * rows // LANES
    lengths, work, ready = stream_lengths(n, seq_dev, slots, parts)
    count = max(lengths)
    bf, f32 = jnp.bfloat16, jnp.float32
    dec = heads * group_size * (seqs - slots)

    def data(c, lanes=LANES):
        return pltpu.VMEM((c, HD, lanes), bf)

    def stat(c, lanes=LANES):
        return pltpu.VMEM((c, 1, lanes), f32)

    dma = pltpu.SemaphoreType.DMA
    scratch = [
        pltpu.SMEM(page_table.shape, jnp.int32),
        pltpu.SMEM(cached_len.shape, jnp.int32),
        pltpu.SMEM(is_prefill.shape, jnp.int32),
        pltpu.VMEM(new_kv.shape, bf),
        pltpu.VMEM((2, heads, pages_dev, 2, PAGE, HD), bf),
        pltpu.VMEM((seq_dev, rows, width), bf),
        data(seq_dev * parts),
        pltpu.VMEM((seq_dev, 2, heads_all, rows, HD), bf),
        pltpu.VMEM((seqs - slots, width), f32),
        pltpu.VMEM((HD, dec), bf),
        pltpu.VMEM((HD, dec), bf),
        pltpu.VMEM((HD, dec), f32),
        pltpu.VMEM((1, dec), f32),
        pltpu.VMEM((dec, HD), f32),
    ]
    scratch += [data(count), stat(count)] * 6
    scratch += [pltpu.VMEM((work, HD, LANES), f32), stat(work)]
    scratch += [pltpu.VMEM((HD, dec), bf)] * 4
    scratch += [pltpu.VMEM((HD, dec), bf), pltpu.VMEM((1, dec), f32)] * 4
    scratch += [pltpu.SMEM((slots,), jnp.int32), pltpu.SMEM((seqs - slots,), jnp.int32)]
    scratch += [pltpu.SMEM((seqs,), jnp.int32)] * 2
    scratch += [pltpu.SMEM((n,), jnp.int32)] * 2 + [pltpu.SMEM((2 * n,), jnp.int32)]
    scratch += [dma((4,)), dma((seq_dev,)), dma((heads,)), dma((heads,)), dma((heads,))] + [dma((seq_dev,))] * 2
    scratch += [dma((count,))] * 8 + [dma((6,))] * 2
    operands = (page_table, cached_len, is_prefill, queries, new_kv, kv_pages)
    return pl.pallas_call(
        functools.partial(fused_kernel, n, lengths, work, ready, heads, group_size, rows, seq_dev, pages_dev),
        out_shape=jax.ShapeDtypeStruct(queries.shape, queries.dtype),
        in_specs=[pl.BlockSpec(memory_space=pltpu.HBM)] * 6,
        out_specs=pl.BlockSpec(memory_space=pltpu.VMEM),
        scratch_shapes=scratch,
        compiler_params=pltpu.CompilerParams(
            collective_id=0, has_side_effects=True, vmem_limit_bytes=48 * 1024 * 1024
        ),
        name="paged_attention",
    )(*[pltpu.with_memory_space_constraint(x, pltpu.HBM) for x in operands])


def per_device(queries, new_kv, kv_pages, page_table, cached_len, is_prefill):
    owners = lax.axis_size("seq") * lax.axis_size("sub")
    if page_table.shape[1] >= owners:
        return fused_attention(queries, new_kv, kv_pages, page_table, cached_len, is_prefill)
    return exchange_pages(queries, new_kv, kv_pages, page_table, cached_len, is_prefill)


def solution(mesh):
    placed = (
        P(("groups", "seq"), None, "head"),
        P(("groups", "seq"), None, None, "head"),
        P(("groups", "seq", "sub"), None, None, "head"),
        P("groups", None),
        P("groups"),
        P("groups"),
    )
    return jax.shard_map(
        per_device,
        mesh=mesh,
        in_specs=placed,
        out_specs=P(("groups", "seq"), None, "head"),
        check_vma=False,
    )
```

```python
import functools
import itertools

import jax
import jax.numpy as jnp
from jax import lax
from jax.experimental import pallas as pl
from jax.experimental.pallas import tpu as pltpu
from jax.sharding import PartitionSpec as P

HD = 128
PAGE = 128


NEG_FILL = -1e30


def partial_softmax(
    query_heads, cache_keys, cache_values, cache_valid, fresh_keys, fresh_values, fresh_valid
):
    score_scale = HD ** (-0.5)
    cache_scores = (
        jnp.einsum("rkgd,nkd->kgrn", query_heads, cache_keys, preferred_element_type=jnp.float32)
        * score_scale
    )
    fresh_scores = (
        jnp.einsum("rkgd,jkd->kgrj", query_heads, fresh_keys, preferred_element_type=jnp.float32)
        * score_scale
    )
    cache_mask = cache_valid[None, None, None, :]
    fresh_mask = fresh_valid[None, None, :, :]
    peak = jnp.maximum(
        jnp.max(jnp.where(cache_mask, cache_scores, NEG_FILL), axis=-1),
        jnp.max(jnp.where(fresh_mask, fresh_scores, NEG_FILL), axis=-1),
    )
    cache_weights = jnp.where(cache_mask, jnp.exp(cache_scores - peak[..., None]), 0.0)
    fresh_weights = jnp.where(fresh_mask, jnp.exp(fresh_scores - peak[..., None]), 0.0)
    weight_sum = jnp.sum(cache_weights, axis=-1) + jnp.sum(fresh_weights, axis=-1)
    numerator = jnp.einsum(
        "kgrn,nkd->kgrd",
        cache_weights.astype(jnp.bfloat16),
        cache_values,
        preferred_element_type=jnp.float32,
    )
    numerator = numerator + jnp.einsum(
        "kgrj,jkd->kgrd",
        fresh_weights.astype(jnp.bfloat16),
        fresh_values,
        preferred_element_type=jnp.float32,
    )
    return (peak, weight_sum, numerator)


def attend_all(
    query_block, fresh_block, received, fetch_index, page_here, lengths, live_rows, causal, fresh_on
):
    kv_width = received.shape[-1]
    heads_kv = kv_width // HD
    row_count = query_block.shape[1]
    group_size = query_block.shape[2] // kv_width
    page_count = fetch_index.shape[1]
    positions = jnp.arange(page_count * PAGE, dtype=jnp.int32)

    def one_sequence(inputs):
        query_rows, fresh_rows, index_row, here_row, length, live_row = inputs
        fetched = jnp.take(received, index_row, axis=0)
        cache_keys = fetched[:, 0].reshape(page_count * PAGE, heads_kv, HD)
        cache_values = fetched[:, 1].reshape(page_count * PAGE, heads_kv, HD)
        page_mask = jnp.broadcast_to(here_row[:, None], (page_count, PAGE)).reshape(
            page_count * PAGE
        )
        cache_valid = page_mask & (positions < length)
        query_heads = query_rows.reshape(row_count, heads_kv, group_size, HD)
        fresh_keys = fresh_rows[:, 0].reshape(row_count, heads_kv, HD)
        fresh_values = fresh_rows[:, 1].reshape(row_count, heads_kv, HD)
        fresh_valid = causal & live_row[:, None] & fresh_on
        return partial_softmax(
            query_heads,
            cache_keys,
            cache_values,
            cache_valid,
            fresh_keys,
            fresh_values,
            fresh_valid,
        )

    return lax.map(
        one_sequence, (query_block, fresh_block, fetch_index, page_here, lengths, live_rows)
    )


def finish(weight_sum, numerator, live_rows):
    unused_rows = 1.0 - live_rows.astype(jnp.float32)
    attended = numerator / (weight_sum + unused_rows[:, None, None, :])[..., None]
    attended = jnp.where(live_rows[:, None, None, :, None], attended, 0.0)
    seq_dev, heads_kv, group_size, row_count, head_dim = attended.shape
    return (
        jnp.transpose(attended, (0, 3, 1, 2, 4))
        .reshape(seq_dev, row_count, heads_kv * group_size * head_dim)
        .astype(jnp.bfloat16)
    )


def exchange_pages(queries, new_kv, kv_pages, page_table, cached_len, is_prefill):
    seq_shards = lax.axis_size("seq")
    sub_count = lax.axis_size("sub")
    owners = seq_shards * sub_count
    seq_index = lax.axis_index("seq")
    core_index = lax.axis_index("sub")
    owner_self = seq_index * sub_count + core_index
    seq_dev, row_count, query_width = queries.shape
    pages_dev = kv_pages.shape[0]
    kv_width = kv_pages.shape[3]
    page_count = page_table.shape[1]
    entries = seq_dev * page_count
    capacity = (entries + owners - 1) // owners
    table_rows = page_table.reshape(seq_shards, entries)
    holder = jnp.where(table_rows >= 0, table_rows // pages_dev, -1)
    slot_of = jnp.where(table_rows >= 0, table_rows % pages_dev, 0)
    owned_here = holder == owner_self
    rank_among = jnp.cumsum(owned_here.astype(jnp.int32), axis=1) - 1
    picked = owned_here[:, :, None] & (
        rank_among[:, :, None] == jnp.arange(capacity, dtype=jnp.int32)[None, None, :]
    )
    send_slots = jnp.sum(jnp.where(picked, slot_of[:, :, None], 0), axis=1).reshape(
        seq_shards * capacity
    )
    first_seq = seq_index * seq_dev
    my_table = lax.dynamic_slice_in_dim(page_table, first_seq, seq_dev, 0)
    my_lengths = lax.dynamic_slice_in_dim(cached_len, first_seq, seq_dev, 0)
    my_flags = lax.dynamic_slice_in_dim(is_prefill, first_seq, seq_dev, 0)
    flat_table = my_table.reshape(entries)
    my_holder = jnp.where(flat_table >= 0, flat_table // pages_dev, -1)
    entry_order = jnp.arange(entries, dtype=jnp.int32)
    earlier = (my_holder[:, None] == my_holder[None, :]) & (
        entry_order[None, :] < entry_order[:, None]
    )
    my_rank = jnp.sum(earlier.astype(jnp.int32), axis=1)
    row_ids = jnp.arange(row_count, dtype=jnp.int32)
    live_rows = (my_flags[:, None] == 1) | (row_ids[None, :] == 0)
    causal = row_ids[None, :] <= row_ids[:, None]
    part_width = kv_width // sub_count
    split_pages = kv_pages.reshape(pages_dev, 2, PAGE, sub_count, part_width)
    chosen = jnp.take(split_pages, send_slots, axis=0).reshape(
        seq_shards, capacity, 2, PAGE, sub_count, part_width
    )
    outgoing = jnp.moveaxis(chosen, 4, 1).reshape(owners, capacity, 2, PAGE, part_width)
    received = lax.all_to_all(
        outgoing, ("seq", "sub"), split_axis=0, concat_axis=0, tiled=True
    ).reshape(owners * capacity, 2, PAGE, part_width)
    present = flat_table >= 0
    fetch_index = jnp.where(present, my_holder * capacity + my_rank, 0)
    query_part = query_width // sub_count
    my_queries = lax.dynamic_slice_in_dim(queries, core_index * query_part, query_part, 2)
    my_fresh = lax.dynamic_slice_in_dim(new_kv, core_index * part_width, part_width, 3)
    peak, weight_sum, numerator = attend_all(
        my_queries,
        my_fresh,
        received,
        fetch_index.reshape(seq_dev, page_count),
        present.reshape(seq_dev, page_count),
        my_lengths,
        live_rows,
        causal,
        core_index >= 0,
    )
    own_heads = finish(weight_sum, numerator, live_rows)
    return lax.all_gather(own_heads, "sub", axis=2, tiled=True)


MESH = pl.DeviceIdType.MESH
SCALE = HD ** (-0.5)
LOG2E = 1.4426950408889634
DEC_MAXP = 4
LANES = 256
LAG = 3
ROWS16 = 16


def hi(a, b):
    return max(a, b) if isinstance(a, int) and isinstance(b, int) else jnp.maximum(a, b)


def lo(a, b):
    return min(a, b) if isinstance(a, int) and isinstance(b, int) else jnp.minimum(a, b)


def sel(c, a, b):
    return (a if c else b) if isinstance(c, bool) else jnp.where(c, a, b)


def query_spans(own):
    spans, leads, span, lead = [], [], 0, 0
    for count in own:
        lead = sel(count > 0, 0, LAG + lead)
        span = sel(span == 0, count, LAG + span + hi(count - LAG, 0))
        spans.append(span)
        leads.append(lead)
    return spans, leads


def work_order(ahead, lead_a, behind, lead_b):
    a, b = sel(ahead == 0, 0, lead_a), sel(behind == 0, 0, lead_b)
    swap = b >= a
    early, late = sel(swap, ahead, behind), sel(swap, behind, ahead)
    skip = lo(sel(swap, b - a, a - b), early)
    both = hi(lo(early - skip, late - skip), 0)
    delay = sel(b > a, sel(late - skip > both, both, hi(both - 1, 0)), both)
    return swap, skip, both, early + late - skip, delay


def chip_order(own, z):
    n = len(own)
    spans, leads = query_spans(own)
    back, back_leads = query_spans(own[::-1])
    ahead = (spans[z - 1], leads[z - 1]) if z else (0, 0)
    behind = (back[n - 2 - z], back_leads[n - 2 - z]) if z < n - 1 else (0, 0)
    return work_order(*ahead, *behind)


def stream_plan(own):
    n = len(own)
    spans, _ = query_spans(own)
    back, back_leads = query_spans(own[::-1])
    bases, base = [], 0
    for z in range(n - 1):
        clear = hi(spans[z] - back_leads[n - 2 - z], chip_order(own, z)[4] + LAG + (1 if z else 0))
        base = hi(base, clear)
        bases.append(base)
        base = base + 2 * LAG
    return spans, bases


def stream_lengths(n, seq_dev, slots, parts):
    lengths, work, ready = [0] * (n - 1), 0, [0] * seq_dev
    for counts in itertools.product(range(seq_dev + 1), repeat=n):
        if sum(counts) != slots or max(counts) != seq_dev:
            continue
        own = [parts * c for c in counts]
        spans, bases = stream_plan(own)
        back, back_bases = stream_plan(own[::-1])
        for z in range(n):
            ahead, behind = (spans[z - 1] if z else 0), (back[n - 2 - z] if z < n - 1 else 0)
            foreign = chip_order(own, z)[3]
            for k in range(own[z]):
                done = [LAG + 1 + foreign + k]
                if z:
                    done.append(LAG + bases[z - 1] + (k if behind == 0 or k < LAG else k + behind))
                if z < n - 1:
                    done.append(LAG + back_bases[n - 2 - z] + (k if ahead == 0 or k < LAG else k + ahead))
                for j in range(k // parts, seq_dev):
                    ready[j] = max(ready[j], *done)
            work = max(work, chip_order(own, z)[3] + own[z])
            if z < n - 1:
                lengths[z] = max(lengths[z], spans[z], bases[z] + behind if behind else 0)
    for j in range(1, seq_dev):
        ready[j] = max(ready[j], ready[j - 1] + 1)
    return lengths, work, ready


def pick(values, z):
    found = 0
    for j, value in enumerate(values):
        found = found + jnp.where(z == j, value, 0)
    return found


def merge(o1, e1, o2, e2):
    top = jnp.maximum(e1, e2)
    w1, w2 = jnp.exp(e1 - top), jnp.exp(e2 - top)
    total = w1 + w2
    inv = 1.0 / total
    return o1 * (w1 * inv) + o2 * (w2 * inv), top + jnp.log(total)


def attend(query, blocks):
    scored = []
    for keys, _, mask in blocks:
        s = lax.dot_general(keys, query, (((1,), (0,)), ((), ())), preferred_element_type=jnp.float32)
        scored.append(jnp.where(mask, s, NEG_FILL))
    peak = functools.reduce(jnp.maximum, [jnp.max(s, axis=0, keepdims=True) for s in scored])
    peak = jnp.maximum(peak, 0.1 * NEG_FILL)
    acc, total = None, None
    for s, (_, values, _) in zip(scored, blocks):
        weights = jnp.exp2((s - peak) * (SCALE * LOG2E))
        part = jnp.sum(weights, axis=0, keepdims=True)
        prod = lax.dot_general(
            values, weights.astype(jnp.bfloat16), (((0,), (0,)), ((), ())), preferred_element_type=jnp.float32
        )
        acc = prod if acc is None else acc + prod
        total = part if total is None else total + part
    empty = total == 0.0
    total = jnp.where(empty, 1.0, total)
    return acc * (1.0 / total), jnp.where(empty, NEG_FILL, peak * SCALE + jnp.log(total))


def fused_kernel(
    n, lengths, work, ready, heads, group_size, rows, seq_dev, pages_dev,
    table_hbm, cached_hbm, flags_hbm, q_hbm, new_hbm, kv_hbm, out,
    table, cached, flags, new_kv,
    kv, q_vm, own_t, fresh, dec_rows, dec_own, dec_all, dec_o, dec_e, dec_fin,
    a_o, a_e, b_o, b_e, c_o, c_e, d_o, d_e, la_o, la_e, lc_o, lc_e, po, pe,
    dqa, dqb, dqc, dqd, doa, dea, dob, deb, doc, dec, dod, ded,
    slot_seq, rest_seq, slot_of, rest_of, own_tab, start_tab, in_tab,
    in_sem, q_sem, kv_sem, kvs_sem, kvr_sem, outs_sem, outr_sem,
    bs, br, bes, ber, ds, dr, des, der, xs, xr,
):
    z, core = lax.axis_index("seq"), lax.axis_index("sub")
    other = 1 - core
    has_left, has_right = z > 0, z < n - 1
    seqs, page_count = table.shape
    owners = 2 * n
    each = page_count // owners
    slots = seqs // 2
    rests = seqs - slots
    width = q_vm.shape[2]
    groups_part = LANES // rows
    parts_head = group_size // groups_part
    parts = heads * parts_head
    first_seq = z * seq_dev
    head_lanes = group_size * rests
    dec_lanes = heads * head_lanes

    barrier = pltpu.get_barrier_semaphore()

    @pl.when(has_left)
    def _():
        pl.semaphore_signal(barrier, inc=1, device_id={"seq": z - 1}, device_id_type=MESH)

    @pl.when(has_right)
    def _():
        pl.semaphore_signal(barrier, inc=1, device_id={"seq": z + 1}, device_id_type=MESH)

    pl.semaphore_signal(barrier, inc=1, device_id={"sub": other}, device_id_type=MESH)

    small = [
        pltpu.make_async_copy(src, dst, in_sem.at[i])
        for i, (src, dst) in enumerate(
            ((table_hbm, table), (cached_hbm, cached), (flags_hbm, flags), (new_hbm, new_kv))
        )
    ]
    for x in small[:3]:
        x.start()
    q_copy = [
        pltpu.make_async_copy(
            q_hbm.at[j, :, pl.ds(pl.multiple_of(core * width, width), width)], q_vm.at[j], q_sem.at[j]
        )
        for j in range(seq_dev)
    ]
    for x in q_copy:
        x.start()

    def kv_cols(side, k):
        return kv_hbm.at[:, :, :, pl.ds(pl.multiple_of((side * heads + k) * HD, HD), HD)]

    kv_own = [pltpu.make_async_copy(kv_cols(core, k), kv.at[0, k], kv_sem.at[k]) for k in range(heads)]
    kv_far = [
        pltpu.make_async_remote_copy(
            src_ref=kv_cols(other, k), dst_ref=kv.at[1, k], send_sem=kvs_sem.at[k], recv_sem=kvr_sem.at[k],
            device_id={"sub": other}, device_id_type=MESH,
        )
        for k in range(heads)
    ]

    for x in small[:3]:
        x.wait()
    count, cum, own, before = 0, [], [], 0
    for j in range(seqs):
        count = count + flags[j]
        cum.append(count)
        slot_of[j] = jnp.clip(count - 1, 0, slots - 1)
        rest_of[j] = jnp.clip(j - count, 0, rests - 1)
        if j % seq_dev == seq_dev - 1:
            start_tab[j // seq_dev] = before
            own.append((count - before) * parts)
            own_tab[j // seq_dev] = own[-1]
            before = count
    for i in range(slots):
        slot_seq[i] = jnp.minimum(sum((c <= i).astype(jnp.int32) for c in cum), seqs - 1)
    for i in range(rests):
        rest_seq[i] = jnp.minimum(
            sum((j + 1 - c <= i).astype(jnp.int32) for j, c in enumerate(cum)), seqs - 1
        )
    spans_r, base_r = stream_plan(own)
    spans_l, base_l = stream_plan(own[::-1])
    ins_r, ins_l = [0] + spans_r[:-1], spans_l[::-1][1:] + [0]
    for w in range(n):
        in_tab[w] = ins_r[w]
        in_tab[n + w] = ins_l[w]
    query_in_r, query_in_l = pick(ins_r, z), pick(ins_l, z)
    query_out_r, query_out_l = pick(spans_r, z), pick(spans_l[::-1], z)
    orders = [chip_order(own, w) for w in range(n)]
    left_late = pick([jnp.asarray(x[0]).astype(jnp.int32) for x in orders], z) == 1
    skip, both, foreign = (pick([x[i] for x in orders], z) for i in (1, 2, 3))
    my_start = start_tab[z]
    out_base_r, in_base_r = pick(base_r + [0], z), pick([0] + base_r, z)
    out_base_l, in_base_l = pick(([0] + base_l[::-1]), z), pick(base_l[::-1] + [0], z)
    in_r, out_r = pick([0] + lengths, z), pick(lengths + [0], z)
    in_l, out_l = pick(lengths[::-1] + [0], z), pick([0] + lengths[::-1], z)
    top = max(lengths) - 1
    reach = LAG * jnp.maximum(z, n - 1 - z)
    dec_at = LAG * (n - 1) + rests * heads
    dec_done = dec_at + LAG * (n - 1)
    ready = [max(at, dec_done + 1 + j) for j, at in enumerate(ready)]

    def when(k, late):
        i = k - skip
        paired = skip + 2 * i + jnp.where(late, 0, 1)
        at = jnp.where(i < both, paired, skip + both + i)
        return jnp.clip(jnp.where(i < 0, k, at), 0, work - 1)

    def send(src, dst, s, r, to):
        return pltpu.make_async_remote_copy(
            src_ref=src, dst_ref=dst, send_sem=s, recv_sem=r, device_id={"seq": to}, device_id_type=MESH
        )

    def right(p):
        return (
            send(b_o.at[p], a_o.at[p], bs.at[p], br.at[p], z + 1),
            send(b_e.at[p], a_e.at[p], bes.at[p], ber.at[p], z + 1),
        )

    def left(p):
        return (
            send(d_o.at[p], c_o.at[p], ds.at[p], dr.at[p], z - 1),
            send(d_e.at[p], c_e.at[p], des.at[p], der.at[p], z - 1),
        )

    def right_dq():
        return send(dqb, dqa, xs.at[0], xr.at[0], z + 1)

    def left_dq():
        return send(dqd, dqc, xs.at[1], xr.at[1], z - 1)

    def right_do():
        return (send(dob, doa, xs.at[2], xr.at[2], z + 1), send(deb, dea, xs.at[3], xr.at[3], z + 1))

    def left_do():
        return (send(dod, doc, xs.at[4], xr.at[4], z - 1), send(ded, dec, xs.at[5], xr.at[5], z - 1))

    pl.semaphore_wait(barrier, has_left.astype(jnp.int32) + has_right.astype(jnp.int32) + 1)
    for x in kv_far:
        x.start()

    dec_lane = lax.broadcasted_iota(jnp.int32, (1, dec_lanes), 1)
    dec_of = dec_lane % rests
    dec_head = dec_lane // head_lanes
    dec_home = jnp.zeros((1, dec_lanes), jnp.int32)
    for j in range(seq_dev):
        q_copy[j].wait()
        for c in range(parts):
            stacked = jnp.concatenate(
                [q_vm[j, :, (c * groups_part + g) * HD : (c * groups_part + g + 1) * HD] for g in range(groups_part)],
                axis=0,
            )
            own_t[j * parts + c] = stacked.astype(jnp.float32).T.astype(jnp.bfloat16)
    for x in kv_own:
        x.start()
    small[3].start()
    for d in range(rests):
        home = rest_seq[d] // seq_dev
        local = jnp.clip(rest_seq[d] - first_seq, 0, seq_dev - 1)
        dec_rows[d : d + 1, :] = q_vm[local, 0:ROWS16, :].astype(jnp.float32)[0:1]
        dec_home = jnp.where(dec_of == d, home, dec_home)
    stacked = jnp.concatenate(
        [dec_rows[:, h * HD : (h + 1) * HD] for h in range(heads * group_size)], axis=0
    )
    dec_own[...] = stacked.T.astype(jnp.bfloat16)

    dec_o[...] = jnp.zeros_like(dec_o)
    dec_e[...] = jnp.full_like(dec_e, NEG_FILL)

    key_id = lax.broadcasted_iota(jnp.int32, (PAGE, 1), 0)
    fresh_id = lax.broadcasted_iota(jnp.int32, (rows, LANES), 0)
    lane_row = lax.broadcasted_iota(jnp.int32, (rows, LANES), 1) % rows
    causal = fresh_id <= lane_row
    dec_fresh = lax.broadcasted_iota(jnp.int32, (ROWS16, 1), 0)

    def own_query(rank):
        rank = jnp.clip(rank, 0, seq_dev * parts - 1)
        slot = jnp.minimum(my_start + rank // parts, slots - 1)
        local = jnp.clip(slot_seq[slot] - first_seq, 0, seq_dev - 1)
        return own_t[local * parts + rank % parts]

    def resolve(q, side):
        w, home, rank, done = z - 1 + 2 * side, 0, 0, False
        for _ in range(n - 1):
            w = jnp.clip(w, 0, n - 1)
            ahead = in_tab[side * n + w]
            direct = (ahead == 0) | (q < jnp.minimum(own_tab[w], LAG))
            hit = direct | (q >= LAG + ahead)
            found = hit & jnp.logical_not(done)
            home = jnp.where(found, w, home)
            rank = jnp.where(found, jnp.where(direct, q, q - ahead), rank)
            done = done | hit
            q = q - LAG
            w = w + 2 * side - 1
        return home, jnp.clip(rank, 0, seq_dev * parts - 1)

    def pages_of(seq, k, few):
        found = []
        start = table[seq, 0] // pages_dev
        for side, owner in enumerate((2 * z + core, 2 * z + other)):
            place = lax.rem(owner - start + owners, owners)
            for j in range(few):
                at = place + owners * j
                valid = jnp.clip(cached[seq] - PAGE * at, 0, PAGE)
                slot = jnp.where(valid > 0, table[seq, jnp.minimum(at, page_count - 1)] - owner * pages_dev, 0)
                slot = jnp.clip(slot, 0, pages_dev - 1)
                found.append((kv[side, k, slot, 0], kv[side, k, slot, 1], key_id < valid))
        return found

    def join(o1, e1, o2, e2, present):
        o2 = jnp.where(present, o2.astype(jnp.float32), 0.0)
        return merge(o1, e1, o2, jnp.where(present, e2, NEG_FILL))

    def assemble_right(p):
        k = jnp.maximum(p - out_base_r, 0)
        at = jnp.clip(k + LAG + in_base_r, 0, top)
        t = when(k, left_late)
        o, e = join(po[t], pe[t], la_o[at], la_e[at], has_left)
        came = (query_in_r > 0) & (p >= LAG) & (p < LAG + query_in_r)
        mine = own_query(jnp.where((query_in_r == 0) | (p < LAG), p, p - query_in_r))
        query = jnp.where(came, la_o[jnp.clip(p - LAG, 0, top)], mine)
        b_o[p] = jnp.where(p < query_out_r, query, o.astype(jnp.bfloat16))
        b_e[p] = e

    def assemble_left(p):
        k = jnp.maximum(p - out_base_l, 0)
        at = jnp.clip(k + LAG + in_base_l, 0, top)
        t = when(k, jnp.logical_not(left_late))
        o, e = join(po[t], pe[t], lc_o[at], lc_e[at], has_right)
        came = (query_in_l > 0) & (p >= LAG) & (p < LAG + query_in_l)
        mine = own_query(jnp.where((query_in_l == 0) | (p < LAG), p, p - query_in_l))
        query = jnp.where(came, lc_o[jnp.clip(p - LAG, 0, top)], mine)
        d_o[p] = jnp.where(p < query_out_l, query, o.astype(jnp.bfloat16))
        d_e[p] = e

    def compute(t):
        i = t - skip
        is_own = t >= foreign
        from_late = jnp.where(i < 2 * both, i % 2 == 0, left_late == (query_in_l > query_in_r)) & (i >= 0)
        side = (from_late == left_late).astype(jnp.int32)
        index = jnp.where(i < 0, t, skip + jnp.where(i < 2 * both, i // 2, i - both))
        index = jnp.clip(index, 0, top)
        home, rank = resolve(index, side)
        home = jnp.where(is_own, z, home)
        own_rank = jnp.clip(t - foreign, 0, seq_dev * parts - 1)
        rank = jnp.where(is_own, own_rank, rank)
        seq = slot_seq[jnp.minimum(start_tab[home] + rank // parts, slots - 1)]
        k = (rank % parts) // parts_head
        query = jnp.where(side == 0, la_o[index], lc_o[index])
        query = jnp.where(is_own, own_query(own_rank), query)
        blocks = pages_of(seq, k, each)
        local = jnp.clip(seq - first_seq, 0, seq_dev - 1)
        head = core * heads + k
        blocks.append((fresh[local, 0, head], fresh[local, 1, head], causal & is_own))
        o, e = attend(query, blocks)
        po[t] = o
        pe[t] = e

    few = min(each, -(-DEC_MAXP // owners))

    def compute_decode(i):
        d, k = i // heads, i % heads
        seq = rest_seq[d]
        local = jnp.clip(seq - first_seq, 0, seq_dev - 1)
        at_home = (seq // seq_dev == z).astype(jnp.int32)
        mine = (dec_of == d) & (dec_head == k)
        blocks = pages_of(seq, k, few)
        head = core * heads + k
        blocks.append((fresh[local, 0, head][:ROWS16], fresh[local, 1, head][:ROWS16], dec_fresh < at_home))
        o, e = attend(dec_all[...], blocks)
        dec_o[...] = jnp.where(mine, o, dec_o[...])
        dec_e[...] = jnp.where(mine, e, dec_e[...])

    top_row = lax.broadcasted_iota(jnp.int32, (rows, 1), 0) == 0

    def share(j, side):
        part = out.at[j, :, pl.ds(pl.multiple_of(side * width, width), width)]
        return pltpu.make_async_remote_copy(
            src_ref=part, dst_ref=part, send_sem=outs_sem.at[j], recv_sem=outr_sem.at[j],
            device_id={"sub": other}, device_id_type=MESH,
        )

    def finish(j):
        seq = first_seq + j
        chosen = flags[seq] == 1
        slot = slot_of[seq]
        for c in range(parts):
            rank = jnp.maximum((slot - my_start) * parts + c, 0)
            t = jnp.minimum(foreign + rank, work - 1)
            to_left = jnp.where((query_in_l == 0) | (rank < LAG), rank, rank + query_in_l)
            to_right = jnp.where((query_in_r == 0) | (rank < LAG), rank, rank + query_in_r)
            at_a = jnp.clip(to_left + in_base_r, 0, top)
            at_c = jnp.clip(to_right + in_base_l, 0, top)
            o, e = join(po[t], pe[t], la_o[at_a], la_e[at_a], has_left)
            o, e = join(o, e, lc_o[at_c], lc_e[at_c], has_right)
            turned = o.T
            for g in range(groups_part):
                h = c * groups_part + g
                line_at = h * rests + rest_of[seq]
                line = jnp.where(top_row, dec_fin[pl.ds(line_at, 1), :], 0.0)
                tile = jnp.where(chosen, turned[g * rows : (g + 1) * rows], line)
                place = pl.multiple_of(core * width + h * HD, HD)
                out[j, :, pl.ds(place, HD)] = tile.astype(out.dtype)
        share(j, core).start()

    middle = has_left & has_right

    def step(s, carry):
        p, w = s - LAG * z, s - LAG * (n - 1 - z)
        t, d, r = s - LAG, s - reach, s - LAG

        @pl.when(has_left & (p == 0))
        def _():
            right_dq().wait_recv()

        @pl.when(has_right & (p == 0))
        def _():
            dqb[...] = jnp.where(dec_home == z, dec_own[...], dqa[...])
            right_dq().start()

        @pl.when(has_right & (w == 0))
        def _():
            left_dq().wait_recv()

        @pl.when(has_left & (w == 0))
        def _():
            dqd[...] = jnp.where(dec_home == z, dec_own[...], dqc[...])
            left_dq().start()

        @pl.when((r >= 0) & (r < in_r))
        def _():
            for x in right(r):
                x.wait_recv()
            la_o[r] = a_o[r]
            la_e[r] = a_e[r]

        @pl.when(jnp.logical_not(has_left) & (r >= 0) & (r < in_l))
        def _():
            for x in left(r):
                x.wait_recv()
            lc_o[r] = c_o[r]
            lc_e[r] = c_e[r]

        @pl.when(jnp.logical_not(middle) & (t == 0))
        def _():
            for x in kv_own:
                x.wait()
            for x in kv_far:
                x.wait_recv()
            small[3].wait()

        @pl.when(jnp.logical_not(middle) & (t >= 0) & (t < work))
        def _():
            compute(t)

        @pl.when(s < out_r)
        def _():
            assemble_right(s)
            for x in right(s):
                x.start()

        @pl.when(has_left & (r >= 0) & (r < in_l))
        def _():
            for x in left(r):
                x.wait_recv()
            lc_o[r] = c_o[r]
            lc_e[r] = c_e[r]

        @pl.when(s < out_l)
        def _():
            assemble_left(s)
            for x in left(s):
                x.start()

        @pl.when(has_left & (p == dec_at))
        def _():
            for x in right_do():
                x.wait_recv()

        @pl.when(has_right & (p == dec_at))
        def _():
            o, e = join(dec_o[...], dec_e[...], doa[...], dea[...], has_left)
            dob[...] = o.astype(jnp.bfloat16)
            deb[...] = e
            for x in right_do():
                x.start()

        @pl.when(has_right & (w == dec_at))
        def _():
            for x in left_do():
                x.wait_recv()

        @pl.when(has_left & (w == dec_at))
        def _():
            o, e = join(dec_o[...], dec_e[...], doc[...], dec[...], has_right)
            dod[...] = o.astype(jnp.bfloat16)
            ded[...] = e
            for x in left_do():
                x.start()

        @pl.when(middle & (t == 0))
        def _():
            for x in kv_own:
                x.wait()
            for x in kv_far:
                x.wait_recv()
            small[3].wait()

        @pl.when((t >= 0) & (t < seq_dev))
        def _():
            for i in range(2):
                for h in range(2 * heads):
                    fresh[t, i, h] = new_kv[t, :, i, h * HD : (h + 1) * HD]

        @pl.when(middle & (t >= 0) & (t < work))
        def _():
            compute(t)

        @pl.when(d == 0)
        def _():
            dec_all[...] = jnp.where(dec_home < z, dqa[...], jnp.where(dec_home == z, dec_own[...], dqc[...]))

        @pl.when((d >= 0) & (d < rests * heads))
        def _():
            compute_decode(d)

        @pl.when(s == dec_done)
        def _():
            o, e = join(dec_o[...], dec_e[...], doa[...], dea[...], has_left)
            o, e = join(o, e, doc[...], dec[...], has_right)
            dec_fin[...] = o.T

        @pl.when(functools.reduce(jnp.logical_or, [s == at for at in ready]))
        def _():
            finish(sum((s > at).astype(jnp.int32) for at in ready[:-1]))

        return carry

    steps = max(max(lengths) + LAG, work + LAG, dec_done + 1, ready[-1] + 1)
    lax.fori_loop(0, steps, step, 0)


    def drain_right(p, carry):
        for x in right(p):
            x.wait_send()
        return carry

    def drain_left(p, carry):
        for x in left(p):
            x.wait_send()
        return carry

    for x in kv_far:
        x.wait_send()

    lax.fori_loop(0, out_r, drain_right, 0)
    lax.fori_loop(0, out_l, drain_left, 0)

    @pl.when(has_right)
    def _():
        right_dq().wait_send()
        for x in right_do():
            x.wait_send()

    @pl.when(has_left)
    def _():
        left_dq().wait_send()
        for x in left_do():
            x.wait_send()

    def drain_out(j, carry):
        share(j, core).wait_send()
        share(j, other).wait_recv()
        return carry

    lax.fori_loop(0, seq_dev, drain_out, 0)


def fused_attention(queries, new_kv, kv_pages, page_table, cached_len, is_prefill):
    n = lax.axis_size("seq")
    sub_count = lax.axis_size("sub")
    seq_dev, rows, query_width = queries.shape
    pages_dev, kv_width = kv_pages.shape[0], kv_pages.shape[3]
    seqs = page_table.shape[0]
    slots = seqs // 2
    group_size = query_width // kv_width
    heads_all = kv_width // HD
    heads = heads_all // sub_count
    width = query_width // sub_count
    parts = heads * group_size * rows // LANES
    lengths, work, ready = stream_lengths(n, seq_dev, slots, parts)
    count = max(lengths)
    bf, f32 = jnp.bfloat16, jnp.float32
    dec = heads * group_size * (seqs - slots)

    def data(c, lanes=LANES):
        return pltpu.VMEM((c, HD, lanes), bf)

    def stat(c, lanes=LANES):
        return pltpu.VMEM((c, 1, lanes), f32)

    dma = pltpu.SemaphoreType.DMA
    scratch = [
        pltpu.SMEM(page_table.shape, jnp.int32),
        pltpu.SMEM(cached_len.shape, jnp.int32),
        pltpu.SMEM(is_prefill.shape, jnp.int32),
        pltpu.VMEM(new_kv.shape, bf),
        pltpu.VMEM((2, heads, pages_dev, 2, PAGE, HD), bf),
        pltpu.VMEM((seq_dev, rows, width), bf),
        data(seq_dev * parts),
        pltpu.VMEM((seq_dev, 2, heads_all, rows, HD), bf),
        pltpu.VMEM((seqs - slots, width), f32),
        pltpu.VMEM((HD, dec), bf),
        pltpu.VMEM((HD, dec), bf),
        pltpu.VMEM((HD, dec), f32),
        pltpu.VMEM((1, dec), f32),
        pltpu.VMEM((dec, HD), f32),
    ]
    scratch += [data(count), stat(count)] * 6
    scratch += [pltpu.VMEM((work, HD, LANES), f32), stat(work)]
    scratch += [pltpu.VMEM((HD, dec), bf)] * 4
    scratch += [pltpu.VMEM((HD, dec), bf), pltpu.VMEM((1, dec), f32)] * 4
    scratch += [pltpu.SMEM((slots,), jnp.int32), pltpu.SMEM((seqs - slots,), jnp.int32)]
    scratch += [pltpu.SMEM((seqs,), jnp.int32)] * 2
    scratch += [pltpu.SMEM((n,), jnp.int32)] * 2 + [pltpu.SMEM((2 * n,), jnp.int32)]
    scratch += [dma((4,)), dma((seq_dev,)), dma((heads,)), dma((heads,)), dma((heads,))] + [dma((seq_dev,))] * 2
    scratch += [dma((count,))] * 8 + [dma((6,))] * 2
    operands = (page_table, cached_len, is_prefill, queries, new_kv, kv_pages)
    return pl.pallas_call(
        functools.partial(fused_kernel, n, lengths, work, ready, heads, group_size, rows, seq_dev, pages_dev),
        out_shape=jax.ShapeDtypeStruct(queries.shape, queries.dtype),
        in_specs=[pl.BlockSpec(memory_space=pltpu.HBM)] * 6,
        out_specs=pl.BlockSpec(memory_space=pltpu.VMEM),
        scratch_shapes=scratch,
        compiler_params=pltpu.CompilerParams(
            collective_id=0, has_side_effects=True, vmem_limit_bytes=48 * 1024 * 1024
        ),
        name="paged_attention",
    )(*[pltpu.with_memory_space_constraint(x, pltpu.HBM) for x in operands])


def per_device(queries, new_kv, kv_pages, page_table, cached_len, is_prefill):
    owners = lax.axis_size("seq") * lax.axis_size("sub")
    if page_table.shape[1] >= owners:
        return fused_attention(queries, new_kv, kv_pages, page_table, cached_len, is_prefill)
    return exchange_pages(queries, new_kv, kv_pages, page_table, cached_len, is_prefill)


def solution(mesh):
    placed = (
        P(("groups", "seq"), None, "head"),
        P(("groups", "seq"), None, None, "head"),
        P(("groups", "seq", "sub"), None, None, "head"),
        P("groups", None),
        P("groups"),
        P("groups"),
    )
    return jax.shard_map(
        per_device,
        mesh=mesh,
        in_specs=placed,
        out_specs=P(("groups", "seq"), None, "head"),
        check_vma=False,
    )
```

```python
import functools
import itertools

import jax
import jax.numpy as jnp
from jax import lax
from jax.experimental import pallas as pl
from jax.experimental.pallas import tpu as pltpu
from jax.sharding import PartitionSpec as P

HD = 128
PAGE = 128


NEG_FILL = -1e30


def partial_softmax(
    query_heads, cache_keys, cache_values, cache_valid, fresh_keys, fresh_values, fresh_valid
):
    score_scale = HD ** (-0.5)
    cache_scores = (
        jnp.einsum("rkgd,nkd->kgrn", query_heads, cache_keys, preferred_element_type=jnp.float32)
        * score_scale
    )
    fresh_scores = (
        jnp.einsum("rkgd,jkd->kgrj", query_heads, fresh_keys, preferred_element_type=jnp.float32)
        * score_scale
    )
    cache_mask = cache_valid[None, None, None, :]
    fresh_mask = fresh_valid[None, None, :, :]
    peak = jnp.maximum(
        jnp.max(jnp.where(cache_mask, cache_scores, NEG_FILL), axis=-1),
        jnp.max(jnp.where(fresh_mask, fresh_scores, NEG_FILL), axis=-1),
    )
    cache_weights = jnp.where(cache_mask, jnp.exp(cache_scores - peak[..., None]), 0.0)
    fresh_weights = jnp.where(fresh_mask, jnp.exp(fresh_scores - peak[..., None]), 0.0)
    weight_sum = jnp.sum(cache_weights, axis=-1) + jnp.sum(fresh_weights, axis=-1)
    numerator = jnp.einsum(
        "kgrn,nkd->kgrd",
        cache_weights.astype(jnp.bfloat16),
        cache_values,
        preferred_element_type=jnp.float32,
    )
    numerator = numerator + jnp.einsum(
        "kgrj,jkd->kgrd",
        fresh_weights.astype(jnp.bfloat16),
        fresh_values,
        preferred_element_type=jnp.float32,
    )
    return (peak, weight_sum, numerator)


def attend_all(
    query_block, fresh_block, received, fetch_index, page_here, lengths, live_rows, causal, fresh_on
):
    kv_width = received.shape[-1]
    heads_kv = kv_width // HD
    row_count = query_block.shape[1]
    group_size = query_block.shape[2] // kv_width
    page_count = fetch_index.shape[1]
    positions = jnp.arange(page_count * PAGE, dtype=jnp.int32)

    def one_sequence(inputs):
        query_rows, fresh_rows, index_row, here_row, length, live_row = inputs
        fetched = jnp.take(received, index_row, axis=0)
        cache_keys = fetched[:, 0].reshape(page_count * PAGE, heads_kv, HD)
        cache_values = fetched[:, 1].reshape(page_count * PAGE, heads_kv, HD)
        page_mask = jnp.broadcast_to(here_row[:, None], (page_count, PAGE)).reshape(
            page_count * PAGE
        )
        cache_valid = page_mask & (positions < length)
        query_heads = query_rows.reshape(row_count, heads_kv, group_size, HD)
        fresh_keys = fresh_rows[:, 0].reshape(row_count, heads_kv, HD)
        fresh_values = fresh_rows[:, 1].reshape(row_count, heads_kv, HD)
        fresh_valid = causal & live_row[:, None] & fresh_on
        return partial_softmax(
            query_heads,
            cache_keys,
            cache_values,
            cache_valid,
            fresh_keys,
            fresh_values,
            fresh_valid,
        )

    return lax.map(
        one_sequence, (query_block, fresh_block, fetch_index, page_here, lengths, live_rows)
    )


def finish(weight_sum, numerator, live_rows):
    unused_rows = 1.0 - live_rows.astype(jnp.float32)
    attended = numerator / (weight_sum + unused_rows[:, None, None, :])[..., None]
    attended = jnp.where(live_rows[:, None, None, :, None], attended, 0.0)
    seq_dev, heads_kv, group_size, row_count, head_dim = attended.shape
    return (
        jnp.transpose(attended, (0, 3, 1, 2, 4))
        .reshape(seq_dev, row_count, heads_kv * group_size * head_dim)
        .astype(jnp.bfloat16)
    )


def exchange_pages(queries, new_kv, kv_pages, page_table, cached_len, is_prefill):
    seq_shards = lax.axis_size("seq")
    sub_count = lax.axis_size("sub")
    owners = seq_shards * sub_count
    seq_index = lax.axis_index("seq")
    core_index = lax.axis_index("sub")
    owner_self = seq_index * sub_count + core_index
    seq_dev, row_count, query_width = queries.shape
    pages_dev = kv_pages.shape[0]
    kv_width = kv_pages.shape[3]
    page_count = page_table.shape[1]
    entries = seq_dev * page_count
    capacity = (entries + owners - 1) // owners
    table_rows = page_table.reshape(seq_shards, entries)
    holder = jnp.where(table_rows >= 0, table_rows // pages_dev, -1)
    slot_of = jnp.where(table_rows >= 0, table_rows % pages_dev, 0)
    owned_here = holder == owner_self
    rank_among = jnp.cumsum(owned_here.astype(jnp.int32), axis=1) - 1
    picked = owned_here[:, :, None] & (
        rank_among[:, :, None] == jnp.arange(capacity, dtype=jnp.int32)[None, None, :]
    )
    send_slots = jnp.sum(jnp.where(picked, slot_of[:, :, None], 0), axis=1).reshape(
        seq_shards * capacity
    )
    first_seq = seq_index * seq_dev
    my_table = lax.dynamic_slice_in_dim(page_table, first_seq, seq_dev, 0)
    my_lengths = lax.dynamic_slice_in_dim(cached_len, first_seq, seq_dev, 0)
    my_flags = lax.dynamic_slice_in_dim(is_prefill, first_seq, seq_dev, 0)
    flat_table = my_table.reshape(entries)
    my_holder = jnp.where(flat_table >= 0, flat_table // pages_dev, -1)
    entry_order = jnp.arange(entries, dtype=jnp.int32)
    earlier = (my_holder[:, None] == my_holder[None, :]) & (
        entry_order[None, :] < entry_order[:, None]
    )
    my_rank = jnp.sum(earlier.astype(jnp.int32), axis=1)
    row_ids = jnp.arange(row_count, dtype=jnp.int32)
    live_rows = (my_flags[:, None] == 1) | (row_ids[None, :] == 0)
    causal = row_ids[None, :] <= row_ids[:, None]
    part_width = kv_width // sub_count
    split_pages = kv_pages.reshape(pages_dev, 2, PAGE, sub_count, part_width)
    chosen = jnp.take(split_pages, send_slots, axis=0).reshape(
        seq_shards, capacity, 2, PAGE, sub_count, part_width
    )
    outgoing = jnp.moveaxis(chosen, 4, 1).reshape(owners, capacity, 2, PAGE, part_width)
    received = lax.all_to_all(
        outgoing, ("seq", "sub"), split_axis=0, concat_axis=0, tiled=True
    ).reshape(owners * capacity, 2, PAGE, part_width)
    present = flat_table >= 0
    fetch_index = jnp.where(present, my_holder * capacity + my_rank, 0)
    query_part = query_width // sub_count
    my_queries = lax.dynamic_slice_in_dim(queries, core_index * query_part, query_part, 2)
    my_fresh = lax.dynamic_slice_in_dim(new_kv, core_index * part_width, part_width, 3)
    peak, weight_sum, numerator = attend_all(
        my_queries,
        my_fresh,
        received,
        fetch_index.reshape(seq_dev, page_count),
        present.reshape(seq_dev, page_count),
        my_lengths,
        live_rows,
        causal,
        core_index >= 0,
    )
    own_heads = finish(weight_sum, numerator, live_rows)
    return lax.all_gather(own_heads, "sub", axis=2, tiled=True)


MESH = pl.DeviceIdType.MESH
SCALE = HD ** (-0.5)
LOG2E = 1.4426950408889634
DEC_MAXP = 4
LANES = 256
LAG = 3
ROWS16 = 16


def hi(a, b):
    return max(a, b) if isinstance(a, int) and isinstance(b, int) else jnp.maximum(a, b)


def lo(a, b):
    return min(a, b) if isinstance(a, int) and isinstance(b, int) else jnp.minimum(a, b)


def sel(c, a, b):
    return (a if c else b) if isinstance(c, bool) else jnp.where(c, a, b)


def query_spans(own):
    spans, leads, span, lead = [], [], 0, 0
    for count in own:
        lead = sel(count > 0, 0, LAG + lead)
        span = sel(span == 0, count, LAG + span + hi(count - LAG, 0))
        spans.append(span)
        leads.append(lead)
    return spans, leads


def work_order(ahead, lead_a, behind, lead_b):
    a, b = sel(ahead == 0, 0, lead_a), sel(behind == 0, 0, lead_b)
    swap = b >= a
    early, late = sel(swap, ahead, behind), sel(swap, behind, ahead)
    skip = lo(sel(swap, b - a, a - b), early)
    both = hi(lo(early - skip, late - skip), 0)
    delay = sel(b > a, sel(late - skip > both, both, hi(both - 1, 0)), both)
    return swap, skip, both, early + late - skip, delay


def chip_order(own, z):
    n = len(own)
    spans, leads = query_spans(own)
    back, back_leads = query_spans(own[::-1])
    ahead = (spans[z - 1], leads[z - 1]) if z else (0, 0)
    behind = (back[n - 2 - z], back_leads[n - 2 - z]) if z < n - 1 else (0, 0)
    return work_order(*ahead, *behind)


def stream_plan(own):
    n = len(own)
    spans, _ = query_spans(own)
    back, back_leads = query_spans(own[::-1])
    bases, base = [], 0
    for z in range(n - 1):
        clear = hi(spans[z] - back_leads[n - 2 - z], chip_order(own, z)[4] + LAG + (1 if z else 0))
        base = hi(base, clear)
        bases.append(base)
        base = base + 2 * LAG
    return spans, bases


def stream_lengths(n, seq_dev, slots, parts):
    lengths, work, ready = [0] * (n - 1), 0, [0] * seq_dev
    for counts in itertools.product(range(seq_dev + 1), repeat=n):
        if sum(counts) != slots or max(counts) != seq_dev:
            continue
        own = [parts * c for c in counts]
        spans, bases = stream_plan(own)
        back, back_bases = stream_plan(own[::-1])
        for z in range(n):
            ahead, behind = (spans[z - 1] if z else 0), (back[n - 2 - z] if z < n - 1 else 0)
            foreign = chip_order(own, z)[3]
            for k in range(own[z]):
                done = [LAG + 1 + foreign + k]
                if z:
                    done.append(LAG + bases[z - 1] + (k if behind == 0 or k < LAG else k + behind))
                if z < n - 1:
                    done.append(LAG + back_bases[n - 2 - z] + (k if ahead == 0 or k < LAG else k + ahead))
                for j in range(k // parts, seq_dev):
                    ready[j] = max(ready[j], *done)
            work = max(work, chip_order(own, z)[3] + own[z])
            if z < n - 1:
                lengths[z] = max(lengths[z], spans[z], bases[z] + behind if behind else 0)
    for j in range(1, seq_dev):
        ready[j] = max(ready[j], ready[j - 1] + 1)
    return lengths, work, ready


def pick(values, z):
    found = 0
    for j, value in enumerate(values):
        found = found + jnp.where(z == j, value, 0)
    return found


def merge(o1, e1, o2, e2):
    top = jnp.maximum(e1, e2)
    w1, w2 = jnp.exp(e1 - top), jnp.exp(e2 - top)
    total = w1 + w2
    inv = 1.0 / total
    return o1 * (w1 * inv) + o2 * (w2 * inv), top + jnp.log(total)


def attend(query, blocks):
    scored = []
    for keys, _, mask in blocks:
        s = lax.dot_general(keys, query, (((1,), (0,)), ((), ())), preferred_element_type=jnp.float32)
        scored.append(jnp.where(mask, s, NEG_FILL))
    peak = functools.reduce(jnp.maximum, [jnp.max(s, axis=0, keepdims=True) for s in scored])
    peak = jnp.maximum(peak, 0.1 * NEG_FILL)
    acc, total = None, None
    for s, (_, values, _) in zip(scored, blocks):
        weights = jnp.exp2((s - peak) * (SCALE * LOG2E))
        part = jnp.sum(weights, axis=0, keepdims=True)
        prod = lax.dot_general(
            values, weights.astype(jnp.bfloat16), (((0,), (0,)), ((), ())), preferred_element_type=jnp.float32
        )
        acc = prod if acc is None else acc + prod
        total = part if total is None else total + part
    empty = total == 0.0
    total = jnp.where(empty, 1.0, total)
    return acc * (1.0 / total), jnp.where(empty, NEG_FILL, peak * SCALE + jnp.log(total))


def fused_kernel(
    n, lengths, work, ready, heads, group_size, rows, seq_dev, pages_dev,
    table_hbm, cached_hbm, flags_hbm, q_hbm, new_hbm, kv_hbm, out,
    table, cached, flags, new_kv,
    kv, q_vm, own_t, fresh, dec_rows, dec_own, dec_all, dec_o, dec_e, dec_fin,
    a_o, a_e, b_o, b_e, c_o, c_e, d_o, d_e, la_o, la_e, lc_o, lc_e, po, pe,
    dqa, dqb, dqc, dqd, doa, dea, dob, deb, doc, dec, dod, ded,
    slot_seq, rest_seq, slot_of, rest_of, own_tab, start_tab, in_tab,
    in_sem, q_sem, kv_sem, kvs_sem, kvr_sem, outs_sem, outr_sem,
    bs, br, bes, ber, ds, dr, des, der, xs, xr,
):
    z, core = lax.axis_index("seq"), lax.axis_index("sub")
    other = 1 - core
    has_left, has_right = z > 0, z < n - 1
    seqs, page_count = table.shape
    owners = 2 * n
    each = page_count // owners
    slots = seqs // 2
    rests = seqs - slots
    width = q_vm.shape[2]
    groups_part = LANES // rows
    parts_head = group_size // groups_part
    parts = heads * parts_head
    first_seq = z * seq_dev
    head_lanes = group_size * rests
    dec_lanes = heads * head_lanes

    barrier = pltpu.get_barrier_semaphore()

    @pl.when(has_left)
    def _():
        pl.semaphore_signal(barrier, inc=1, device_id={"seq": z - 1}, device_id_type=MESH)

    @pl.when(has_right)
    def _():
        pl.semaphore_signal(barrier, inc=1, device_id={"seq": z + 1}, device_id_type=MESH)

    pl.semaphore_signal(barrier, inc=1, device_id={"sub": other}, device_id_type=MESH)

    small = [
        pltpu.make_async_copy(src, dst, in_sem.at[i])
        for i, (src, dst) in enumerate(
            ((table_hbm, table), (cached_hbm, cached), (flags_hbm, flags), (new_hbm, new_kv))
        )
    ]
    for x in small[:3]:
        x.start()
    q_copy = [
        pltpu.make_async_copy(
            q_hbm.at[j, :, pl.ds(pl.multiple_of(core * width, width), width)], q_vm.at[j], q_sem.at[j]
        )
        for j in range(seq_dev)
    ]
    for x in q_copy:
        x.start()

    def kv_cols(side, k):
        return kv_hbm.at[:, :, :, pl.ds(pl.multiple_of((side * heads + k) * HD, HD), HD)]

    kv_own = [pltpu.make_async_copy(kv_cols(core, k), kv.at[0, k], kv_sem.at[k]) for k in range(heads)]
    kv_far = [
        pltpu.make_async_remote_copy(
            src_ref=kv_cols(other, k), dst_ref=kv.at[1, k], send_sem=kvs_sem.at[k], recv_sem=kvr_sem.at[k],
            device_id={"sub": other}, device_id_type=MESH,
        )
        for k in range(heads)
    ]

    for x in small[:3]:
        x.wait()
    count, cum, own, before = 0, [], [], 0
    for j in range(seqs):
        count = count + flags[j]
        cum.append(count)
        slot_of[j] = jnp.clip(count - 1, 0, slots - 1)
        rest_of[j] = jnp.clip(j - count, 0, rests - 1)
        if j % seq_dev == seq_dev - 1:
            start_tab[j // seq_dev] = before
            own.append((count - before) * parts)
            own_tab[j // seq_dev] = own[-1]
            before = count
    for i in range(slots):
        slot_seq[i] = jnp.minimum(sum((c <= i).astype(jnp.int32) for c in cum), seqs - 1)
    for i in range(rests):
        rest_seq[i] = jnp.minimum(
            sum((j + 1 - c <= i).astype(jnp.int32) for j, c in enumerate(cum)), seqs - 1
        )
    spans_r, base_r = stream_plan(own)
    spans_l, base_l = stream_plan(own[::-1])
    ins_r, ins_l = [0] + spans_r[:-1], spans_l[::-1][1:] + [0]
    for w in range(n):
        in_tab[w] = ins_r[w]
        in_tab[n + w] = ins_l[w]
    query_in_r, query_in_l = pick(ins_r, z), pick(ins_l, z)
    query_out_r, query_out_l = pick(spans_r, z), pick(spans_l[::-1], z)
    orders = [chip_order(own, w) for w in range(n)]
    left_late = pick([jnp.asarray(x[0]).astype(jnp.int32) for x in orders], z) == 1
    skip, both, foreign = (pick([x[i] for x in orders], z) for i in (1, 2, 3))
    my_start = start_tab[z]
    out_base_r, in_base_r = pick(base_r + [0], z), pick([0] + base_r, z)
    out_base_l, in_base_l = pick(([0] + base_l[::-1]), z), pick(base_l[::-1] + [0], z)
    in_r, out_r = pick([0] + lengths, z), pick(lengths + [0], z)
    in_l, out_l = pick(lengths[::-1] + [0], z), pick([0] + lengths[::-1], z)
    top = max(lengths) - 1
    reach = LAG * jnp.maximum(z, n - 1 - z)
    dec_at = LAG * (n - 1) + rests * heads
    dec_done = dec_at + 1 + LAG * (n - 1)
    ready = [max(at, dec_done + 1 + j) for j, at in enumerate(ready)]

    def when(k, late):
        i = k - skip
        paired = skip + 2 * i + jnp.where(late, 0, 1)
        at = jnp.where(i < both, paired, skip + both + i)
        return jnp.clip(jnp.where(i < 0, k, at), 0, work - 1)

    def send(src, dst, s, r, to):
        return pltpu.make_async_remote_copy(
            src_ref=src, dst_ref=dst, send_sem=s, recv_sem=r, device_id={"seq": to}, device_id_type=MESH
        )

    def right(p):
        return (
            send(b_o.at[p], a_o.at[p], bs.at[p], br.at[p], z + 1),
            send(b_e.at[p], a_e.at[p], bes.at[p], ber.at[p], z + 1),
        )

    def left(p):
        return (
            send(d_o.at[p], c_o.at[p], ds.at[p], dr.at[p], z - 1),
            send(d_e.at[p], c_e.at[p], des.at[p], der.at[p], z - 1),
        )

    def right_dq():
        return send(dqb, dqa, xs.at[0], xr.at[0], z + 1)

    def left_dq():
        return send(dqd, dqc, xs.at[1], xr.at[1], z - 1)

    def right_do():
        return (send(dob, doa, xs.at[2], xr.at[2], z + 1), send(deb, dea, xs.at[3], xr.at[3], z + 1))

    def left_do():
        return (send(dod, doc, xs.at[4], xr.at[4], z - 1), send(ded, dec, xs.at[5], xr.at[5], z - 1))

    pl.semaphore_wait(barrier, has_left.astype(jnp.int32) + has_right.astype(jnp.int32) + 1)
    for x in kv_far:
        x.start()

    dec_lane = lax.broadcasted_iota(jnp.int32, (1, dec_lanes), 1)
    dec_of = dec_lane % rests
    dec_head = dec_lane // head_lanes
    dec_home = jnp.zeros((1, dec_lanes), jnp.int32)
    for j in range(seq_dev):
        q_copy[j].wait()
        for c in range(parts):
            stacked = jnp.concatenate(
                [q_vm[j, :, (c * groups_part + g) * HD : (c * groups_part + g + 1) * HD] for g in range(groups_part)],
                axis=0,
            )
            own_t[j * parts + c] = stacked.astype(jnp.float32).T.astype(jnp.bfloat16)
    for x in kv_own:
        x.start()
    small[3].start()
    for d in range(rests):
        dec_home = jnp.where(dec_of == d, rest_seq[d] // seq_dev, dec_home)

    dec_o[...] = jnp.zeros_like(dec_o)
    dec_e[...] = jnp.full_like(dec_e, NEG_FILL)

    key_id = lax.broadcasted_iota(jnp.int32, (PAGE, 1), 0)
    fresh_id = lax.broadcasted_iota(jnp.int32, (rows, LANES), 0)
    lane_row = lax.broadcasted_iota(jnp.int32, (rows, LANES), 1) % rows
    causal = fresh_id <= lane_row
    dec_fresh = lax.broadcasted_iota(jnp.int32, (ROWS16, 1), 0)

    def own_query(rank):
        rank = jnp.clip(rank, 0, seq_dev * parts - 1)
        slot = jnp.minimum(my_start + rank // parts, slots - 1)
        local = jnp.clip(slot_seq[slot] - first_seq, 0, seq_dev - 1)
        return own_t[local * parts + rank % parts]

    def resolve(q, side):
        w, home, rank, done = z - 1 + 2 * side, 0, 0, False
        for _ in range(n - 1):
            w = jnp.clip(w, 0, n - 1)
            ahead = in_tab[side * n + w]
            direct = (ahead == 0) | (q < jnp.minimum(own_tab[w], LAG))
            hit = direct | (q >= LAG + ahead)
            found = hit & jnp.logical_not(done)
            home = jnp.where(found, w, home)
            rank = jnp.where(found, jnp.where(direct, q, q - ahead), rank)
            done = done | hit
            q = q - LAG
            w = w + 2 * side - 1
        return home, jnp.clip(rank, 0, seq_dev * parts - 1)

    def pages_of(seq, k, few):
        found = []
        start = table[seq, 0] // pages_dev
        for side, owner in enumerate((2 * z + core, 2 * z + other)):
            place = lax.rem(owner - start + owners, owners)
            for j in range(few):
                at = place + owners * j
                valid = jnp.clip(cached[seq] - PAGE * at, 0, PAGE)
                slot = jnp.where(valid > 0, table[seq, jnp.minimum(at, page_count - 1)] - owner * pages_dev, 0)
                slot = jnp.clip(slot, 0, pages_dev - 1)
                found.append((kv[side, k, slot, 0], kv[side, k, slot, 1], key_id < valid))
        return found

    def join(o1, e1, o2, e2, present):
        o2 = jnp.where(present, o2.astype(jnp.float32), 0.0)
        return merge(o1, e1, o2, jnp.where(present, e2, NEG_FILL))

    def assemble_right(p):
        k = jnp.maximum(p - out_base_r, 0)
        at = jnp.clip(k + LAG + in_base_r, 0, top)
        t = when(k, left_late)
        o, e = join(po[t], pe[t], la_o[at], la_e[at], has_left)
        came = (query_in_r > 0) & (p >= LAG) & (p < LAG + query_in_r)
        mine = own_query(jnp.where((query_in_r == 0) | (p < LAG), p, p - query_in_r))
        query = jnp.where(came, la_o[jnp.clip(p - LAG, 0, top)], mine)
        b_o[p] = jnp.where(p < query_out_r, query, o.astype(jnp.bfloat16))
        b_e[p] = e

    def assemble_left(p):
        k = jnp.maximum(p - out_base_l, 0)
        at = jnp.clip(k + LAG + in_base_l, 0, top)
        t = when(k, jnp.logical_not(left_late))
        o, e = join(po[t], pe[t], lc_o[at], lc_e[at], has_right)
        came = (query_in_l > 0) & (p >= LAG) & (p < LAG + query_in_l)
        mine = own_query(jnp.where((query_in_l == 0) | (p < LAG), p, p - query_in_l))
        query = jnp.where(came, lc_o[jnp.clip(p - LAG, 0, top)], mine)
        d_o[p] = jnp.where(p < query_out_l, query, o.astype(jnp.bfloat16))
        d_e[p] = e

    def compute(t):
        i = t - skip
        is_own = t >= foreign
        from_late = jnp.where(i < 2 * both, i % 2 == 0, left_late == (query_in_l > query_in_r)) & (i >= 0)
        side = (from_late == left_late).astype(jnp.int32)
        index = jnp.where(i < 0, t, skip + jnp.where(i < 2 * both, i // 2, i - both))
        index = jnp.clip(index, 0, top)
        home, rank = resolve(index, side)
        home = jnp.where(is_own, z, home)
        own_rank = jnp.clip(t - foreign, 0, seq_dev * parts - 1)
        rank = jnp.where(is_own, own_rank, rank)
        seq = slot_seq[jnp.minimum(start_tab[home] + rank // parts, slots - 1)]
        k = (rank % parts) // parts_head
        query = jnp.where(side == 0, la_o[index], lc_o[index])
        query = jnp.where(is_own, own_query(own_rank), query)
        blocks = pages_of(seq, k, each)
        local = jnp.clip(seq - first_seq, 0, seq_dev - 1)
        head = core * heads + k
        blocks.append((fresh[local, 0, head], fresh[local, 1, head], causal & is_own))
        o, e = attend(query, blocks)
        po[t] = o
        pe[t] = e

    few = min(each, -(-DEC_MAXP // owners))

    def compute_decode(i):
        d, k = i // heads, i % heads
        seq = rest_seq[d]
        local = jnp.clip(seq - first_seq, 0, seq_dev - 1)
        at_home = (seq // seq_dev == z).astype(jnp.int32)
        mine = (dec_of == d) & (dec_head == k)
        blocks = pages_of(seq, k, few)
        head = core * heads + k
        blocks.append((fresh[local, 0, head][:ROWS16], fresh[local, 1, head][:ROWS16], dec_fresh < at_home))
        o, e = attend(dec_all[...], blocks)
        dec_o[...] = jnp.where(mine, o, dec_o[...])
        dec_e[...] = jnp.where(mine, e, dec_e[...])

    top_row = lax.broadcasted_iota(jnp.int32, (rows, 1), 0) == 0

    def share(j, side):
        part = out.at[j, :, pl.ds(pl.multiple_of(side * width, width), width)]
        return pltpu.make_async_remote_copy(
            src_ref=part, dst_ref=part, send_sem=outs_sem.at[j], recv_sem=outr_sem.at[j],
            device_id={"sub": other}, device_id_type=MESH,
        )

    def finish(j):
        seq = first_seq + j
        chosen = flags[seq] == 1
        slot = slot_of[seq]
        for c in range(parts):
            rank = jnp.maximum((slot - my_start) * parts + c, 0)
            t = jnp.minimum(foreign + rank, work - 1)
            to_left = jnp.where((query_in_l == 0) | (rank < LAG), rank, rank + query_in_l)
            to_right = jnp.where((query_in_r == 0) | (rank < LAG), rank, rank + query_in_r)
            at_a = jnp.clip(to_left + in_base_r, 0, top)
            at_c = jnp.clip(to_right + in_base_l, 0, top)
            o, e = join(po[t], pe[t], la_o[at_a], la_e[at_a], has_left)
            o, e = join(o, e, lc_o[at_c], lc_e[at_c], has_right)
            turned = o.T
            for g in range(groups_part):
                h = c * groups_part + g
                line_at = h * rests + rest_of[seq]
                line = jnp.where(top_row, dec_fin[pl.ds(line_at, 1), :], 0.0)
                tile = jnp.where(chosen, turned[g * rows : (g + 1) * rows], line)
                place = pl.multiple_of(core * width + h * HD, HD)
                out[j, :, pl.ds(place, HD)] = tile.astype(out.dtype)
        share(j, core).start()

    middle = has_left & has_right

    def step(s, carry):
        p, w = s - 1 - LAG * z, s - 1 - LAG * (n - 1 - z)
        t, d, r = s - LAG, s - 1 - reach, s - LAG

        @pl.when(has_left & (p == 0))
        def _():
            right_dq().wait_recv()

        @pl.when(has_right & (p == 0))
        def _():
            dqb[...] = jnp.where(dec_home == z, dec_own[...], dqa[...])
            right_dq().start()

        @pl.when(has_right & (w == 0))
        def _():
            left_dq().wait_recv()

        @pl.when(has_left & (w == 0))
        def _():
            dqd[...] = jnp.where(dec_home == z, dec_own[...], dqc[...])
            left_dq().start()

        @pl.when((r >= 0) & (r < in_r))
        def _():
            for x in right(r):
                x.wait_recv()
            la_o[r] = a_o[r]
            la_e[r] = a_e[r]

        @pl.when(jnp.logical_not(has_left) & (r >= 0) & (r < in_l))
        def _():
            for x in left(r):
                x.wait_recv()
            lc_o[r] = c_o[r]
            lc_e[r] = c_e[r]

        @pl.when(jnp.logical_not(middle) & (t == 0))
        def _():
            for x in kv_own:
                x.wait()
            for x in kv_far:
                x.wait_recv()

        @pl.when(jnp.logical_not(middle) & (t >= 0) & (t < work))
        def _():
            compute(t)

        @pl.when(s < out_r)
        def _():
            assemble_right(s)
            for x in right(s):
                x.start()

        @pl.when(has_left & (r >= 0) & (r < in_l))
        def _():
            for x in left(r):
                x.wait_recv()
            lc_o[r] = c_o[r]
            lc_e[r] = c_e[r]

        @pl.when(s < out_l)
        def _():
            assemble_left(s)
            for x in left(s):
                x.start()

        @pl.when(has_left & (p == dec_at))
        def _():
            for x in right_do():
                x.wait_recv()

        @pl.when(has_right & (p == dec_at))
        def _():
            o, e = join(dec_o[...], dec_e[...], doa[...], dea[...], has_left)
            dob[...] = o.astype(jnp.bfloat16)
            deb[...] = e
            for x in right_do():
                x.start()

        @pl.when(has_right & (w == dec_at))
        def _():
            for x in left_do():
                x.wait_recv()

        @pl.when(has_left & (w == dec_at))
        def _():
            o, e = join(dec_o[...], dec_e[...], doc[...], dec[...], has_right)
            dod[...] = o.astype(jnp.bfloat16)
            ded[...] = e
            for x in left_do():
                x.start()

        @pl.when(middle & (t == 0))
        def _():
            for x in kv_own:
                x.wait()
            for x in kv_far:
                x.wait_recv()

        @pl.when(s == LAG - 1)
        def _():
            small[3].wait()
            for j in range(seq_dev):
                for i in range(2):
                    for h in range(2 * heads):
                        fresh[j, i, h] = new_kv[j, :, i, h * HD : (h + 1) * HD]

        @pl.when(middle & (t >= 0) & (t < work))
        def _():
            compute(t)

        @pl.when(s == 0)
        def _():
            for d in range(rests):
                local = jnp.clip(rest_seq[d] - first_seq, 0, seq_dev - 1)
                dec_rows[d : d + 1, :] = q_vm[local, 0:ROWS16, :].astype(jnp.float32)[0:1]
            stacked = jnp.concatenate(
                [dec_rows[:, h * HD : (h + 1) * HD] for h in range(heads * group_size)], axis=0
            )
            dec_own[...] = stacked.T.astype(jnp.bfloat16)

        @pl.when(d == 0)
        def _():
            dec_all[...] = jnp.where(dec_home < z, dqa[...], jnp.where(dec_home == z, dec_own[...], dqc[...]))

        @pl.when((d >= 0) & (d < rests * heads))
        def _():
            compute_decode(d)

        @pl.when(s == dec_done)
        def _():
            o, e = join(dec_o[...], dec_e[...], doa[...], dea[...], has_left)
            o, e = join(o, e, doc[...], dec[...], has_right)
            dec_fin[...] = o.T

        @pl.when(functools.reduce(jnp.logical_or, [s == at for at in ready]))
        def _():
            finish(sum((s > at).astype(jnp.int32) for at in ready[:-1]))

        return carry

    steps = max(max(lengths) + LAG, work + LAG, dec_done + 1, ready[-1] + 1)
    lax.fori_loop(0, steps, step, 0)


    def drain_right(p, carry):
        for x in right(p):
            x.wait_send()
        return carry

    def drain_left(p, carry):
        for x in left(p):
            x.wait_send()
        return carry

    for x in kv_far:
        x.wait_send()

    lax.fori_loop(0, out_r, drain_right, 0)
    lax.fori_loop(0, out_l, drain_left, 0)

    @pl.when(has_right)
    def _():
        right_dq().wait_send()
        for x in right_do():
            x.wait_send()

    @pl.when(has_left)
    def _():
        left_dq().wait_send()
        for x in left_do():
            x.wait_send()

    def drain_out(j, carry):
        share(j, core).wait_send()
        share(j, other).wait_recv()
        return carry

    lax.fori_loop(0, seq_dev, drain_out, 0)


def fused_attention(queries, new_kv, kv_pages, page_table, cached_len, is_prefill):
    n = lax.axis_size("seq")
    sub_count = lax.axis_size("sub")
    seq_dev, rows, query_width = queries.shape
    pages_dev, kv_width = kv_pages.shape[0], kv_pages.shape[3]
    seqs = page_table.shape[0]
    slots = seqs // 2
    group_size = query_width // kv_width
    heads_all = kv_width // HD
    heads = heads_all // sub_count
    width = query_width // sub_count
    parts = heads * group_size * rows // LANES
    lengths, work, ready = stream_lengths(n, seq_dev, slots, parts)
    count = max(lengths)
    bf, f32 = jnp.bfloat16, jnp.float32
    dec = heads * group_size * (seqs - slots)

    def data(c, lanes=LANES):
        return pltpu.VMEM((c, HD, lanes), bf)

    def stat(c, lanes=LANES):
        return pltpu.VMEM((c, 1, lanes), f32)

    dma = pltpu.SemaphoreType.DMA
    scratch = [
        pltpu.SMEM(page_table.shape, jnp.int32),
        pltpu.SMEM(cached_len.shape, jnp.int32),
        pltpu.SMEM(is_prefill.shape, jnp.int32),
        pltpu.VMEM(new_kv.shape, bf),
        pltpu.VMEM((2, heads, pages_dev, 2, PAGE, HD), bf),
        pltpu.VMEM((seq_dev, rows, width), bf),
        data(seq_dev * parts),
        pltpu.VMEM((seq_dev, 2, heads_all, rows, HD), bf),
        pltpu.VMEM((seqs - slots, width), f32),
        pltpu.VMEM((HD, dec), bf),
        pltpu.VMEM((HD, dec), bf),
        pltpu.VMEM((HD, dec), f32),
        pltpu.VMEM((1, dec), f32),
        pltpu.VMEM((dec, HD), f32),
    ]
    scratch += [data(count), stat(count)] * 6
    scratch += [pltpu.VMEM((work, HD, LANES), f32), stat(work)]
    scratch += [pltpu.VMEM((HD, dec), bf)] * 4
    scratch += [pltpu.VMEM((HD, dec), bf), pltpu.VMEM((1, dec), f32)] * 4
    scratch += [pltpu.SMEM((slots,), jnp.int32), pltpu.SMEM((seqs - slots,), jnp.int32)]
    scratch += [pltpu.SMEM((seqs,), jnp.int32)] * 2
    scratch += [pltpu.SMEM((n,), jnp.int32)] * 2 + [pltpu.SMEM((2 * n,), jnp.int32)]
    scratch += [dma((4,)), dma((seq_dev,)), dma((heads,)), dma((heads,)), dma((heads,))] + [dma((seq_dev,))] * 2
    scratch += [dma((count,))] * 8 + [dma((6,))] * 2
    operands = (page_table, cached_len, is_prefill, queries, new_kv, kv_pages)
    return pl.pallas_call(
        functools.partial(fused_kernel, n, lengths, work, ready, heads, group_size, rows, seq_dev, pages_dev),
        out_shape=jax.ShapeDtypeStruct(queries.shape, queries.dtype),
        in_specs=[pl.BlockSpec(memory_space=pltpu.HBM)] * 6,
        out_specs=pl.BlockSpec(memory_space=pltpu.VMEM),
        scratch_shapes=scratch,
        compiler_params=pltpu.CompilerParams(
            collective_id=0, has_side_effects=True, vmem_limit_bytes=48 * 1024 * 1024
        ),
        name="paged_attention",
    )(*[pltpu.with_memory_space_constraint(x, pltpu.HBM) for x in operands])


def per_device(queries, new_kv, kv_pages, page_table, cached_len, is_prefill):
    owners = lax.axis_size("seq") * lax.axis_size("sub")
    if page_table.shape[1] >= owners:
        return fused_attention(queries, new_kv, kv_pages, page_table, cached_len, is_prefill)
    return exchange_pages(queries, new_kv, kv_pages, page_table, cached_len, is_prefill)


def solution(mesh):
    placed = (
        P(("groups", "seq"), None, "head"),
        P(("groups", "seq"), None, None, "head"),
        P(("groups", "seq", "sub"), None, None, "head"),
        P("groups", None),
        P("groups"),
        P("groups"),
    )
    return jax.shard_map(
        per_device,
        mesh=mesh,
        in_specs=placed,
        out_specs=P(("groups", "seq"), None, "head"),
        check_vma=False,
    )
```

```python
import functools
import itertools

import jax
import jax.numpy as jnp
from jax import lax
from jax.experimental import pallas as pl
from jax.experimental.pallas import tpu as pltpu
from jax.sharding import PartitionSpec as P

HD = 128
PAGE = 128


NEG_FILL = -1e30


def partial_softmax(
    query_heads, cache_keys, cache_values, cache_valid, fresh_keys, fresh_values, fresh_valid
):
    score_scale = HD ** (-0.5)
    cache_scores = (
        jnp.einsum("rkgd,nkd->kgrn", query_heads, cache_keys, preferred_element_type=jnp.float32)
        * score_scale
    )
    fresh_scores = (
        jnp.einsum("rkgd,jkd->kgrj", query_heads, fresh_keys, preferred_element_type=jnp.float32)
        * score_scale
    )
    cache_mask = cache_valid[None, None, None, :]
    fresh_mask = fresh_valid[None, None, :, :]
    peak = jnp.maximum(
        jnp.max(jnp.where(cache_mask, cache_scores, NEG_FILL), axis=-1),
        jnp.max(jnp.where(fresh_mask, fresh_scores, NEG_FILL), axis=-1),
    )
    cache_weights = jnp.where(cache_mask, jnp.exp(cache_scores - peak[..., None]), 0.0)
    fresh_weights = jnp.where(fresh_mask, jnp.exp(fresh_scores - peak[..., None]), 0.0)
    weight_sum = jnp.sum(cache_weights, axis=-1) + jnp.sum(fresh_weights, axis=-1)
    numerator = jnp.einsum(
        "kgrn,nkd->kgrd",
        cache_weights.astype(jnp.bfloat16),
        cache_values,
        preferred_element_type=jnp.float32,
    )
    numerator = numerator + jnp.einsum(
        "kgrj,jkd->kgrd",
        fresh_weights.astype(jnp.bfloat16),
        fresh_values,
        preferred_element_type=jnp.float32,
    )
    return (peak, weight_sum, numerator)


def attend_all(
    query_block, fresh_block, received, fetch_index, page_here, lengths, live_rows, causal, fresh_on
):
    kv_width = received.shape[-1]
    heads_kv = kv_width // HD
    row_count = query_block.shape[1]
    group_size = query_block.shape[2] // kv_width
    page_count = fetch_index.shape[1]
    positions = jnp.arange(page_count * PAGE, dtype=jnp.int32)

    def one_sequence(inputs):
        query_rows, fresh_rows, index_row, here_row, length, live_row = inputs
        fetched = jnp.take(received, index_row, axis=0)
        cache_keys = fetched[:, 0].reshape(page_count * PAGE, heads_kv, HD)
        cache_values = fetched[:, 1].reshape(page_count * PAGE, heads_kv, HD)
        page_mask = jnp.broadcast_to(here_row[:, None], (page_count, PAGE)).reshape(
            page_count * PAGE
        )
        cache_valid = page_mask & (positions < length)
        query_heads = query_rows.reshape(row_count, heads_kv, group_size, HD)
        fresh_keys = fresh_rows[:, 0].reshape(row_count, heads_kv, HD)
        fresh_values = fresh_rows[:, 1].reshape(row_count, heads_kv, HD)
        fresh_valid = causal & live_row[:, None] & fresh_on
        return partial_softmax(
            query_heads,
            cache_keys,
            cache_values,
            cache_valid,
            fresh_keys,
            fresh_values,
            fresh_valid,
        )

    return lax.map(
        one_sequence, (query_block, fresh_block, fetch_index, page_here, lengths, live_rows)
    )


def finish(weight_sum, numerator, live_rows):
    unused_rows = 1.0 - live_rows.astype(jnp.float32)
    attended = numerator / (weight_sum + unused_rows[:, None, None, :])[..., None]
    attended = jnp.where(live_rows[:, None, None, :, None], attended, 0.0)
    seq_dev, heads_kv, group_size, row_count, head_dim = attended.shape
    return (
        jnp.transpose(attended, (0, 3, 1, 2, 4))
        .reshape(seq_dev, row_count, heads_kv * group_size * head_dim)
        .astype(jnp.bfloat16)
    )


def exchange_pages(queries, new_kv, kv_pages, page_table, cached_len, is_prefill):
    seq_shards = lax.axis_size("seq")
    sub_count = lax.axis_size("sub")
    owners = seq_shards * sub_count
    seq_index = lax.axis_index("seq")
    core_index = lax.axis_index("sub")
    owner_self = seq_index * sub_count + core_index
    seq_dev, row_count, query_width = queries.shape
    pages_dev = kv_pages.shape[0]
    kv_width = kv_pages.shape[3]
    page_count = page_table.shape[1]
    entries = seq_dev * page_count
    capacity = (entries + owners - 1) // owners
    table_rows = page_table.reshape(seq_shards, entries)
    holder = jnp.where(table_rows >= 0, table_rows // pages_dev, -1)
    slot_of = jnp.where(table_rows >= 0, table_rows % pages_dev, 0)
    owned_here = holder == owner_self
    rank_among = jnp.cumsum(owned_here.astype(jnp.int32), axis=1) - 1
    picked = owned_here[:, :, None] & (
        rank_among[:, :, None] == jnp.arange(capacity, dtype=jnp.int32)[None, None, :]
    )
    send_slots = jnp.sum(jnp.where(picked, slot_of[:, :, None], 0), axis=1).reshape(
        seq_shards * capacity
    )
    first_seq = seq_index * seq_dev
    my_table = lax.dynamic_slice_in_dim(page_table, first_seq, seq_dev, 0)
    my_lengths = lax.dynamic_slice_in_dim(cached_len, first_seq, seq_dev, 0)
    my_flags = lax.dynamic_slice_in_dim(is_prefill, first_seq, seq_dev, 0)
    flat_table = my_table.reshape(entries)
    my_holder = jnp.where(flat_table >= 0, flat_table // pages_dev, -1)
    entry_order = jnp.arange(entries, dtype=jnp.int32)
    earlier = (my_holder[:, None] == my_holder[None, :]) & (
        entry_order[None, :] < entry_order[:, None]
    )
    my_rank = jnp.sum(earlier.astype(jnp.int32), axis=1)
    row_ids = jnp.arange(row_count, dtype=jnp.int32)
    live_rows = (my_flags[:, None] == 1) | (row_ids[None, :] == 0)
    causal = row_ids[None, :] <= row_ids[:, None]
    part_width = kv_width // sub_count
    split_pages = kv_pages.reshape(pages_dev, 2, PAGE, sub_count, part_width)
    chosen = jnp.take(split_pages, send_slots, axis=0).reshape(
        seq_shards, capacity, 2, PAGE, sub_count, part_width
    )
    outgoing = jnp.moveaxis(chosen, 4, 1).reshape(owners, capacity, 2, PAGE, part_width)
    received = lax.all_to_all(
        outgoing, ("seq", "sub"), split_axis=0, concat_axis=0, tiled=True
    ).reshape(owners * capacity, 2, PAGE, part_width)
    present = flat_table >= 0
    fetch_index = jnp.where(present, my_holder * capacity + my_rank, 0)
    query_part = query_width // sub_count
    my_queries = lax.dynamic_slice_in_dim(queries, core_index * query_part, query_part, 2)
    my_fresh = lax.dynamic_slice_in_dim(new_kv, core_index * part_width, part_width, 3)
    peak, weight_sum, numerator = attend_all(
        my_queries,
        my_fresh,
        received,
        fetch_index.reshape(seq_dev, page_count),
        present.reshape(seq_dev, page_count),
        my_lengths,
        live_rows,
        causal,
        core_index >= 0,
    )
    own_heads = finish(weight_sum, numerator, live_rows)
    return lax.all_gather(own_heads, "sub", axis=2, tiled=True)


MESH = pl.DeviceIdType.MESH
SCALE = HD ** (-0.5)
LOG2E = 1.4426950408889634
DEC_MAXP = 4
LANES = 256
LAG = 3
ROWS16 = 16


def hi(a, b):
    return max(a, b) if isinstance(a, int) and isinstance(b, int) else jnp.maximum(a, b)


def lo(a, b):
    return min(a, b) if isinstance(a, int) and isinstance(b, int) else jnp.minimum(a, b)


def sel(c, a, b):
    return (a if c else b) if isinstance(c, bool) else jnp.where(c, a, b)


def query_spans(own):
    spans, leads, span, lead = [], [], 0, 0
    for count in own:
        lead = sel(count > 0, 0, LAG + lead)
        span = sel(span == 0, count, LAG + span + hi(count - LAG, 0))
        spans.append(span)
        leads.append(lead)
    return spans, leads


def work_order(ahead, lead_a, behind, lead_b):
    a, b = sel(ahead == 0, 0, lead_a), sel(behind == 0, 0, lead_b)
    swap = b >= a
    early, late = sel(swap, ahead, behind), sel(swap, behind, ahead)
    skip = lo(sel(swap, b - a, a - b), early)
    both = hi(lo(early - skip, late - skip), 0)
    delay = sel(b > a, sel(late - skip > both, both, hi(both - 1, 0)), both)
    return swap, skip, both, early + late - skip, delay


def chip_order(own, z):
    n = len(own)
    spans, leads = query_spans(own)
    back, back_leads = query_spans(own[::-1])
    ahead = (spans[z - 1], leads[z - 1]) if z else (0, 0)
    behind = (back[n - 2 - z], back_leads[n - 2 - z]) if z < n - 1 else (0, 0)
    return work_order(*ahead, *behind)


def stream_plan(own):
    n = len(own)
    spans, _ = query_spans(own)
    back, back_leads = query_spans(own[::-1])
    bases, base = [], 0
    for z in range(n - 1):
        clear = hi(spans[z] - back_leads[n - 2 - z], chip_order(own, z)[4] + LAG + (1 if z else 0))
        base = hi(base, clear)
        bases.append(base)
        base = base + 2 * LAG
    return spans, bases


def stream_lengths(n, seq_dev, slots, parts):
    lengths, work, ready = [0] * (n - 1), 0, [0] * seq_dev
    for counts in itertools.product(range(seq_dev + 1), repeat=n):
        if sum(counts) != slots or max(counts) != seq_dev:
            continue
        own = [parts * c for c in counts]
        spans, bases = stream_plan(own)
        back, back_bases = stream_plan(own[::-1])
        for z in range(n):
            ahead, behind = (spans[z - 1] if z else 0), (back[n - 2 - z] if z < n - 1 else 0)
            foreign = chip_order(own, z)[3]
            for k in range(own[z]):
                done = [LAG + 1 + foreign + k]
                if z:
                    done.append(LAG + bases[z - 1] + (k if behind == 0 or k < LAG else k + behind))
                if z < n - 1:
                    done.append(LAG + back_bases[n - 2 - z] + (k if ahead == 0 or k < LAG else k + ahead))
                for j in range(k // parts, seq_dev):
                    ready[j] = max(ready[j], *done)
            work = max(work, chip_order(own, z)[3] + own[z])
            if z < n - 1:
                lengths[z] = max(lengths[z], spans[z], bases[z] + behind if behind else 0)
    for j in range(1, seq_dev):
        ready[j] = max(ready[j], ready[j - 1] + 1)
    return lengths, work, ready


def pick(values, z):
    found = 0
    for j, value in enumerate(values):
        found = found + jnp.where(z == j, value, 0)
    return found


def merge(o1, e1, o2, e2):
    top = jnp.maximum(e1, e2)
    w1, w2 = jnp.exp(e1 - top), jnp.exp(e2 - top)
    total = w1 + w2
    inv = 1.0 / total
    return o1 * (w1 * inv) + o2 * (w2 * inv), top + jnp.log(total)


def attend(query, blocks):
    scored = []
    for keys, _, mask in blocks:
        s = lax.dot_general(keys, query, (((1,), (0,)), ((), ())), preferred_element_type=jnp.float32)
        scored.append(jnp.where(mask, s, NEG_FILL))
    peak = functools.reduce(jnp.maximum, [jnp.max(s, axis=0, keepdims=True) for s in scored])
    peak = jnp.maximum(peak, 0.1 * NEG_FILL)
    acc, total = None, None
    for s, (_, values, _) in zip(scored, blocks):
        weights = jnp.exp2((s - peak) * (SCALE * LOG2E))
        part = jnp.sum(weights, axis=0, keepdims=True)
        prod = lax.dot_general(
            values, weights.astype(jnp.bfloat16), (((0,), (0,)), ((), ())), preferred_element_type=jnp.float32
        )
        acc = prod if acc is None else acc + prod
        total = part if total is None else total + part
    empty = total == 0.0
    total = jnp.where(empty, 1.0, total)
    return acc * (1.0 / total), jnp.where(empty, NEG_FILL, peak * SCALE + jnp.log(total))


def fused_kernel(
    n, lengths, work, ready, heads, group_size, rows, seq_dev, pages_dev,
    table_hbm, cached_hbm, flags_hbm, q_hbm, new_hbm, kv_hbm, out,
    table, cached, flags, new_kv,
    kv, q_vm, own_t, fresh, dec_rows, dec_own, dec_all, dec_o, dec_e, dec_fin,
    a_o, a_e, b_o, b_e, c_o, c_e, d_o, d_e, la_o, la_e, lc_o, lc_e, po, pe,
    dqa, dqb, dqc, dqd, doa, dea, dob, deb, doc, dec, dod, ded,
    slot_seq, rest_seq, slot_of, rest_of, own_tab, start_tab, in_tab,
    in_sem, q_sem, kv_sem, kvs_sem, kvr_sem, outs_sem, outr_sem,
    bs, br, bes, ber, ds, dr, des, der, xs, xr,
):
    z, core = lax.axis_index("seq"), lax.axis_index("sub")
    other = 1 - core
    has_left, has_right = z > 0, z < n - 1
    seqs, page_count = table.shape
    owners = 2 * n
    each = page_count // owners
    slots = seqs // 2
    rests = seqs - slots
    width = q_vm.shape[2]
    groups_part = LANES // rows
    parts_head = group_size // groups_part
    parts = heads * parts_head
    first_seq = z * seq_dev
    head_lanes = group_size * rests
    dec_lanes = heads * head_lanes

    barrier = pltpu.get_barrier_semaphore()

    @pl.when(has_left)
    def _():
        pl.semaphore_signal(barrier, inc=1, device_id={"seq": z - 1}, device_id_type=MESH)

    @pl.when(has_right)
    def _():
        pl.semaphore_signal(barrier, inc=1, device_id={"seq": z + 1}, device_id_type=MESH)

    pl.semaphore_signal(barrier, inc=1, device_id={"sub": other}, device_id_type=MESH)

    small = [
        pltpu.make_async_copy(src, dst, in_sem.at[i])
        for i, (src, dst) in enumerate(
            ((table_hbm, table), (cached_hbm, cached), (flags_hbm, flags), (new_hbm, new_kv))
        )
    ]
    for x in small[:3]:
        x.start()
    piece = groups_part * HD

    def q_piece(c):
        src = pl.ds(pl.multiple_of(core * width + c * piece, piece), piece)
        dst = pl.ds(pl.multiple_of(c * piece, piece), piece)
        return pltpu.make_async_copy(q_hbm.at[:, :, src], q_vm.at[:, :, dst], q_sem.at[c])

    for c in range(parts):
        q_piece(c).start()

    def kv_cols(side, k):
        return kv_hbm.at[:, :, :, pl.ds(pl.multiple_of((side * heads + k) * HD, HD), HD)]

    kv_own = [pltpu.make_async_copy(kv_cols(core, k), kv.at[0, k], kv_sem.at[k]) for k in range(heads)]
    kv_far = [
        pltpu.make_async_remote_copy(
            src_ref=kv_cols(other, k), dst_ref=kv.at[1, k], send_sem=kvs_sem.at[k], recv_sem=kvr_sem.at[k],
            device_id={"sub": other}, device_id_type=MESH,
        )
        for k in range(heads)
    ]

    for x in small[:3]:
        x.wait()
    count, cum, own, before = 0, [], [], 0
    for j in range(seqs):
        count = count + flags[j]
        cum.append(count)
        slot_of[j] = jnp.clip(count - 1, 0, slots - 1)
        rest_of[j] = jnp.clip(j - count, 0, rests - 1)
        if j % seq_dev == seq_dev - 1:
            start_tab[j // seq_dev] = before
            own.append((count - before) * parts)
            own_tab[j // seq_dev] = own[-1]
            before = count
    for i in range(slots):
        slot_seq[i] = jnp.minimum(sum((c <= i).astype(jnp.int32) for c in cum), seqs - 1)
    for i in range(rests):
        rest_seq[i] = jnp.minimum(
            sum((j + 1 - c <= i).astype(jnp.int32) for j, c in enumerate(cum)), seqs - 1
        )
    spans_r, base_r = stream_plan(own)
    spans_l, base_l = stream_plan(own[::-1])
    ins_r, ins_l = [0] + spans_r[:-1], spans_l[::-1][1:] + [0]
    for w in range(n):
        in_tab[w] = ins_r[w]
        in_tab[n + w] = ins_l[w]
    query_in_r, query_in_l = pick(ins_r, z), pick(ins_l, z)
    query_out_r, query_out_l = pick(spans_r, z), pick(spans_l[::-1], z)
    orders = [chip_order(own, w) for w in range(n)]
    left_late = pick([jnp.asarray(x[0]).astype(jnp.int32) for x in orders], z) == 1
    skip, both, foreign = (pick([x[i] for x in orders], z) for i in (1, 2, 3))
    my_start = start_tab[z]
    out_base_r, in_base_r = pick(base_r + [0], z), pick([0] + base_r, z)
    out_base_l, in_base_l = pick(([0] + base_l[::-1]), z), pick(base_l[::-1] + [0], z)
    in_r, out_r = pick([0] + lengths, z), pick(lengths + [0], z)
    in_l, out_l = pick(lengths[::-1] + [0], z), pick([0] + lengths[::-1], z)
    top = max(lengths) - 1
    reach = LAG * jnp.maximum(z, n - 1 - z)
    dec_at = LAG * (n - 1) + rests * heads
    dec_done = dec_at + parts - 1 + LAG * (n - 1)
    ready = [max(at, dec_done + 1 + j) for j, at in enumerate(ready)]

    def when(k, late):
        i = k - skip
        paired = skip + 2 * i + jnp.where(late, 0, 1)
        at = jnp.where(i < both, paired, skip + both + i)
        return jnp.clip(jnp.where(i < 0, k, at), 0, work - 1)

    def send(src, dst, s, r, to):
        return pltpu.make_async_remote_copy(
            src_ref=src, dst_ref=dst, send_sem=s, recv_sem=r, device_id={"seq": to}, device_id_type=MESH
        )

    def right(p):
        return (
            send(b_o.at[p], a_o.at[p], bs.at[p], br.at[p], z + 1),
            send(b_e.at[p], a_e.at[p], bes.at[p], ber.at[p], z + 1),
        )

    def left(p):
        return (
            send(d_o.at[p], c_o.at[p], ds.at[p], dr.at[p], z - 1),
            send(d_e.at[p], c_e.at[p], des.at[p], der.at[p], z - 1),
        )

    def right_dq():
        return send(dqb, dqa, xs.at[0], xr.at[0], z + 1)

    def left_dq():
        return send(dqd, dqc, xs.at[1], xr.at[1], z - 1)

    def right_do():
        return (send(dob, doa, xs.at[2], xr.at[2], z + 1), send(deb, dea, xs.at[3], xr.at[3], z + 1))

    def left_do():
        return (send(dod, doc, xs.at[4], xr.at[4], z - 1), send(ded, dec, xs.at[5], xr.at[5], z - 1))

    pl.semaphore_wait(barrier, has_left.astype(jnp.int32) + has_right.astype(jnp.int32) + 1)
    for x in kv_far:
        x.start()

    dec_lane = lax.broadcasted_iota(jnp.int32, (1, dec_lanes), 1)
    dec_of = dec_lane % rests
    dec_head = dec_lane // head_lanes
    dec_home = jnp.zeros((1, dec_lanes), jnp.int32)
    def turn(c):
        q_piece(c).wait()
        for j in range(seq_dev):
            stacked = jnp.concatenate(
                [q_vm[j, :, pl.ds(pl.multiple_of(c * piece + g * HD, HD), HD)] for g in range(groups_part)],
                axis=0,
            )
            own_t[j * parts + c] = stacked.astype(jnp.float32).T.astype(jnp.bfloat16)

    turn(0)
    for x in kv_own:
        x.start()
    small[3].start()
    for d in range(rests):
        dec_home = jnp.where(dec_of == d, rest_seq[d] // seq_dev, dec_home)

    dec_o[...] = jnp.zeros_like(dec_o)
    dec_e[...] = jnp.full_like(dec_e, NEG_FILL)

    key_id = lax.broadcasted_iota(jnp.int32, (PAGE, 1), 0)
    fresh_id = lax.broadcasted_iota(jnp.int32, (rows, LANES), 0)
    lane_row = lax.broadcasted_iota(jnp.int32, (rows, LANES), 1) % rows
    causal = fresh_id <= lane_row
    dec_fresh = lax.broadcasted_iota(jnp.int32, (ROWS16, 1), 0)

    def own_query(rank):
        rank = jnp.clip(rank, 0, seq_dev * parts - 1)
        slot = jnp.minimum(my_start + rank // parts, slots - 1)
        local = jnp.clip(slot_seq[slot] - first_seq, 0, seq_dev - 1)
        return own_t[local * parts + rank % parts]

    def resolve(q, side):
        w, home, rank, done = z - 1 + 2 * side, 0, 0, False
        for _ in range(n - 1):
            w = jnp.clip(w, 0, n - 1)
            ahead = in_tab[side * n + w]
            direct = (ahead == 0) | (q < jnp.minimum(own_tab[w], LAG))
            hit = direct | (q >= LAG + ahead)
            found = hit & jnp.logical_not(done)
            home = jnp.where(found, w, home)
            rank = jnp.where(found, jnp.where(direct, q, q - ahead), rank)
            done = done | hit
            q = q - LAG
            w = w + 2 * side - 1
        return home, jnp.clip(rank, 0, seq_dev * parts - 1)

    def pages_of(seq, k, few):
        found = []
        start = table[seq, 0] // pages_dev
        for side, owner in enumerate((2 * z + core, 2 * z + other)):
            place = lax.rem(owner - start + owners, owners)
            for j in range(few):
                at = place + owners * j
                valid = jnp.clip(cached[seq] - PAGE * at, 0, PAGE)
                slot = jnp.where(valid > 0, table[seq, jnp.minimum(at, page_count - 1)] - owner * pages_dev, 0)
                slot = jnp.clip(slot, 0, pages_dev - 1)
                found.append((kv[side, k, slot, 0], kv[side, k, slot, 1], key_id < valid))
        return found

    def join(o1, e1, o2, e2, present):
        o2 = jnp.where(present, o2.astype(jnp.float32), 0.0)
        return merge(o1, e1, o2, jnp.where(present, e2, NEG_FILL))

    def assemble_right(p):
        k = jnp.maximum(p - out_base_r, 0)
        at = jnp.clip(k + LAG + in_base_r, 0, top)
        t = when(k, left_late)
        o, e = join(po[t], pe[t], la_o[at], la_e[at], has_left)
        came = (query_in_r > 0) & (p >= LAG) & (p < LAG + query_in_r)
        mine = own_query(jnp.where((query_in_r == 0) | (p < LAG), p, p - query_in_r))
        query = jnp.where(came, la_o[jnp.clip(p - LAG, 0, top)], mine)
        b_o[p] = jnp.where(p < query_out_r, query, o.astype(jnp.bfloat16))
        b_e[p] = e

    def assemble_left(p):
        k = jnp.maximum(p - out_base_l, 0)
        at = jnp.clip(k + LAG + in_base_l, 0, top)
        t = when(k, jnp.logical_not(left_late))
        o, e = join(po[t], pe[t], lc_o[at], lc_e[at], has_right)
        came = (query_in_l > 0) & (p >= LAG) & (p < LAG + query_in_l)
        mine = own_query(jnp.where((query_in_l == 0) | (p < LAG), p, p - query_in_l))
        query = jnp.where(came, lc_o[jnp.clip(p - LAG, 0, top)], mine)
        d_o[p] = jnp.where(p < query_out_l, query, o.astype(jnp.bfloat16))
        d_e[p] = e

    def compute(t):
        i = t - skip
        is_own = t >= foreign
        from_late = jnp.where(i < 2 * both, i % 2 == 0, left_late == (query_in_l > query_in_r)) & (i >= 0)
        side = (from_late == left_late).astype(jnp.int32)
        index = jnp.where(i < 0, t, skip + jnp.where(i < 2 * both, i // 2, i - both))
        index = jnp.clip(index, 0, top)
        home, rank = resolve(index, side)
        home = jnp.where(is_own, z, home)
        own_rank = jnp.clip(t - foreign, 0, seq_dev * parts - 1)
        rank = jnp.where(is_own, own_rank, rank)
        seq = slot_seq[jnp.minimum(start_tab[home] + rank // parts, slots - 1)]
        k = (rank % parts) // parts_head
        query = jnp.where(side == 0, la_o[index], lc_o[index])
        query = jnp.where(is_own, own_query(own_rank), query)
        blocks = pages_of(seq, k, each)
        local = jnp.clip(seq - first_seq, 0, seq_dev - 1)
        head = core * heads + k
        blocks.append((fresh[local, 0, head], fresh[local, 1, head], causal & is_own))
        o, e = attend(query, blocks)
        po[t] = o
        pe[t] = e

    few = min(each, -(-DEC_MAXP // owners))

    def compute_decode(i):
        d, k = i // heads, i % heads
        seq = rest_seq[d]
        local = jnp.clip(seq - first_seq, 0, seq_dev - 1)
        at_home = (seq // seq_dev == z).astype(jnp.int32)
        mine = (dec_of == d) & (dec_head == k)
        blocks = pages_of(seq, k, few)
        head = core * heads + k
        blocks.append((fresh[local, 0, head][:ROWS16], fresh[local, 1, head][:ROWS16], dec_fresh < at_home))
        o, e = attend(dec_all[...], blocks)
        dec_o[...] = jnp.where(mine, o, dec_o[...])
        dec_e[...] = jnp.where(mine, e, dec_e[...])

    top_row = lax.broadcasted_iota(jnp.int32, (rows, 1), 0) == 0

    def share(j, side):
        part = out.at[j, :, pl.ds(pl.multiple_of(side * width, width), width)]
        return pltpu.make_async_remote_copy(
            src_ref=part, dst_ref=part, send_sem=outs_sem.at[j], recv_sem=outr_sem.at[j],
            device_id={"sub": other}, device_id_type=MESH,
        )

    def finish(j):
        seq = first_seq + j
        chosen = flags[seq] == 1
        slot = slot_of[seq]
        for c in range(parts):
            rank = jnp.maximum((slot - my_start) * parts + c, 0)
            t = jnp.minimum(foreign + rank, work - 1)
            to_left = jnp.where((query_in_l == 0) | (rank < LAG), rank, rank + query_in_l)
            to_right = jnp.where((query_in_r == 0) | (rank < LAG), rank, rank + query_in_r)
            at_a = jnp.clip(to_left + in_base_r, 0, top)
            at_c = jnp.clip(to_right + in_base_l, 0, top)
            o, e = join(po[t], pe[t], la_o[at_a], la_e[at_a], has_left)
            o, e = join(o, e, lc_o[at_c], lc_e[at_c], has_right)
            turned = o.T
            for g in range(groups_part):
                h = c * groups_part + g
                line_at = h * rests + rest_of[seq]
                line = jnp.where(top_row, dec_fin[pl.ds(line_at, 1), :], 0.0)
                tile = jnp.where(chosen, turned[g * rows : (g + 1) * rows], line)
                place = pl.multiple_of(core * width + h * HD, HD)
                out[j, :, pl.ds(place, HD)] = tile.astype(out.dtype)
        share(j, core).start()

    middle = has_left & has_right

    def step(s, carry):
        p, w = s - parts + 1 - LAG * z, s - parts + 1 - LAG * (n - 1 - z)
        t, d, r = s - LAG, s - parts + 1 - reach, s - LAG

        @pl.when(has_left & (p == 0))
        def _():
            right_dq().wait_recv()

        @pl.when(has_right & (p == 0))
        def _():
            dqb[...] = jnp.where(dec_home == z, dec_own[...], dqa[...])
            right_dq().start()

        @pl.when(has_right & (w == 0))
        def _():
            left_dq().wait_recv()

        @pl.when(has_left & (w == 0))
        def _():
            dqd[...] = jnp.where(dec_home == z, dec_own[...], dqc[...])
            left_dq().start()

        @pl.when((r >= 0) & (r < in_r))
        def _():
            for x in right(r):
                x.wait_recv()
            la_o[r] = a_o[r]
            la_e[r] = a_e[r]

        @pl.when(jnp.logical_not(has_left) & (r >= 0) & (r < in_l))
        def _():
            for x in left(r):
                x.wait_recv()
            lc_o[r] = c_o[r]
            lc_e[r] = c_e[r]

        @pl.when(jnp.logical_not(middle) & (t == 0))
        def _():
            for x in kv_own:
                x.wait()
            for x in kv_far:
                x.wait_recv()

        @pl.when(jnp.logical_not(middle) & (t >= 0) & (t < work))
        def _():
            compute(t)

        @pl.when(s < out_r)
        def _():
            assemble_right(s)
            for x in right(s):
                x.start()

        @pl.when(has_left & (r >= 0) & (r < in_l))
        def _():
            for x in left(r):
                x.wait_recv()
            lc_o[r] = c_o[r]
            lc_e[r] = c_e[r]

        @pl.when(s < out_l)
        def _():
            assemble_left(s)
            for x in left(s):
                x.start()

        @pl.when(has_left & (p == dec_at))
        def _():
            for x in right_do():
                x.wait_recv()

        @pl.when(has_right & (p == dec_at))
        def _():
            o, e = join(dec_o[...], dec_e[...], doa[...], dea[...], has_left)
            dob[...] = o.astype(jnp.bfloat16)
            deb[...] = e
            for x in right_do():
                x.start()

        @pl.when(has_right & (w == dec_at))
        def _():
            for x in left_do():
                x.wait_recv()

        @pl.when(has_left & (w == dec_at))
        def _():
            o, e = join(dec_o[...], dec_e[...], doc[...], dec[...], has_right)
            dod[...] = o.astype(jnp.bfloat16)
            ded[...] = e
            for x in left_do():
                x.start()

        @pl.when(middle & (t == 0))
        def _():
            for x in kv_own:
                x.wait()
            for x in kv_far:
                x.wait_recv()

        @pl.when(s < parts - 1)
        def _():
            turn(s + 1)

        @pl.when(s == parts - 2)
        def _():
            for d in range(rests):
                local = jnp.clip(rest_seq[d] - first_seq, 0, seq_dev - 1)
                dec_rows[d : d + 1, :] = q_vm[local, 0:ROWS16, :].astype(jnp.float32)[0:1]
            stacked = jnp.concatenate(
                [dec_rows[:, h * HD : (h + 1) * HD] for h in range(heads * group_size)], axis=0
            )
            dec_own[...] = stacked.T.astype(jnp.bfloat16)

        @pl.when(s == LAG - 1)
        def _():
            small[3].wait()
            for j in range(seq_dev):
                for i in range(2):
                    for h in range(2 * heads):
                        fresh[j, i, h] = new_kv[j, :, i, h * HD : (h + 1) * HD]

        @pl.when(middle & (t >= 0) & (t < work))
        def _():
            compute(t)

        @pl.when(d == 0)
        def _():
            dec_all[...] = jnp.where(dec_home < z, dqa[...], jnp.where(dec_home == z, dec_own[...], dqc[...]))

        @pl.when((d >= 0) & (d < rests * heads))
        def _():
            compute_decode(d)

        @pl.when(s == dec_done)
        def _():
            o, e = join(dec_o[...], dec_e[...], doa[...], dea[...], has_left)
            o, e = join(o, e, doc[...], dec[...], has_right)
            dec_fin[...] = o.T

        @pl.when(functools.reduce(jnp.logical_or, [s == at for at in ready]))
        def _():
            finish(sum((s > at).astype(jnp.int32) for at in ready[:-1]))

        return carry

    steps = max(max(lengths) + LAG, work + LAG, dec_done + 1, ready[-1] + 1)
    lax.fori_loop(0, steps, step, 0)


    def drain_right(p, carry):
        for x in right(p):
            x.wait_send()
        return carry

    def drain_left(p, carry):
        for x in left(p):
            x.wait_send()
        return carry

    for x in kv_far:
        x.wait_send()

    lax.fori_loop(0, out_r, drain_right, 0)
    lax.fori_loop(0, out_l, drain_left, 0)

    @pl.when(has_right)
    def _():
        right_dq().wait_send()
        for x in right_do():
            x.wait_send()

    @pl.when(has_left)
    def _():
        left_dq().wait_send()
        for x in left_do():
            x.wait_send()

    def drain_out(j, carry):
        share(j, core).wait_send()
        share(j, other).wait_recv()
        return carry

    lax.fori_loop(0, seq_dev, drain_out, 0)


def fused_attention(queries, new_kv, kv_pages, page_table, cached_len, is_prefill):
    n = lax.axis_size("seq")
    sub_count = lax.axis_size("sub")
    seq_dev, rows, query_width = queries.shape
    pages_dev, kv_width = kv_pages.shape[0], kv_pages.shape[3]
    seqs = page_table.shape[0]
    slots = seqs // 2
    group_size = query_width // kv_width
    heads_all = kv_width // HD
    heads = heads_all // sub_count
    width = query_width // sub_count
    parts = heads * group_size * rows // LANES
    lengths, work, ready = stream_lengths(n, seq_dev, slots, parts)
    count = max(lengths)
    bf, f32 = jnp.bfloat16, jnp.float32
    dec = heads * group_size * (seqs - slots)

    def data(c, lanes=LANES):
        return pltpu.VMEM((c, HD, lanes), bf)

    def stat(c, lanes=LANES):
        return pltpu.VMEM((c, 1, lanes), f32)

    dma = pltpu.SemaphoreType.DMA
    scratch = [
        pltpu.SMEM(page_table.shape, jnp.int32),
        pltpu.SMEM(cached_len.shape, jnp.int32),
        pltpu.SMEM(is_prefill.shape, jnp.int32),
        pltpu.VMEM(new_kv.shape, bf),
        pltpu.VMEM((2, heads, pages_dev, 2, PAGE, HD), bf),
        pltpu.VMEM((seq_dev, rows, width), bf),
        data(seq_dev * parts),
        pltpu.VMEM((seq_dev, 2, heads_all, rows, HD), bf),
        pltpu.VMEM((seqs - slots, width), f32),
        pltpu.VMEM((HD, dec), bf),
        pltpu.VMEM((HD, dec), bf),
        pltpu.VMEM((HD, dec), f32),
        pltpu.VMEM((1, dec), f32),
        pltpu.VMEM((dec, HD), f32),
    ]
    scratch += [data(count), stat(count)] * 6
    scratch += [pltpu.VMEM((work, HD, LANES), f32), stat(work)]
    scratch += [pltpu.VMEM((HD, dec), bf)] * 4
    scratch += [pltpu.VMEM((HD, dec), bf), pltpu.VMEM((1, dec), f32)] * 4
    scratch += [pltpu.SMEM((slots,), jnp.int32), pltpu.SMEM((seqs - slots,), jnp.int32)]
    scratch += [pltpu.SMEM((seqs,), jnp.int32)] * 2
    scratch += [pltpu.SMEM((n,), jnp.int32)] * 2 + [pltpu.SMEM((2 * n,), jnp.int32)]
    scratch += [dma((4,)), dma((parts,)), dma((heads,)), dma((heads,)), dma((heads,))] + [dma((seq_dev,))] * 2
    scratch += [dma((count,))] * 8 + [dma((6,))] * 2
    operands = (page_table, cached_len, is_prefill, queries, new_kv, kv_pages)
    return pl.pallas_call(
        functools.partial(fused_kernel, n, lengths, work, ready, heads, group_size, rows, seq_dev, pages_dev),
        out_shape=jax.ShapeDtypeStruct(queries.shape, queries.dtype),
        in_specs=[pl.BlockSpec(memory_space=pltpu.HBM)] * 6,
        out_specs=pl.BlockSpec(memory_space=pltpu.VMEM),
        scratch_shapes=scratch,
        compiler_params=pltpu.CompilerParams(
            collective_id=0, has_side_effects=True, vmem_limit_bytes=48 * 1024 * 1024
        ),
        name="paged_attention",
    )(*[pltpu.with_memory_space_constraint(x, pltpu.HBM) for x in operands])


def per_device(queries, new_kv, kv_pages, page_table, cached_len, is_prefill):
    owners = lax.axis_size("seq") * lax.axis_size("sub")
    if page_table.shape[1] >= owners:
        return fused_attention(queries, new_kv, kv_pages, page_table, cached_len, is_prefill)
    return exchange_pages(queries, new_kv, kv_pages, page_table, cached_len, is_prefill)


def solution(mesh):
    placed = (
        P(("groups", "seq"), None, "head"),
        P(("groups", "seq"), None, None, "head"),
        P(("groups", "seq", "sub"), None, None, "head"),
        P("groups", None),
        P("groups"),
        P("groups"),
    )
    return jax.shard_map(
        per_device,
        mesh=mesh,
        in_specs=placed,
        out_specs=P(("groups", "seq"), None, "head"),
        check_vma=False,
    )
```

```python
import functools
import itertools

import jax
import jax.numpy as jnp
from jax import lax
from jax.experimental import pallas as pl
from jax.experimental.pallas import tpu as pltpu
from jax.sharding import PartitionSpec as P

HD = 128
PAGE = 128


NEG_FILL = -1e30


def partial_softmax(
    query_heads, cache_keys, cache_values, cache_valid, fresh_keys, fresh_values, fresh_valid
):
    score_scale = HD ** (-0.5)
    cache_scores = (
        jnp.einsum("rkgd,nkd->kgrn", query_heads, cache_keys, preferred_element_type=jnp.float32)
        * score_scale
    )
    fresh_scores = (
        jnp.einsum("rkgd,jkd->kgrj", query_heads, fresh_keys, preferred_element_type=jnp.float32)
        * score_scale
    )
    cache_mask = cache_valid[None, None, None, :]
    fresh_mask = fresh_valid[None, None, :, :]
    peak = jnp.maximum(
        jnp.max(jnp.where(cache_mask, cache_scores, NEG_FILL), axis=-1),
        jnp.max(jnp.where(fresh_mask, fresh_scores, NEG_FILL), axis=-1),
    )
    cache_weights = jnp.where(cache_mask, jnp.exp(cache_scores - peak[..., None]), 0.0)
    fresh_weights = jnp.where(fresh_mask, jnp.exp(fresh_scores - peak[..., None]), 0.0)
    weight_sum = jnp.sum(cache_weights, axis=-1) + jnp.sum(fresh_weights, axis=-1)
    numerator = jnp.einsum(
        "kgrn,nkd->kgrd",
        cache_weights.astype(jnp.bfloat16),
        cache_values,
        preferred_element_type=jnp.float32,
    )
    numerator = numerator + jnp.einsum(
        "kgrj,jkd->kgrd",
        fresh_weights.astype(jnp.bfloat16),
        fresh_values,
        preferred_element_type=jnp.float32,
    )
    return (peak, weight_sum, numerator)


def attend_all(
    query_block, fresh_block, received, fetch_index, page_here, lengths, live_rows, causal, fresh_on
):
    kv_width = received.shape[-1]
    heads_kv = kv_width // HD
    row_count = query_block.shape[1]
    group_size = query_block.shape[2] // kv_width
    page_count = fetch_index.shape[1]
    positions = jnp.arange(page_count * PAGE, dtype=jnp.int32)

    def one_sequence(inputs):
        query_rows, fresh_rows, index_row, here_row, length, live_row = inputs
        fetched = jnp.take(received, index_row, axis=0)
        cache_keys = fetched[:, 0].reshape(page_count * PAGE, heads_kv, HD)
        cache_values = fetched[:, 1].reshape(page_count * PAGE, heads_kv, HD)
        page_mask = jnp.broadcast_to(here_row[:, None], (page_count, PAGE)).reshape(
            page_count * PAGE
        )
        cache_valid = page_mask & (positions < length)
        query_heads = query_rows.reshape(row_count, heads_kv, group_size, HD)
        fresh_keys = fresh_rows[:, 0].reshape(row_count, heads_kv, HD)
        fresh_values = fresh_rows[:, 1].reshape(row_count, heads_kv, HD)
        fresh_valid = causal & live_row[:, None] & fresh_on
        return partial_softmax(
            query_heads,
            cache_keys,
            cache_values,
            cache_valid,
            fresh_keys,
            fresh_values,
            fresh_valid,
        )

    return lax.map(
        one_sequence, (query_block, fresh_block, fetch_index, page_here, lengths, live_rows)
    )


def finish(weight_sum, numerator, live_rows):
    unused_rows = 1.0 - live_rows.astype(jnp.float32)
    attended = numerator / (weight_sum + unused_rows[:, None, None, :])[..., None]
    attended = jnp.where(live_rows[:, None, None, :, None], attended, 0.0)
    seq_dev, heads_kv, group_size, row_count, head_dim = attended.shape
    return (
        jnp.transpose(attended, (0, 3, 1, 2, 4))
        .reshape(seq_dev, row_count, heads_kv * group_size * head_dim)
        .astype(jnp.bfloat16)
    )


def exchange_pages(queries, new_kv, kv_pages, page_table, cached_len, is_prefill):
    seq_shards = lax.axis_size("seq")
    sub_count = lax.axis_size("sub")
    owners = seq_shards * sub_count
    seq_index = lax.axis_index("seq")
    core_index = lax.axis_index("sub")
    owner_self = seq_index * sub_count + core_index
    seq_dev, row_count, query_width = queries.shape
    pages_dev = kv_pages.shape[0]
    kv_width = kv_pages.shape[3]
    page_count = page_table.shape[1]
    entries = seq_dev * page_count
    capacity = (entries + owners - 1) // owners
    table_rows = page_table.reshape(seq_shards, entries)
    holder = jnp.where(table_rows >= 0, table_rows // pages_dev, -1)
    slot_of = jnp.where(table_rows >= 0, table_rows % pages_dev, 0)
    owned_here = holder == owner_self
    rank_among = jnp.cumsum(owned_here.astype(jnp.int32), axis=1) - 1
    picked = owned_here[:, :, None] & (
        rank_among[:, :, None] == jnp.arange(capacity, dtype=jnp.int32)[None, None, :]
    )
    send_slots = jnp.sum(jnp.where(picked, slot_of[:, :, None], 0), axis=1).reshape(
        seq_shards * capacity
    )
    first_seq = seq_index * seq_dev
    my_table = lax.dynamic_slice_in_dim(page_table, first_seq, seq_dev, 0)
    my_lengths = lax.dynamic_slice_in_dim(cached_len, first_seq, seq_dev, 0)
    my_flags = lax.dynamic_slice_in_dim(is_prefill, first_seq, seq_dev, 0)
    flat_table = my_table.reshape(entries)
    my_holder = jnp.where(flat_table >= 0, flat_table // pages_dev, -1)
    entry_order = jnp.arange(entries, dtype=jnp.int32)
    earlier = (my_holder[:, None] == my_holder[None, :]) & (
        entry_order[None, :] < entry_order[:, None]
    )
    my_rank = jnp.sum(earlier.astype(jnp.int32), axis=1)
    row_ids = jnp.arange(row_count, dtype=jnp.int32)
    live_rows = (my_flags[:, None] == 1) | (row_ids[None, :] == 0)
    causal = row_ids[None, :] <= row_ids[:, None]
    part_width = kv_width // sub_count
    split_pages = kv_pages.reshape(pages_dev, 2, PAGE, sub_count, part_width)
    chosen = jnp.take(split_pages, send_slots, axis=0).reshape(
        seq_shards, capacity, 2, PAGE, sub_count, part_width
    )
    outgoing = jnp.moveaxis(chosen, 4, 1).reshape(owners, capacity, 2, PAGE, part_width)
    received = lax.all_to_all(
        outgoing, ("seq", "sub"), split_axis=0, concat_axis=0, tiled=True
    ).reshape(owners * capacity, 2, PAGE, part_width)
    present = flat_table >= 0
    fetch_index = jnp.where(present, my_holder * capacity + my_rank, 0)
    query_part = query_width // sub_count
    my_queries = lax.dynamic_slice_in_dim(queries, core_index * query_part, query_part, 2)
    my_fresh = lax.dynamic_slice_in_dim(new_kv, core_index * part_width, part_width, 3)
    peak, weight_sum, numerator = attend_all(
        my_queries,
        my_fresh,
        received,
        fetch_index.reshape(seq_dev, page_count),
        present.reshape(seq_dev, page_count),
        my_lengths,
        live_rows,
        causal,
        core_index >= 0,
    )
    own_heads = finish(weight_sum, numerator, live_rows)
    return lax.all_gather(own_heads, "sub", axis=2, tiled=True)


MESH = pl.DeviceIdType.MESH
SCALE = HD ** (-0.5)
LOG2E = 1.4426950408889634
DEC_MAXP = 4
LANES = 256
LAG = 3
ROWS16 = 16


def hi(a, b):
    return max(a, b) if isinstance(a, int) and isinstance(b, int) else jnp.maximum(a, b)


def lo(a, b):
    return min(a, b) if isinstance(a, int) and isinstance(b, int) else jnp.minimum(a, b)


def sel(c, a, b):
    return (a if c else b) if isinstance(c, bool) else jnp.where(c, a, b)


def query_spans(own):
    spans, leads, span, lead = [], [], 0, 0
    for count in own:
        lead = sel(count > 0, 0, LAG + lead)
        span = sel(span == 0, count, LAG + span + hi(count - LAG, 0))
        spans.append(span)
        leads.append(lead)
    return spans, leads


def work_order(ahead, lead_a, behind, lead_b):
    a, b = sel(ahead == 0, 0, lead_a), sel(behind == 0, 0, lead_b)
    swap = b >= a
    early, late = sel(swap, ahead, behind), sel(swap, behind, ahead)
    skip = lo(sel(swap, b - a, a - b), early)
    both = hi(lo(early - skip, late - skip), 0)
    delay = sel(b > a, sel(late - skip > both, both, hi(both - 1, 0)), both)
    return swap, skip, both, early + late - skip, delay


def chip_order(own, z):
    n = len(own)
    spans, leads = query_spans(own)
    back, back_leads = query_spans(own[::-1])
    ahead = (spans[z - 1], leads[z - 1]) if z else (0, 0)
    behind = (back[n - 2 - z], back_leads[n - 2 - z]) if z < n - 1 else (0, 0)
    return work_order(*ahead, *behind)


def stream_plan(own):
    n = len(own)
    spans, _ = query_spans(own)
    back, back_leads = query_spans(own[::-1])
    bases, base = [], 0
    for z in range(n - 1):
        clear = hi(spans[z] - back_leads[n - 2 - z], chip_order(own, z)[4] + LAG + (1 if z else 0))
        base = hi(base, clear)
        bases.append(base)
        base = base + 2 * LAG
    return spans, bases


def stream_lengths(n, seq_dev, slots, parts):
    lengths, work, ready = [0] * (n - 1), 0, [0] * seq_dev
    quiet = [LAG * slots * parts] * (n - 1)
    for counts in itertools.product(range(seq_dev + 1), repeat=n):
        if sum(counts) != slots or max(counts) != seq_dev:
            continue
        own = [parts * c for c in counts]
        spans, bases = stream_plan(own)
        back, back_bases = stream_plan(own[::-1])
        for z in range(n):
            ahead, behind = (spans[z - 1] if z else 0), (back[n - 2 - z] if z < n - 1 else 0)
            foreign = chip_order(own, z)[3]
            for k in range(own[z]):
                done = [LAG + 1 + foreign + k]
                if z:
                    done.append(LAG + bases[z - 1] + (k if behind == 0 or k < LAG else k + behind))
                if z < n - 1:
                    done.append(LAG + back_bases[n - 2 - z] + (k if ahead == 0 or k < LAG else k + ahead))
                for j in range(k // parts, seq_dev):
                    ready[j] = max(ready[j], *done)
            work = max(work, chip_order(own, z)[3] + own[z])
            if z < n - 1 and behind:
                quiet[z] = min(quiet[z], bases[z])
            if z < n - 1:
                lengths[z] = max(lengths[z], spans[z], bases[z] + behind if behind else 0)
    for j in range(1, seq_dev):
        ready[j] = max(ready[j], ready[j - 1] + 1)
    return lengths, work, ready, quiet


def pick(values, z):
    found = 0
    for j, value in enumerate(values):
        found = found + jnp.where(z == j, value, 0)
    return found


def merge(o1, e1, o2, e2):
    top = jnp.maximum(e1, e2)
    w1, w2 = jnp.exp(e1 - top), jnp.exp(e2 - top)
    total = w1 + w2
    inv = 1.0 / total
    return o1 * (w1 * inv) + o2 * (w2 * inv), top + jnp.log(total)


def attend(query, blocks):
    scored = []
    for keys, _, mask in blocks:
        s = lax.dot_general(keys, query, (((1,), (0,)), ((), ())), preferred_element_type=jnp.float32)
        scored.append(jnp.where(mask, s, NEG_FILL))
    peak = functools.reduce(jnp.maximum, [jnp.max(s, axis=0, keepdims=True) for s in scored])
    peak = jnp.maximum(peak, 0.1 * NEG_FILL)
    acc, total = None, None
    for s, (_, values, _) in zip(scored, blocks):
        weights = jnp.exp2((s - peak) * (SCALE * LOG2E))
        part = jnp.sum(weights, axis=0, keepdims=True)
        prod = lax.dot_general(
            values, weights.astype(jnp.bfloat16), (((0,), (0,)), ((), ())), preferred_element_type=jnp.float32
        )
        acc = prod if acc is None else acc + prod
        total = part if total is None else total + part
    empty = total == 0.0
    total = jnp.where(empty, 1.0, total)
    return acc * (1.0 / total), jnp.where(empty, NEG_FILL, peak * SCALE + jnp.log(total))


def fused_kernel(
    n, lengths, work, ready, quiet, heads, group_size, rows, seq_dev, pages_dev,
    table_hbm, cached_hbm, flags_hbm, q_hbm, new_hbm, kv_hbm, out,
    table, cached, flags, new_kv,
    kv, q_vm, own_t, fresh, dec_rows, dec_own, dec_all, dec_o, dec_e, dec_fin,
    a_o, a_e, b_o, b_e, c_o, c_e, d_o, d_e, la_o, la_e, lc_o, lc_e, po, pe,
    dqa, dqb, dqc, dqd, doa, dea, dob, deb, doc, dec, dod, ded,
    slot_seq, rest_seq, slot_of, rest_of, own_tab, start_tab, in_tab,
    in_sem, q_sem, kv_sem, kvs_sem, kvr_sem, outs_sem, outr_sem,
    bs, br, bes, ber, ds, dr, des, der, xs, xr,
):
    z, core = lax.axis_index("seq"), lax.axis_index("sub")
    other = 1 - core
    has_left, has_right = z > 0, z < n - 1
    seqs, page_count = table.shape
    owners = 2 * n
    each = page_count // owners
    slots = seqs // 2
    rests = seqs - slots
    width = q_vm.shape[2]
    groups_part = LANES // rows
    parts_head = group_size // groups_part
    parts = heads * parts_head
    first_seq = z * seq_dev
    head_lanes = group_size * rests
    dec_lanes = heads * head_lanes

    barrier = pltpu.get_barrier_semaphore()

    @pl.when(has_left)
    def _():
        pl.semaphore_signal(barrier, inc=1, device_id={"seq": z - 1}, device_id_type=MESH)

    @pl.when(has_right)
    def _():
        pl.semaphore_signal(barrier, inc=1, device_id={"seq": z + 1}, device_id_type=MESH)

    pl.semaphore_signal(barrier, inc=1, device_id={"sub": other}, device_id_type=MESH)

    small = [
        pltpu.make_async_copy(src, dst, in_sem.at[i])
        for i, (src, dst) in enumerate(
            ((table_hbm, table), (cached_hbm, cached), (flags_hbm, flags), (new_hbm, new_kv))
        )
    ]
    for x in small[:3]:
        x.start()
    piece = groups_part * HD

    def q_piece(c):
        src = pl.ds(pl.multiple_of(core * width + c * piece, piece), piece)
        dst = pl.ds(pl.multiple_of(c * piece, piece), piece)
        return pltpu.make_async_copy(q_hbm.at[:, :, src], q_vm.at[:, :, dst], q_sem.at[c])

    for c in range(parts):
        q_piece(c).start()

    def kv_cols(side, k):
        return kv_hbm.at[:, :, :, pl.ds(pl.multiple_of((side * heads + k) * HD, HD), HD)]

    kv_own = [pltpu.make_async_copy(kv_cols(core, k), kv.at[0, k], kv_sem.at[k]) for k in range(heads)]
    kv_far = [
        pltpu.make_async_remote_copy(
            src_ref=kv_cols(other, k), dst_ref=kv.at[1, k], send_sem=kvs_sem.at[k], recv_sem=kvr_sem.at[k],
            device_id={"sub": other}, device_id_type=MESH,
        )
        for k in range(heads)
    ]

    for x in small[:3]:
        x.wait()
    count, cum, own, before = 0, [], [], 0
    for j in range(seqs):
        count = count + flags[j]
        cum.append(count)
        slot_of[j] = jnp.clip(count - 1, 0, slots - 1)
        rest_of[j] = jnp.clip(j - count, 0, rests - 1)
        if j % seq_dev == seq_dev - 1:
            start_tab[j // seq_dev] = before
            own.append((count - before) * parts)
            own_tab[j // seq_dev] = own[-1]
            before = count
    for i in range(slots):
        slot_seq[i] = jnp.minimum(sum((c <= i).astype(jnp.int32) for c in cum), seqs - 1)
    for i in range(rests):
        rest_seq[i] = jnp.minimum(
            sum((j + 1 - c <= i).astype(jnp.int32) for j, c in enumerate(cum)), seqs - 1
        )
    spans_r, base_r = stream_plan(own)
    spans_l, base_l = stream_plan(own[::-1])
    ins_r, ins_l = [0] + spans_r[:-1], spans_l[::-1][1:] + [0]
    for w in range(n):
        in_tab[w] = ins_r[w]
        in_tab[n + w] = ins_l[w]
    query_in_r, query_in_l = pick(ins_r, z), pick(ins_l, z)
    query_out_r, query_out_l = pick(spans_r, z), pick(spans_l[::-1], z)
    orders = [chip_order(own, w) for w in range(n)]
    left_late = pick([jnp.asarray(x[0]).astype(jnp.int32) for x in orders], z) == 1
    skip, both, foreign = (pick([x[i] for x in orders], z) for i in (1, 2, 3))
    my_start = start_tab[z]
    out_base_r, in_base_r = pick(base_r + [0], z), pick([0] + base_r, z)
    out_base_l, in_base_l = pick(([0] + base_l[::-1]), z), pick(base_l[::-1] + [0], z)
    in_r, out_r = pick([0] + lengths, z), pick(lengths + [0], z)
    in_l, out_l = pick(lengths[::-1] + [0], z), pick([0] + lengths[::-1], z)
    quiet_in_r, quiet_out_r = pick([0] + quiet, z), pick(quiet + [0], z)
    quiet_in_l, quiet_out_l = pick(quiet[::-1] + [0], z), pick([0] + quiet[::-1], z)
    top = max(lengths) - 1
    reach = LAG * jnp.maximum(z, n - 1 - z)
    dec_at = LAG * (n - 1) + rests * heads
    dec_done = dec_at + parts - 1 + LAG * (n - 1)
    ready = [max(at, dec_done + 1 + j) for j, at in enumerate(ready)]

    def when(k, late):
        i = k - skip
        paired = skip + 2 * i + jnp.where(late, 0, 1)
        at = jnp.where(i < both, paired, skip + both + i)
        return jnp.clip(jnp.where(i < 0, k, at), 0, work - 1)

    def send(src, dst, s, r, to):
        return pltpu.make_async_remote_copy(
            src_ref=src, dst_ref=dst, send_sem=s, recv_sem=r, device_id={"seq": to}, device_id_type=MESH
        )

    def right(p):
        return (
            send(b_o.at[p], a_o.at[p], bs.at[p], br.at[p], z + 1),
            send(b_e.at[p], a_e.at[p], bes.at[p], ber.at[p], z + 1),
        )

    def left(p):
        return (
            send(d_o.at[p], c_o.at[p], ds.at[p], dr.at[p], z - 1),
            send(d_e.at[p], c_e.at[p], des.at[p], der.at[p], z - 1),
        )

    def right_dq():
        return send(dqb, dqa, xs.at[0], xr.at[0], z + 1)

    def left_dq():
        return send(dqd, dqc, xs.at[1], xr.at[1], z - 1)

    def right_do():
        return (send(dob, doa, xs.at[2], xr.at[2], z + 1), send(deb, dea, xs.at[3], xr.at[3], z + 1))

    def left_do():
        return (send(dod, doc, xs.at[4], xr.at[4], z - 1), send(ded, dec, xs.at[5], xr.at[5], z - 1))

    pl.semaphore_wait(barrier, has_left.astype(jnp.int32) + has_right.astype(jnp.int32) + 1)
    for x in kv_far:
        x.start()

    dec_lane = lax.broadcasted_iota(jnp.int32, (1, dec_lanes), 1)
    dec_of = dec_lane % rests
    dec_head = dec_lane // head_lanes
    dec_home = jnp.zeros((1, dec_lanes), jnp.int32)
    def turn(c):
        q_piece(c).wait()
        for j in range(seq_dev):
            stacked = jnp.concatenate(
                [q_vm[j, :, pl.ds(pl.multiple_of(c * piece + g * HD, HD), HD)] for g in range(groups_part)],
                axis=0,
            )
            own_t[j * parts + c] = stacked.astype(jnp.float32).T.astype(jnp.bfloat16)

    turn(0)
    kv_own[0].start()
    small[3].start()
    for d in range(rests):
        dec_home = jnp.where(dec_of == d, rest_seq[d] // seq_dev, dec_home)

    dec_o[...] = jnp.zeros_like(dec_o)
    dec_e[...] = jnp.full_like(dec_e, NEG_FILL)

    key_id = lax.broadcasted_iota(jnp.int32, (PAGE, 1), 0)
    fresh_id = lax.broadcasted_iota(jnp.int32, (rows, LANES), 0)
    lane_row = lax.broadcasted_iota(jnp.int32, (rows, LANES), 1) % rows
    causal = fresh_id <= lane_row
    dec_fresh = lax.broadcasted_iota(jnp.int32, (ROWS16, 1), 0)

    def own_query(rank):
        rank = jnp.clip(rank, 0, seq_dev * parts - 1)
        slot = jnp.minimum(my_start + rank // parts, slots - 1)
        local = jnp.clip(slot_seq[slot] - first_seq, 0, seq_dev - 1)
        return own_t[local * parts + rank % parts]

    def resolve(q, side):
        w, home, rank, done = z - 1 + 2 * side, 0, 0, False
        for _ in range(n - 1):
            w = jnp.clip(w, 0, n - 1)
            ahead = in_tab[side * n + w]
            direct = (ahead == 0) | (q < jnp.minimum(own_tab[w], LAG))
            hit = direct | (q >= LAG + ahead)
            found = hit & jnp.logical_not(done)
            home = jnp.where(found, w, home)
            rank = jnp.where(found, jnp.where(direct, q, q - ahead), rank)
            done = done | hit
            q = q - LAG
            w = w + 2 * side - 1
        return home, jnp.clip(rank, 0, seq_dev * parts - 1)

    def pages_of(seq, k, few):
        found = []
        start = table[seq, 0] // pages_dev
        for side, owner in enumerate((2 * z + core, 2 * z + other)):
            place = lax.rem(owner - start + owners, owners)
            for j in range(few):
                at = place + owners * j
                valid = jnp.clip(cached[seq] - PAGE * at, 0, PAGE)
                slot = jnp.where(valid > 0, table[seq, jnp.minimum(at, page_count - 1)] - owner * pages_dev, 0)
                slot = jnp.clip(slot, 0, pages_dev - 1)
                found.append((kv[side, k, slot, 0], kv[side, k, slot, 1], key_id < valid))
        return found

    def join(o1, e1, o2, e2, present):
        o2 = jnp.where(present, o2.astype(jnp.float32), 0.0)
        return merge(o1, e1, o2, jnp.where(present, e2, NEG_FILL))

    def assemble_right(p):
        k = jnp.maximum(p - out_base_r, 0)
        at = jnp.clip(k + LAG + in_base_r, 0, top)
        t = when(k, left_late)
        o, e = join(po[t], pe[t], la_o[at], la_e[at], has_left)
        came = (query_in_r > 0) & (p >= LAG) & (p < LAG + query_in_r)
        mine = own_query(jnp.where((query_in_r == 0) | (p < LAG), p, p - query_in_r))
        query = jnp.where(came, la_o[jnp.clip(p - LAG, 0, top)], mine)
        b_o[p] = jnp.where(p < query_out_r, query, o.astype(jnp.bfloat16))
        b_e[p] = e

    def assemble_left(p):
        k = jnp.maximum(p - out_base_l, 0)
        at = jnp.clip(k + LAG + in_base_l, 0, top)
        t = when(k, jnp.logical_not(left_late))
        o, e = join(po[t], pe[t], lc_o[at], lc_e[at], has_right)
        came = (query_in_l > 0) & (p >= LAG) & (p < LAG + query_in_l)
        mine = own_query(jnp.where((query_in_l == 0) | (p < LAG), p, p - query_in_l))
        query = jnp.where(came, lc_o[jnp.clip(p - LAG, 0, top)], mine)
        d_o[p] = jnp.where(p < query_out_l, query, o.astype(jnp.bfloat16))
        d_e[p] = e

    def compute(t):
        i = t - skip
        is_own = t >= foreign
        from_late = jnp.where(i < 2 * both, i % 2 == 0, left_late == (query_in_l > query_in_r)) & (i >= 0)
        side = (from_late == left_late).astype(jnp.int32)
        index = jnp.where(i < 0, t, skip + jnp.where(i < 2 * both, i // 2, i - both))
        index = jnp.clip(index, 0, top)
        home, rank = resolve(index, side)
        home = jnp.where(is_own, z, home)
        own_rank = jnp.clip(t - foreign, 0, seq_dev * parts - 1)
        rank = jnp.where(is_own, own_rank, rank)
        seq = slot_seq[jnp.minimum(start_tab[home] + rank // parts, slots - 1)]
        k = (rank % parts) // parts_head
        query = jnp.where(side == 0, la_o[index], lc_o[index])
        query = jnp.where(is_own, own_query(own_rank), query)
        blocks = pages_of(seq, k, each)
        local = jnp.clip(seq - first_seq, 0, seq_dev - 1)
        head = core * heads + k
        blocks.append((fresh[local, 0, head], fresh[local, 1, head], causal & is_own))
        o, e = attend(query, blocks)
        po[t] = o
        pe[t] = e

    few = min(each, -(-DEC_MAXP // owners))

    def compute_decode(i):
        d, k = i // heads, i % heads
        seq = rest_seq[d]
        local = jnp.clip(seq - first_seq, 0, seq_dev - 1)
        at_home = (seq // seq_dev == z).astype(jnp.int32)
        mine = (dec_of == d) & (dec_head == k)
        blocks = pages_of(seq, k, few)
        head = core * heads + k
        blocks.append((fresh[local, 0, head][:ROWS16], fresh[local, 1, head][:ROWS16], dec_fresh < at_home))
        o, e = attend(dec_all[...], blocks)
        dec_o[...] = jnp.where(mine, o, dec_o[...])
        dec_e[...] = jnp.where(mine, e, dec_e[...])

    top_row = lax.broadcasted_iota(jnp.int32, (rows, 1), 0) == 0

    def share(j, side):
        part = out.at[j, :, pl.ds(pl.multiple_of(side * width, width), width)]
        return pltpu.make_async_remote_copy(
            src_ref=part, dst_ref=part, send_sem=outs_sem.at[j], recv_sem=outr_sem.at[j],
            device_id={"sub": other}, device_id_type=MESH,
        )

    def finish(j):
        seq = first_seq + j
        chosen = flags[seq] == 1
        slot = slot_of[seq]
        for c in range(parts):
            rank = jnp.maximum((slot - my_start) * parts + c, 0)
            t = jnp.minimum(foreign + rank, work - 1)
            to_left = jnp.where((query_in_l == 0) | (rank < LAG), rank, rank + query_in_l)
            to_right = jnp.where((query_in_r == 0) | (rank < LAG), rank, rank + query_in_r)
            at_a = jnp.clip(to_left + in_base_r, 0, top)
            at_c = jnp.clip(to_right + in_base_l, 0, top)
            o, e = join(po[t], pe[t], la_o[at_a], la_e[at_a], has_left)
            o, e = join(o, e, lc_o[at_c], lc_e[at_c], has_right)
            turned = o.T
            for g in range(groups_part):
                h = c * groups_part + g
                line_at = h * rests + rest_of[seq]
                line = jnp.where(top_row, dec_fin[pl.ds(line_at, 1), :], 0.0)
                tile = jnp.where(chosen, turned[g * rows : (g + 1) * rows], line)
                place = pl.multiple_of(core * width + h * HD, HD)
                out[j, :, pl.ds(place, HD)] = tile.astype(out.dtype)
        share(j, core).start()

    middle = has_left & has_right

    def step(s, carry):
        p, w = s - parts + 1 - LAG * z, s - parts + 1 - LAG * (n - 1 - z)
        t, d, r = s - LAG, s - parts + 1 - reach, s - LAG

        @pl.when(has_left & (p == 0))
        def _():
            right_dq().wait_recv()

        @pl.when(has_right & (p == 0))
        def _():
            dqb[...] = jnp.where(dec_home == z, dec_own[...], dqa[...])
            right_dq().start()

        @pl.when(has_right & (w == 0))
        def _():
            left_dq().wait_recv()

        @pl.when(has_left & (w == 0))
        def _():
            dqd[...] = jnp.where(dec_home == z, dec_own[...], dqc[...])
            left_dq().start()

        @pl.when((r >= 0) & (r < in_r))
        def _():
            right(r)[0].wait_recv()
            la_o[r] = a_o[r]

            @pl.when(r >= quiet_in_r)
            def _():
                right(r)[1].wait_recv()
                la_e[r] = a_e[r]

        @pl.when(jnp.logical_not(has_left) & (r >= 0) & (r < in_l))
        def _():
            left(r)[0].wait_recv()
            lc_o[r] = c_o[r]

            @pl.when(r >= quiet_in_l)
            def _():
                left(r)[1].wait_recv()
                lc_e[r] = c_e[r]

        @pl.when(jnp.logical_not(middle) & (t == 0))
        def _():
            for x in kv_own:
                x.wait()
            for x in kv_far:
                x.wait_recv()

        @pl.when(jnp.logical_not(middle) & (t >= 0) & (t < work))
        def _():
            compute(t)

        @pl.when(s < out_r)
        def _():
            assemble_right(s)
            right(s)[0].start()

            @pl.when(s >= quiet_out_r)
            def _():
                right(s)[1].start()

        @pl.when(has_left & (r >= 0) & (r < in_l))
        def _():
            left(r)[0].wait_recv()
            lc_o[r] = c_o[r]

            @pl.when(r >= quiet_in_l)
            def _():
                left(r)[1].wait_recv()
                lc_e[r] = c_e[r]

        @pl.when(s < out_l)
        def _():
            assemble_left(s)
            left(s)[0].start()

            @pl.when(s >= quiet_out_l)
            def _():
                left(s)[1].start()

        @pl.when(has_left & (p == dec_at))
        def _():
            for x in right_do():
                x.wait_recv()

        @pl.when(has_right & (p == dec_at))
        def _():
            o, e = join(dec_o[...], dec_e[...], doa[...], dea[...], has_left)
            dob[...] = o.astype(jnp.bfloat16)
            deb[...] = e
            for x in right_do():
                x.start()

        @pl.when(has_right & (w == dec_at))
        def _():
            for x in left_do():
                x.wait_recv()

        @pl.when(has_left & (w == dec_at))
        def _():
            o, e = join(dec_o[...], dec_e[...], doc[...], dec[...], has_right)
            dod[...] = o.astype(jnp.bfloat16)
            ded[...] = e
            for x in left_do():
                x.start()

        @pl.when(middle & (t == 0))
        def _():
            for x in kv_own:
                x.wait()
            for x in kv_far:
                x.wait_recv()

        @pl.when(s == 0)
        def _():
            for x in kv_own[1:]:
                x.start()

        @pl.when(s < parts - 1)
        def _():
            turn(s + 1)

        @pl.when(s == parts - 2)
        def _():
            for d in range(rests):
                local = jnp.clip(rest_seq[d] - first_seq, 0, seq_dev - 1)
                dec_rows[d : d + 1, :] = q_vm[local, 0:ROWS16, :].astype(jnp.float32)[0:1]
            stacked = jnp.concatenate(
                [dec_rows[:, h * HD : (h + 1) * HD] for h in range(heads * group_size)], axis=0
            )
            dec_own[...] = stacked.T.astype(jnp.bfloat16)

        @pl.when(s == LAG - 1)
        def _():
            small[3].wait()
            for j in range(seq_dev):
                for i in range(2):
                    for h in range(2 * heads):
                        fresh[j, i, h] = new_kv[j, :, i, h * HD : (h + 1) * HD]

        @pl.when(middle & (t >= 0) & (t < work))
        def _():
            compute(t)

        @pl.when(d == 0)
        def _():
            dec_all[...] = jnp.where(dec_home < z, dqa[...], jnp.where(dec_home == z, dec_own[...], dqc[...]))

        @pl.when((d >= 0) & (d < rests * heads))
        def _():
            compute_decode(d)

        @pl.when(s == dec_done)
        def _():
            o, e = join(dec_o[...], dec_e[...], doa[...], dea[...], has_left)
            o, e = join(o, e, doc[...], dec[...], has_right)
            dec_fin[...] = o.T

        @pl.when(functools.reduce(jnp.logical_or, [s == at for at in ready]))
        def _():
            finish(sum((s > at).astype(jnp.int32) for at in ready[:-1]))

        return carry

    steps = max(max(lengths) + LAG, work + LAG, dec_done + 1, ready[-1] + 1)
    lax.fori_loop(0, steps, step, 0)


    def drain_right(p, carry):
        right(p)[0].wait_send()

        @pl.when(p >= quiet_out_r)
        def _():
            right(p)[1].wait_send()

        return carry

    def drain_left(p, carry):
        left(p)[0].wait_send()

        @pl.when(p >= quiet_out_l)
        def _():
            left(p)[1].wait_send()

        return carry

    for x in kv_far:
        x.wait_send()

    lax.fori_loop(0, out_r, drain_right, 0)
    lax.fori_loop(0, out_l, drain_left, 0)

    @pl.when(has_right)
    def _():
        right_dq().wait_send()
        for x in right_do():
            x.wait_send()

    @pl.when(has_left)
    def _():
        left_dq().wait_send()
        for x in left_do():
            x.wait_send()

    def drain_out(j, carry):
        share(j, core).wait_send()
        share(j, other).wait_recv()
        return carry

    lax.fori_loop(0, seq_dev, drain_out, 0)


def fused_attention(queries, new_kv, kv_pages, page_table, cached_len, is_prefill):
    n = lax.axis_size("seq")
    sub_count = lax.axis_size("sub")
    seq_dev, rows, query_width = queries.shape
    pages_dev, kv_width = kv_pages.shape[0], kv_pages.shape[3]
    seqs = page_table.shape[0]
    slots = seqs // 2
    group_size = query_width // kv_width
    heads_all = kv_width // HD
    heads = heads_all // sub_count
    width = query_width // sub_count
    parts = heads * group_size * rows // LANES
    lengths, work, ready, quiet = stream_lengths(n, seq_dev, slots, parts)
    count = max(lengths)
    bf, f32 = jnp.bfloat16, jnp.float32
    dec = heads * group_size * (seqs - slots)

    def data(c, lanes=LANES):
        return pltpu.VMEM((c, HD, lanes), bf)

    def stat(c, lanes=LANES):
        return pltpu.VMEM((c, 1, lanes), f32)

    dma = pltpu.SemaphoreType.DMA
    scratch = [
        pltpu.SMEM(page_table.shape, jnp.int32),
        pltpu.SMEM(cached_len.shape, jnp.int32),
        pltpu.SMEM(is_prefill.shape, jnp.int32),
        pltpu.VMEM(new_kv.shape, bf),
        pltpu.VMEM((2, heads, pages_dev, 2, PAGE, HD), bf),
        pltpu.VMEM((seq_dev, rows, width), bf),
        data(seq_dev * parts),
        pltpu.VMEM((seq_dev, 2, heads_all, rows, HD), bf),
        pltpu.VMEM((seqs - slots, width), f32),
        pltpu.VMEM((HD, dec), bf),
        pltpu.VMEM((HD, dec), bf),
        pltpu.VMEM((HD, dec), f32),
        pltpu.VMEM((1, dec), f32),
        pltpu.VMEM((dec, HD), f32),
    ]
    scratch += [data(count), stat(count)] * 6
    scratch += [pltpu.VMEM((work, HD, LANES), f32), stat(work)]
    scratch += [pltpu.VMEM((HD, dec), bf)] * 4
    scratch += [pltpu.VMEM((HD, dec), bf), pltpu.VMEM((1, dec), f32)] * 4
    scratch += [pltpu.SMEM((slots,), jnp.int32), pltpu.SMEM((seqs - slots,), jnp.int32)]
    scratch += [pltpu.SMEM((seqs,), jnp.int32)] * 2
    scratch += [pltpu.SMEM((n,), jnp.int32)] * 2 + [pltpu.SMEM((2 * n,), jnp.int32)]
    scratch += [dma((4,)), dma((parts,)), dma((heads,)), dma((heads,)), dma((heads,))] + [dma((seq_dev,))] * 2
    scratch += [dma((count,))] * 8 + [dma((6,))] * 2
    operands = (page_table, cached_len, is_prefill, queries, new_kv, kv_pages)
    return pl.pallas_call(
        functools.partial(fused_kernel, n, lengths, work, ready, quiet, heads, group_size, rows, seq_dev, pages_dev),
        out_shape=jax.ShapeDtypeStruct(queries.shape, queries.dtype),
        in_specs=[pl.BlockSpec(memory_space=pltpu.HBM)] * 6,
        out_specs=pl.BlockSpec(memory_space=pltpu.VMEM),
        scratch_shapes=scratch,
        compiler_params=pltpu.CompilerParams(
            collective_id=0, has_side_effects=True, vmem_limit_bytes=48 * 1024 * 1024
        ),
        name="paged_attention",
    )(*[pltpu.with_memory_space_constraint(x, pltpu.HBM) for x in operands])


def per_device(queries, new_kv, kv_pages, page_table, cached_len, is_prefill):
    owners = lax.axis_size("seq") * lax.axis_size("sub")
    if page_table.shape[1] >= owners:
        return fused_attention(queries, new_kv, kv_pages, page_table, cached_len, is_prefill)
    return exchange_pages(queries, new_kv, kv_pages, page_table, cached_len, is_prefill)


def solution(mesh):
    placed = (
        P(("groups", "seq"), None, "head"),
        P(("groups", "seq"), None, None, "head"),
        P(("groups", "seq", "sub"), None, None, "head"),
        P("groups", None),
        P("groups"),
        P("groups"),
    )
    return jax.shard_map(
        per_device,
        mesh=mesh,
        in_specs=placed,
        out_specs=P(("groups", "seq"), None, "head"),
        check_vma=False,
    )
```
